32 devices in a mesh: seq: 16 (over z, x, core), head: 2 (over y).
Axes of the slice: x: 2, y: 2, z: 4, core: 2. Of those that a mesh axis runs over, the one named last changes fastest.
Arguments:
- hidden: bfloat16 [4608, 8192], P('seq'), may hold values from -6 to 6
- norm_gain: bfloat16 [8192], replicated, may hold values from 0.099609375 to 1.8984375
- w_query: bfloat16 [8192, 1024], P('seq', 'head'), may hold values from -0.125 to 0.125
- w_key: bfloat16 [8192, 256], P('seq', 'head'), may hold values from -0.125 to 0.125
- w_value: bfloat16 [8192, 256], P('seq', 'head'), may hold values from -0.0625 to 0.0625
- bias_query: bfloat16 [1024], P('head'), may hold values from -3 to 3
- bias_key: bfloat16 [256], P('head'), may hold values from -200 to 200
- bias_value: bfloat16 [256], P('head'), may hold values from -3 to 3
- w_out: bfloat16 [1024, 8192], P('head', 'seq'), may hold values from -0.1875 to 0.1875
Outputs:
- attn_out: bfloat16 [4608, 8192], P(('seq', 'head'))
The draws below stay inside these ranges and needn't reach their ends.
All inputs are finite; a program needn't handle non-finite values.
Results may differ from the reference program's by a relative error of at most 0.014.
The reference program's roundings to bfloat16 on the way count: a program that leaves them out, or rounds other values in their place, can miss the bound.
Values may be sent and summed in bfloat16 or wider, within the bound.
A program may use at most 192 MiB of HBM per device.

```python
import jax
import jax.numpy as jnp
from jax import lax

D = 8192
HEAD_DIM = 128
QPG = 4
KV_HEADS = 2
LENGTH = 4608


def draw_bias_key(key, part):
    count = KV_HEADS * HEAD_DIM
    base = jax.random.normal(key, (count,), jnp.float32)
    return jnp.clip(0.5 * base, -3.0, 3.0).astype(jnp.bfloat16)


def steps_of(own_key, extent, split, least, high):
    gain = 1.0
    for position, shards_of in split:
        heights = jax.random.uniform(jax.random.fold_in(jax.random.fold_in(own_key, 6), position), (shards_of,), jnp.float32, least / len(split), high / len(split))
        gain = gain * jnp.repeat(jnp.exp(heights), extent[position] // shards_of).reshape((-1,) + (1,) * (len(extent) - 1 - position))
    return gain


def noise(own_key, dims, deviation, limit, split=(), kind=jnp.bfloat16):
    values = deviation * jax.random.normal(own_key, dims, jnp.float32)
    if split:
        values = values * steps_of(own_key, dims, split, -0.22, 0.18)
    return jnp.clip(values, -limit, limit).astype(kind)


def setup_inputs(seed: int = 0) -> dict:
    key_of = jax.random.split(jax.random.key(seed), 10)
    hidden = noise(key_of[0], (LENGTH, D), 1.0, 6.0, ((0, 16),))
    norm_gain = jnp.clip(1.0 + 0.18 * jax.random.normal(key_of[1], (D,), jnp.float32), 0.099609375, 1.8984375).astype(jnp.bfloat16)
    w_query = noise(key_of[2], (D, KV_HEADS * QPG * HEAD_DIM), (D // 4) ** -0.5, 0.125, ((0, 16), (1, 2)))
    w_key = noise(key_of[3], (D, KV_HEADS * HEAD_DIM), (D // 4) ** -0.5, 0.125, ((0, 16), (1, 2)))
    w_value = noise(key_of[4], (D, KV_HEADS * HEAD_DIM), D ** -0.5, 0.0625, ((0, 16), (1, 2)))
    bias_query = noise(key_of[5], (KV_HEADS * QPG * HEAD_DIM,), 0.5, 3.0, ((0, 2),))
    bias_key = draw_bias_key(jax.random.fold_in(key_of[9], 71), 0)
    bias_value = noise(key_of[7], (KV_HEADS * HEAD_DIM,), 0.5, 3.0, ((0, 2),))
    w_out = noise(key_of[8], (KV_HEADS * QPG * HEAD_DIM, D), (KV_HEADS * QPG * HEAD_DIM) ** -0.5, 0.1875, ((0, 2), (1, 16)))
    return dict(hidden=hidden, norm_gain=norm_gain, w_query=w_query, w_key=w_key, w_value=w_value, bias_query=bias_query, bias_key=bias_key, bias_value=bias_value, w_out=w_out)


ROPE_BASE = 1000000.0
EPSILON = 1e-06

def rotary(values, positions):
    half = values.shape[-1] // 2
    freq = ROPE_BASE ** (-2.0 * jnp.arange(half, dtype=jnp.float32) / values.shape[-1])
    angles = positions.astype(jnp.float32)[:, None, None] * freq[None, None, :]
    cosine = jnp.cos(angles)
    sine = jnp.sin(angles)
    first = values[..., :half]
    second = values[..., half:]
    return jnp.concatenate([first * cosine - second * sine, second * cosine + first * sine], axis=-1)

def reference(hidden, norm_gain, w_query, w_key, w_value, bias_query, bias_key, bias_value, w_out):
    length = hidden.shape[0]
    widened = hidden.astype(jnp.float32)
    inverse = lax.rsqrt(lax.optimization_barrier(jnp.mean(widened * widened, axis=-1, keepdims=True)) + EPSILON)
    normed = (widened * inverse * norm_gain.astype(jnp.float32)).astype(jnp.bfloat16)
    positions = jnp.arange(length, dtype=jnp.int32)
    query = jnp.dot(normed, w_query, preferred_element_type=jnp.float32) + bias_query.astype(jnp.float32)
    keys = jnp.dot(normed, w_key, preferred_element_type=jnp.float32) + bias_key.astype(jnp.float32)
    values = jnp.dot(normed, w_value, preferred_element_type=jnp.float32) + bias_value.astype(jnp.float32)
    query = rotary(query.reshape(length, KV_HEADS * QPG, HEAD_DIM), positions).astype(jnp.bfloat16)
    keys = rotary(keys.reshape(length, KV_HEADS, HEAD_DIM), positions).astype(jnp.bfloat16)
    values = values.reshape(length, KV_HEADS, HEAD_DIM).astype(jnp.bfloat16)
    query_groups = query.reshape(length, KV_HEADS, QPG, HEAD_DIM).transpose(1, 2, 0, 3)
    key_groups = keys.transpose(1, 0, 2)
    value_groups = values.transpose(1, 0, 2)
    causal = positions[:, None] >= positions[None, :]
    out_groups = w_out.reshape(KV_HEADS, QPG * HEAD_DIM, w_out.shape[1])

    def attend(carry, group):
        group_query, group_key, group_value, group_out = group
        scores = jnp.einsum('hqd,kd->hqk', group_query.astype(jnp.float32), group_key.astype(jnp.float32)) * HEAD_DIM ** (-0.5)
        scores = jnp.where(causal[None], scores, -jnp.inf)
        highest = lax.optimization_barrier(jnp.max(scores, axis=-1, keepdims=True))
        probs = jnp.exp(scores - highest)
        total = lax.optimization_barrier(jnp.sum(probs, axis=-1, keepdims=True))
        rounded = lax.optimization_barrier(probs.astype(jnp.bfloat16))
        mixed = jnp.einsum('hqk,kd->hqd', rounded.astype(jnp.float32), group_value.astype(jnp.float32))
        attended = (mixed / total).astype(jnp.bfloat16)
        attended = attended.transpose(1, 0, 2).reshape(length, QPG * HEAD_DIM)
        term = jnp.dot(attended, group_out, preferred_element_type=jnp.float32)
        term = lax.optimization_barrier(term.astype(jnp.bfloat16))
        return (carry + term.astype(jnp.float32), None)
    start = jnp.zeros((length, w_out.shape[1]), jnp.float32)
    summed, unused = lax.scan(attend, start, (query_groups, key_groups, value_groups, out_groups))
    return summed.astype(jnp.bfloat16)
```

```python
import functools

import jax
import jax.numpy as jnp
import numpy as np
from jax import lax
from jax.experimental import pallas as pl
from jax.experimental.pallas import tpu as pltpu
from jax.sharding import PartitionSpec as P

HEAD_DIM = 128
ROPE_BASE = 1000000.0
EPSILON = 1e-06
MESH = pl.DeviceIdType.MESH
F32 = jnp.float32
BF16 = jnp.bfloat16
VMEM_LIMIT = 48 * 1024 * 1024


def kernel(
    n, groups, exchange,
    hidden, w_query, w_key, w_value, w_out, gain, bias_query, bias_key, bias_value,
    near_cos, near_sin, far_cos, far_sin,
    out,
    hid, w_all, wo_all, acc, kv_all, q_ref, high, total, mixed, att, ts, tr, tm,
    load_sem, ws, wr, wps, wpr, os_, or_, ops, opr, ks, kr, kps, kpr, ys, yr,
):
    chips = n // 2
    depth = chips // 2
    me = lax.axis_index("seq")
    group = lax.axis_index("head")
    core = me % 2
    chip = me // 2
    ring = chip // 2 + (chip % 2) * (2 * depth - 1 - 2 * (chip // 2))

    def device_at(position, which):
        position = (position + 2 * chips) % chips
        side = position // depth
        row = position + side * (2 * depth - 1 - 2 * position)
        return 2 * (2 * row + side) + which

    right = device_at(ring + 1, core)
    left = device_at(ring - 1, core)
    partner = 2 * chip + (1 - core)
    neighbours = (right, left)

    def source_at(direction, offset, which):
        return device_at(ring - offset if direction == 0 else ring + offset, which)

    rows, width = hidden.shape
    half_depth = w_query.shape[0] // 2
    q_cols = w_query.shape[1]
    heads = q_cols // HEAD_DIM
    half_cols = w_out.shape[1] // 2
    rh = rows // groups

    loads = []
    late = [pltpu.make_async_copy(hidden, hid, load_sem.at[0])]
    for h in range(2):
        span = pl.ds(h * half_depth, half_depth)
        slot = w_all.at[2 * me + h]
        loads.append(pltpu.make_async_copy(w_query.at[span], slot.at[:, pl.ds(0, q_cols)], load_sem.at[1 + 4 * h]))
        loads.append(pltpu.make_async_copy(w_key.at[span], slot.at[:, pl.ds(q_cols, HEAD_DIM)], load_sem.at[2 + 4 * h]))
        loads.append(pltpu.make_async_copy(w_value.at[span], slot.at[:, pl.ds(q_cols + HEAD_DIM, HEAD_DIM)], load_sem.at[3 + 4 * h]))
        late.append(pltpu.make_async_copy(w_out.at[:, pl.ds(h * half_cols, half_cols)], wo_all.at[2 * me + h], load_sem.at[4 + 4 * h]))
    for copy in loads + late:
        copy.start()

    barrier = pltpu.get_barrier_semaphore()
    for device in (right, left, partner):
        pl.semaphore_signal(barrier, inc=1, device_id={"seq": device}, device_id_type=MESH)
    peers = range(1, groups) if exchange else ()
    for p in peers:
        pl.semaphore_signal(barrier, inc=1, device_id={"head": (group + p) % groups}, device_id_type=MESH)
    pl.semaphore_wait(barrier, 3 + len(peers))

    def remote(ref, send, recv, key, device):
        return pltpu.make_async_remote_copy(
            src_ref=ref, dst_ref=ref, send_sem=send.at[key], recv_sem=recv.at[key],
            device_id={"seq": device}, device_id_type=MESH,
        )

    def piece(buffer, index, j):
        size = buffer.shape[1] // 2
        return buffer.at[index, pl.ds(j * size, size)]

    def key_of(direction, step, j):
        return (direction * chips + step) * 2 + j

    def ring_begin(buffer, sems):
        ss, rs, pss, prs = sems
        for j in range(2):
            for d in range(2):
                own = piece(buffer, 2 * me + d, j)
                remote(own, ss, rs, key_of(d, 0, j), neighbours[d]).start()
        for j in range(2):
            for d in range(2):
                own = piece(buffer, 2 * me + d, j)
                remote(own, pss, prs, key_of(d, chips - 1, j), partner).start()

    def ring_advance(buffer, sems, t):
        ss, rs, pss, prs = sems

        @pl.when(t < chips - 1)
        def _():
            for j in range(2):
                for d in range(2):
                    block = piece(buffer, 2 * source_at(d, t + 1, core) + d, j)
                    remote(block, ss, rs, key_of(d, t, j), neighbours[d]).wait_recv()

                    @pl.when(t < chips - 2)
                    def _():
                        remote(block, ss, rs, key_of(d, t + 1, j), neighbours[d]).start()

                    remote(block, pss, prs, key_of(d, t, j), partner).start()

    def partner_wait(buffer, sems, t):
        ss, rs, pss, prs = sems
        for j in range(2):
            for d in range(2):
                block = piece(buffer, 2 * source_at(d, t, 1 - core) + d, j)
                remote(block, pss, prs, key_of(d, (t + chips - 1) % chips, j), partner).wait_recv()

    def ring_drain(buffer, sems):
        ss, rs, pss, prs = sems

        def body(t, carry):
            for j in range(2):
                for d in range(2):
                    block = piece(buffer, 2 * me + d, j)

                    @pl.when(t < chips - 1)
                    def _():
                        remote(block, ss, rs, key_of(d, t, j), neighbours[d]).wait_send()

                    remote(block, pss, prs, key_of(d, t, j), partner).wait_send()
            return carry

        lax.fori_loop(0, chips, body, 0)

    w_sems = (ws, wr, wps, wpr)
    o_sems = (os_, or_, ops, opr)

    for copy in loads:
        copy.wait()
    ring_begin(w_all, w_sems)
    for copy in late:
        copy.wait()
    slices = 2 * n
    step_cols = width // slices

    def columns(i):
        return pl.ds(pl.multiple_of(i * step_cols, step_cols), step_cols)

    def square(i, carry):
        x = hid[:, columns(i)].astype(F32)
        return carry + x * x

    squares = lax.fori_loop(0, slices, square, jnp.zeros((rows, step_cols), F32))
    inverse = lax.rsqrt(jnp.sum(squares, axis=-1, keepdims=True) * (1.0 / width) + EPSILON)

    def normed(i):
        scaled = hid[:, columns(i)].astype(F32) * inverse * gain[:, columns(i)].astype(F32)
        return scaled.astype(BF16)

    bias = (bias_query, bias_key, bias_value)
    starts = (0, q_cols, q_cols + HEAD_DIM)
    for start, part in zip(starts, bias):
        span = pl.ds(start, part.shape[1])
        acc[:, span] = jnp.broadcast_to(part[...].astype(F32), (rows, part.shape[1]))

    def project(t, carry):
        ring_advance(w_all, w_sems, t)
        partner_wait(w_all, w_sems, t)
        for d in range(2):
            i = 2 * source_at(d, t, core) + d
            k = 2 * source_at(d, t, 1 - core) + d
            acc[...] += jnp.dot(normed(i), w_all[i], preferred_element_type=F32) + jnp.dot(
                normed(k), w_all[k], preferred_element_type=F32
            )
        return carry

    lax.fori_loop(0, chips, project, 0)

    block_cos, block_sin = far_cos[me], far_sin[me]
    cosine = near_cos[...] * block_cos - near_sin[...] * block_sin
    lane = lax.broadcasted_iota(jnp.int32, cosine.shape, 1)
    sine = near_sin[...] * block_cos + near_cos[...] * block_sin
    sine = jnp.where(lane < HEAD_DIM // 2, -sine, sine)

    def rotary(x):
        return x * cosine + pltpu.roll(x, HEAD_DIM // 2, 1) * sine

    def kv_rows(which):
        return pl.ds(pl.multiple_of(which * rows, rows), rows)

    kv_all[chip, kv_rows(core), pl.ds(0, HEAD_DIM)] = rotary(acc[:, pl.ds(q_cols, HEAD_DIM)]).astype(BF16)
    kv_all[chip, kv_rows(core), pl.ds(HEAD_DIM, HEAD_DIM)] = acc[:, pl.ds(q_cols + HEAD_DIM, HEAD_DIM)].astype(BF16)
    for h in range(heads):
        q_ref[h] = rotary(acc[:, pl.ds(h * HEAD_DIM, HEAD_DIM)]).astype(BF16)

    reach = (chips // 2, chips - 1 - chips // 2)

    parts = 2 if rows % 32 == 0 else 1
    piece_rows = rows // parts

    def kv_copy(owner, ss, rs, direction, step, j, device):
        start = pl.multiple_of((owner % 2) * rows + j * piece_rows, piece_rows)
        block = kv_all.at[owner // 2, pl.ds(start, piece_rows)]
        return remote(block, ss, rs, key_of(direction, step, j), device)

    for j in range(parts):
        for d in range(2):
            kv_copy(me, ks, kr, d, 0, j, neighbours[d]).start()
        kv_copy(me, kps, kpr, 0, chips - 1, j, partner).start()

    factor = HEAD_DIM ** (-0.5) * 1.4426950408889634

    def attend(c, own):
        for h in range(heads):
            scores = lax.dot_general(
                q_ref[h], kv_all[c, :, pl.ds(0, HEAD_DIM)], (((1,), (1,)), ((), ())),
                preferred_element_type=F32,
            )
            if own:
                row = lax.broadcasted_iota(jnp.int32, scores.shape, 0) + core * rows
                col = lax.broadcasted_iota(jnp.int32, scores.shape, 1)
                scores = jnp.where(row >= col, scores, -jnp.inf)
            top = jnp.max(scores, axis=-1, keepdims=True)
            if not own:
                old = high[h]
                top = jnp.maximum(old, top)
            probs = jnp.exp2((scores - top) * factor)
            part = jnp.sum(probs, axis=-1, keepdims=True)
            product = jnp.dot(
                probs.astype(BF16), kv_all[c, :, pl.ds(HEAD_DIM, HEAD_DIM)], preferred_element_type=F32
            )
            if not own:
                shrink = jnp.exp2((old - top) * factor)
                part = part + total[h] * shrink
                product = product + mixed[h] * shrink
            high[h] = top
            total[h] = part
            mixed[h] = product

    for j in range(parts):
        kv_copy(partner, kps, kpr, 0, chips - 1, j, partner).wait_recv()
    attend(chip, True)

    def attention(t, carry):
        for j in range(parts):
            for d in range(2):
                @pl.when(t < reach[d])
                def _():
                    owner = source_at(d, t + 1, core)
                    kv_copy(owner, ks, kr, d, t, j, neighbours[d]).wait_recv()

                    @pl.when(t + 1 < reach[d])
                    def _():
                        kv_copy(owner, ks, kr, d, t + 1, j, neighbours[d]).start()

                    kv_copy(owner, kps, kpr, d, t, j, partner).start()

        @pl.when(t == reach[0] - 1)
        def _():
            ring_begin(wo_all, o_sems)

        for d in range(2):
            @pl.when((t > 0) & (t <= reach[d]))
            def _():
                owner = source_at(d, t, 1 - core)
                for j in range(parts):
                    kv_copy(owner, kps, kpr, d, t - 1, j, partner).wait_recv()

                @pl.when(owner // 2 < chip)
                def _():
                    attend(owner // 2, False)
        return carry

    lax.fori_loop(0, reach[0] + 1, attention, 0)
    for h in range(heads):
        att[:, pl.ds(h * HEAD_DIM, HEAD_DIM)] = (mixed[h] / total[h]).astype(BF16)

    def term_copy(p, i):
        return pltpu.make_async_remote_copy(
            src_ref=ts.at[p - 1, i], dst_ref=tr.at[p - 1, i],
            send_sem=ys.at[(p - 1) * slices + i], recv_sem=yr.at[(p - 1) * slices + i],
            device_id={"head": (group + p) % groups}, device_id_type=MESH,
        )

    def out_columns(i):
        return pl.ds(pl.multiple_of(i * half_cols, half_cols), half_cols)

    def make_term(i):
        if not exchange:
            out[:, out_columns(i)] = jnp.dot(att[...], wo_all[i], preferred_element_type=F32).astype(BF16)
            return
        for p in peers:
            span = pl.ds(pl.multiple_of(((group + p) % groups) * rh, rh), rh)
            ts[p - 1, i] = jnp.dot(att[span, :], wo_all[i], preferred_element_type=F32).astype(BF16)
            term_copy(p, i).start()
        span = pl.ds(pl.multiple_of(group * rh, rh), rh)
        tm[i] = jnp.dot(att[span, :], wo_all[i], preferred_element_type=F32).astype(BF16)

    def blocks_of(t):
        return [2 * source_at(d, t, which) + d for d in range(2) for which in (core, 1 - core)]

    def finish(t, carry):
        for i in blocks_of(t):
            value = tm[i].astype(F32)
            for p in peers:
                term_copy(p, i).wait_recv()
                value = value + tr[p - 1, i].astype(F32)
            out[:, out_columns(i)] = value.astype(BF16)
        return carry

    lag = 3

    def partner_terms(t):
        partner_wait(wo_all, o_sems, t)
        for d in range(2):
            make_term(2 * source_at(d, t, 1 - core) + d)

    for d in range(2):
        make_term(2 * me + d)
    partner_terms(0)

    def project_out(t, carry):
        ring_advance(wo_all, o_sems, t)

        @pl.when(t < chips - 1)
        def _():
            for d in range(2):
                make_term(2 * source_at(d, t + 1, core) + d)

        @pl.when(t > 0)
        def _():
            partner_terms(t)

        if exchange:
            @pl.when(t >= lag)
            def _():
                finish(t - lag, 0)
        return carry

    lax.fori_loop(0, chips, project_out, 0)

    if exchange:
        lax.fori_loop(chips - lag, chips, finish, 0)

        def sent(i, carry):
            for p in peers:
                term_copy(p, i).wait_send()
            return carry

        lax.fori_loop(0, slices, sent, 0)

    ring_drain(w_all, w_sems)
    ring_drain(wo_all, o_sems)
    for j in range(parts):
        for d in range(2):
            for t in range(reach[d]):
                kv_copy(me, ks, kr, d, t, j, neighbours[d]).wait_send()
                kv_copy(me, kps, kpr, d, t, j, partner).wait_send()
        kv_copy(me, kps, kpr, 0, chips - 1, j, partner).wait_send()


def pair_kernel(
    n, chunks_wide, chunks_narrow, chunks_out,
    hidden, w_query, w_key, w_value, w_out, gain, bias_query, bias_key, bias_value,
    near_cos, near_sin, far_cos, far_sin,
    out,
    hid, w_first, w_second, wo, acc_first, acc_second, kv_all, q_ref, high, total, mixed, att, terms,
    load_sem, swap_s, swap_r, att_s, att_r, own_s, ys, yr,
    fs, fr, fps, fpr, ss, sr, sps, spr, os_, or_, ops, opr, ks, kr, kps, kpr,
):
    chips = n // 2
    depth = chips // 2
    me = lax.axis_index("seq")
    group = lax.axis_index("head")
    peer = 1 - group
    core = me % 2
    chip = me // 2
    ring = chip // 2 + (chip % 2) * (2 * depth - 1 - 2 * (chip // 2))

    def device_at(position, which):
        position = (position + 2 * chips) % chips
        side = position // depth
        row = position + side * (2 * depth - 1 - 2 * position)
        return 2 * (2 * row + side) + which

    right = device_at(ring + 1, core)
    left = device_at(ring - 1, core)
    partner = 2 * chip + (1 - core)
    neighbours = (right, left)

    def source_at(direction, offset, which):
        return device_at(ring - offset if direction == 0 else ring + offset, which)

    rows, width = hidden.shape
    half_depth = w_query.shape[0] // 2
    q_cols = w_query.shape[1]
    heads = q_cols // HEAD_DIM
    early = heads // 2
    q_early = early * HEAD_DIM
    q_late = q_cols - q_early
    out_depth = w_out.shape[0]
    group_cols = w_out.shape[1] // 2
    lane_cols = group_cols // 2
    rh = rows // 2

    def remote(ref, send, recv, key, device):
        return pltpu.make_async_remote_copy(
            src_ref=ref, dst_ref=ref, send_sem=send.at[key], recv_sem=recv.at[key],
            device_id={"seq": device}, device_id_type=MESH,
        )

    def lanes(which):
        return pl.ds(pl.multiple_of(which * lane_cols, lane_cols), lane_cols)

    def wo_lanes(which, d):
        start = which * group_cols + d * lane_cols
        return pl.ds(pl.multiple_of(start, lane_cols), lane_cols)

    def group_rows(which):
        return pl.ds(pl.multiple_of(which * out_depth, out_depth), out_depth)

    loads, later, last = [], [], []
    for h in range(2):
        span = pl.ds(h * half_depth, half_depth)
        slot = w_first.at[2 * me + h]
        loads.append((w_key.at[span], slot.at[:, pl.ds(0, HEAD_DIM)]))
        loads.append((w_value.at[span], slot.at[:, pl.ds(HEAD_DIM, HEAD_DIM)]))
        loads.append((w_query.at[span, pl.ds(0, q_early)], slot.at[:, pl.ds(2 * HEAD_DIM, q_early)]))
        later.append((w_query.at[span, pl.ds(q_early, q_late)], w_second.at[2 * me + h]))
        last.append((w_out.at[:, wo_lanes(group, h)], wo.at[chip, h, group_rows(group), lanes(core)]))
    later.append((hidden, hid))
    copies = [pltpu.make_async_copy(a, b, load_sem.at[i]) for i, (a, b) in enumerate(loads + later + last)]
    for copy in copies:
        copy.start()

    barrier = pltpu.get_barrier_semaphore()
    for device in (right, left, partner):
        pl.semaphore_signal(barrier, inc=1, device_id={"seq": device}, device_id_type=MESH)
    pl.semaphore_signal(barrier, inc=1, device_id={"head": peer}, device_id_type=MESH)
    pl.semaphore_wait(barrier, 4)

    def across(src, dst, send, recv, key):
        return pltpu.make_async_remote_copy(
            src_ref=src, dst_ref=dst, send_sem=send.at[key], recv_sem=recv.at[key],
            device_id={"head": peer}, device_id_type=MESH,
        )

    def swap(d):
        return across(
            w_out.at[:, wo_lanes(peer, d)], wo.at[chip, d, group_rows(group), lanes(core)], swap_s, swap_r, d
        )

    class Ring:
        def __init__(self, view, sems, pieces):
            self.view, self.sems, self.pieces = view, sems, pieces

        def key(self, d, step, j):
            return (d * chips + step) * self.pieces + j

        def begin(self, j):
            send, recv, psend, precv = self.sems
            for d in range(2):
                own = self.view(me, d, j)
                remote(own, send, recv, self.key(d, 0, j), neighbours[d]).start()
            for d in range(2):
                own = self.view(me, d, j)
                remote(own, psend, precv, self.key(d, chips - 1, j), partner).start()

        def advance(self, t, j):
            send, recv, psend, precv = self.sems
            for d in range(2):
                block = self.view(source_at(d, t + 1, core), d, j)
                remote(block, send, recv, self.key(d, t, j), neighbours[d]).wait_recv()

                @pl.when(t < chips - 2)
                def _():
                    remote(block, send, recv, self.key(d, t + 1, j), neighbours[d]).start()

                remote(block, psend, precv, self.key(d, t, j), partner).start()

        def partner_wait(self, t):
            send, recv, psend, precv = self.sems
            for j in range(self.pieces):
                for d in range(2):
                    block = self.view(source_at(d, t, 1 - core), d, j)
                    remote(block, psend, precv, self.key(d, (t + chips - 1) % chips, j), partner).wait_recv()

        def drain(self):
            send, recv, psend, precv = self.sems

            def body(t, carry):
                for j in range(self.pieces):
                    for d in range(2):
                        block = self.view(me, d, j)

                        @pl.when(t < chips - 1)
                        def _():
                            remote(block, send, recv, self.key(d, t, j), neighbours[d]).wait_send()

                        remote(block, psend, precv, self.key(d, t, j), partner).wait_send()
                return carry

            lax.fori_loop(0, chips, body, 0)

    def rows_view(buffer, pieces):
        size = buffer.shape[1] // pieces
        return lambda owner, d, j: buffer.at[2 * owner + d, pl.ds(pl.multiple_of(j * size, size), size)]

    def wo_view(owner, d, j):
        size = wo.shape[2] // chunks_out
        return wo.at[owner // 2, d, pl.ds(pl.multiple_of(j * size, size), size), lanes(owner % 2)]

    first = Ring(rows_view(w_first, chunks_wide), (fs, fr, fps, fpr), chunks_wide)
    second = Ring(rows_view(w_second, chunks_narrow), (ss, sr, sps, spr), chunks_narrow)
    third = Ring(wo_view, (os_, or_, ops, opr), chunks_out)

    for copy in copies[: len(loads)]:
        copy.wait()
    for j in range(chunks_wide):
        first.begin(j)
    for d in range(2):
        swap(d).start()
    for copy in copies[len(loads):]:
        copy.wait()

    slices = 2 * n
    step_cols = width // slices

    def columns(i):
        return pl.ds(pl.multiple_of(i * step_cols, step_cols), step_cols)

    def square(i, carry):
        x = hid[:, columns(i)].astype(F32)
        return carry + x * x

    squares = lax.fori_loop(0, slices, square, jnp.zeros((rows, step_cols), F32))
    inverse = lax.rsqrt(jnp.sum(squares, axis=-1, keepdims=True) * (1.0 / width) + EPSILON)

    def normed(i):
        scaled = hid[:, columns(i)].astype(F32) * inverse * gain[:, columns(i)].astype(F32)
        value = scaled.astype(BF16)
        hid[:, columns(i)] = value
        return value

    def widen(value, size):
        return jnp.broadcast_to(value.astype(F32), (rows, size))

    acc_first[:, pl.ds(0, HEAD_DIM)] = widen(bias_key[...], HEAD_DIM)
    acc_first[:, pl.ds(HEAD_DIM, HEAD_DIM)] = widen(bias_value[...], HEAD_DIM)
    acc_first[:, pl.ds(2 * HEAD_DIM, q_early)] = widen(bias_query[:, pl.ds(0, q_early)], q_early)
    acc_second[...] = widen(bias_query[:, pl.ds(q_early, q_late)], q_late)

    def project_first(t, carry):
        @pl.when(t < chips - 1)
        def _():
            for j in range(chunks_wide):
                first.advance(t, j)

        @pl.when(t == chips - 3)
        def _():
            for j in range(chunks_narrow):
                second.begin(j)

        first.partner_wait(t)
        for d in range(2):
            i = 2 * source_at(d, t, core) + d
            k = 2 * source_at(d, t, 1 - core) + d
            acc_first[...] += jnp.dot(normed(i), w_first[i], preferred_element_type=F32) + jnp.dot(
                normed(k), w_first[k], preferred_element_type=F32
            )
        return carry

    lax.fori_loop(0, chips, project_first, 0)

    block_cos, block_sin = far_cos[me], far_sin[me]
    cosine = near_cos[...] * block_cos - near_sin[...] * block_sin
    lane = lax.broadcasted_iota(jnp.int32, cosine.shape, 1)
    sine = near_sin[...] * block_cos + near_cos[...] * block_sin
    sine = jnp.where(lane < HEAD_DIM // 2, -sine, sine)

    def rotary(x):
        return x * cosine + pltpu.roll(x, HEAD_DIM // 2, 1) * sine

    def kv_rows(which):
        return pl.ds(pl.multiple_of(which * rows, rows), rows)

    kv_all[chip, kv_rows(core), pl.ds(0, HEAD_DIM)] = rotary(acc_first[:, pl.ds(0, HEAD_DIM)]).astype(BF16)
    kv_all[chip, kv_rows(core), pl.ds(HEAD_DIM, HEAD_DIM)] = acc_first[:, pl.ds(HEAD_DIM, HEAD_DIM)].astype(BF16)
    for h in range(early):
        q_ref[h] = rotary(acc_first[:, pl.ds((2 + h) * HEAD_DIM, HEAD_DIM)]).astype(BF16)

    reach = (chips // 2, chips - 1 - chips // 2)
    parts = 2 if rows % 32 == 0 else 1
    piece_rows = rows // parts

    def kv_copy(owner, send, recv, direction, step, j, device):
        start = pl.multiple_of((owner % 2) * rows + j * piece_rows, piece_rows)
        block = kv_all.at[owner // 2, pl.ds(start, piece_rows)]
        return remote(block, send, recv, (direction * chips + step) * parts + j, device)

    for j in range(parts):
        for d in range(2):
            kv_copy(me, ks, kr, d, 0, j, neighbours[d]).start()
        kv_copy(me, kps, kpr, 0, chips - 1, j, partner).start()
    for j in range(chunks_narrow):
        second.advance(0, j)

    factor = HEAD_DIM ** (-0.5) * 1.4426950408889634

    def attend(c, own, which):
        for h in which:
            scores = lax.dot_general(
                q_ref[h], kv_all[c, :, pl.ds(0, HEAD_DIM)], (((1,), (1,)), ((), ())),
                preferred_element_type=F32,
            )
            if own:
                row = lax.broadcasted_iota(jnp.int32, scores.shape, 0) + core * rows
                col = lax.broadcasted_iota(jnp.int32, scores.shape, 1)
                scores = jnp.where(row >= col, scores, -jnp.inf)
            top = jnp.max(scores, axis=-1, keepdims=True)
            if not own:
                old = high[h]
                top = jnp.maximum(old, top)
            probs = jnp.exp2((scores - top) * factor)
            part = jnp.sum(probs, axis=-1, keepdims=True)
            product = jnp.dot(
                probs.astype(BF16), kv_all[c, :, pl.ds(HEAD_DIM, HEAD_DIM)], preferred_element_type=F32
            )
            if not own:
                shrink = jnp.exp2((old - top) * factor)
                part = part + total[h] * shrink
                product = product + mixed[h] * shrink
            high[h] = top
            total[h] = part
            mixed[h] = product

    sooner, rest = range(early), range(early, heads)
    for j in range(parts):
        kv_copy(partner, kps, kpr, 0, chips - 1, j, partner).wait_recv()
    attend(chip, True, sooner)

    for d in range(2):
        swap(d).wait_recv()

    def attention(t, carry):
        for j in range(parts):
            for d in range(2):
                @pl.when(t < reach[d])
                def _():
                    owner = source_at(d, t + 1, core)
                    kv_copy(owner, ks, kr, d, t, j, neighbours[d]).wait_recv()

                    @pl.when(t + 1 < reach[d])
                    def _():
                        kv_copy(owner, ks, kr, d, t + 1, j, neighbours[d]).start()

                    kv_copy(owner, kps, kpr, d, t, j, partner).start()

        @pl.when(t + 1 < chips - 1)
        def _():
            for j in range(chunks_narrow):
                second.advance(t + 1, j)

        for j in range(chunks_out):
            @pl.when(t == min(reach[0] - 1 + j, chips - 3))
            def _():
                third.begin(j)

        for d in range(2):
            @pl.when((t > 0) & (t <= reach[d]))
            def _():
                owner = source_at(d, t, 1 - core)
                for j in range(parts):
                    kv_copy(owner, kps, kpr, d, t - 1, j, partner).wait_recv()

                @pl.when(owner // 2 < chip)
                def _():
                    attend(owner // 2, False, sooner)

        second.partner_wait(t)
        for d in range(2):
            i = 2 * source_at(d, t, core) + d
            k = 2 * source_at(d, t, 1 - core) + d
            acc_second[...] += jnp.dot(hid[:, columns(i)], w_second[i], preferred_element_type=F32) + jnp.dot(
                hid[:, columns(k)], w_second[k], preferred_element_type=F32
            )
        return carry

    lax.fori_loop(0, chips, attention, 0)

    def head_span(which):
        return pl.ds(which[0] * HEAD_DIM, len(which) * HEAD_DIM)

    def att_copy(key, which):
        ref = att.at[group, :, head_span(which)]
        return across(ref, ref, att_s, att_r, key)

    def settle(which):
        for h in which:
            att[group, :, pl.ds(h * HEAD_DIM, HEAD_DIM)] = (mixed[h] / total[h]).astype(BF16)

    settle(sooner)
    for h in rest:
        q_ref[h] = rotary(acc_second[:, pl.ds((h - early) * HEAD_DIM, HEAD_DIM)]).astype(BF16)
    att_copy(0, sooner).start()
    attend(chip, True, rest)

    def attention_rest(c, carry):
        third.advance(c // chunks_out, c % chunks_out)

        @pl.when(c < chip)
        def _():
            attend(c, False, rest)
        return carry

    lax.fori_loop(0, chips, attention_rest, 0)
    settle(rest)
    att_copy(1, rest).start()
    lead = chips // chunks_out

    def out_copy(c, d, which, key):
        start = (2 * c + which) * 2 * group_cols + group * group_cols + d * lane_cols
        span = pl.ds(pl.multiple_of(start, lane_cols), lane_cols)
        src = terms.at[c, d, pl.ds(pl.multiple_of(group * rh, rh), rh), lanes(which)]
        return pltpu.make_async_copy(src, out.at[:, span], own_s.at[key])

    def peer_copy(c, d, which, key):
        start = (2 * c + which) * 2 * group_cols + group * group_cols + d * lane_cols
        span = pl.ds(pl.multiple_of(start, lane_cols), lane_cols)
        src = terms.at[c, d, pl.ds(pl.multiple_of(peer * rh, rh), rh), lanes(which)]
        return across(src, out.at[:, span], ys, yr, key)

    def chip_keys(c, d):
        return [(which, (2 * c + d) * 2 + which) for which in range(2)]

    def make_term(t, d):
        c = source_at(d, t, core) // 2
        value = None
        for g in range(2):
            depth_rows = pl.ds(g * out_depth, out_depth)
            term = jnp.dot(att[g], wo[c, d, depth_rows, :], preferred_element_type=F32).astype(BF16).astype(F32)
            value = term if value is None else value + term
        terms[c, d] = value.astype(BF16)
        for which, key in chip_keys(c, d):
            peer_copy(c, d, which, key).start()
            out_copy(c, d, which, key).start()

    att_copy(0, sooner).wait_recv()
    att_copy(1, rest).wait_recv()

    def project_out(t, carry):
        third.partner_wait(t)
        for j in range(chunks_out):
            @pl.when((t >= lead) & (t < chips - 1))
            def _():
                third.advance(t, j)

            if j < 2:
                make_term(t, j)
        return carry

    lax.fori_loop(0, chips, project_out, 0)

    first.drain()
    second.drain()
    third.drain()
    for j in range(parts):
        for d in range(2):
            for t in range(reach[d]):
                kv_copy(me, ks, kr, d, t, j, neighbours[d]).wait_send()
                kv_copy(me, kps, kpr, d, t, j, partner).wait_send()
        kv_copy(me, kps, kpr, 0, chips - 1, j, partner).wait_send()
    for d in range(2):
        swap(d).wait_send()
    att_copy(0, sooner).wait_send()
    att_copy(1, rest).wait_send()

    def finish(c, carry):
        for d in range(2):
            for which, key in chip_keys(c, d):
                peer_copy(c, d, which, key).wait_send()
                out_copy(c, d, which, key).wait()
                peer_copy(c, d, which, key).wait_recv()
        return carry

    lax.fori_loop(0, chips, finish, 0)


def tables_of(n, rows):
    freq = ROPE_BASE ** (-2.0 * np.arange(HEAD_DIM // 2, dtype=np.float64) / HEAD_DIM)
    freq = np.concatenate([freq, freq])
    near = np.arange(rows, dtype=np.float64)[:, None] * freq
    far = (np.arange(n, dtype=np.float64) * rows)[:, None, None] * freq
    return [f(a).astype(np.float32) for a in (near, far) for f in (np.cos, np.sin)]


def pair_local(n, hidden, norm_gain, w_query, w_key, w_value, bias_query, bias_key, bias_value, w_out):
    rows, width = hidden.shape
    cols = w_query.shape[1]
    heads = cols // HEAD_DIM
    early = heads // 2 * HEAD_DIM
    chips = n // 2
    slices = 2 * n
    half_depth = w_query.shape[0] // 2
    group_cols = w_out.shape[1] // 2
    wide, narrow, fine = 4, 2, 4
    vectors = [v.reshape(1, -1) for v in (norm_gain, bias_query, bias_key, bias_value)]
    any_spec = pl.BlockSpec(memory_space=pl.ANY)
    vmem = pl.BlockSpec(memory_space=pltpu.VMEM)
    dma = pltpu.SemaphoreType.DMA
    return pl.pallas_call(
        functools.partial(pair_kernel, n, wide, narrow, fine),
        out_shape=jax.ShapeDtypeStruct((rows // 2, w_out.shape[1] * n), BF16),
        in_specs=[pl.BlockSpec(memory_space=pltpu.HBM)] * 5 + [vmem] * 8,
        out_specs=any_spec,
        scratch_shapes=[
            pltpu.VMEM((rows, width), BF16),
            pltpu.VMEM((slices, half_depth, 2 * HEAD_DIM + early), BF16),
            pltpu.VMEM((slices, half_depth, cols - early), BF16),
            pltpu.VMEM((chips, 2, 2 * w_out.shape[0], group_cols), BF16),
            pltpu.VMEM((rows, 2 * HEAD_DIM + early), F32),
            pltpu.VMEM((rows, cols - early), F32),
            pltpu.VMEM((chips, 2 * rows, 2 * HEAD_DIM), BF16),
            pltpu.VMEM((heads, rows, HEAD_DIM), BF16),
            pltpu.VMEM((heads, rows, 1), F32),
            pltpu.VMEM((heads, rows, 1), F32),
            pltpu.VMEM((heads, rows, HEAD_DIM), F32),
            pltpu.VMEM((2, rows, cols), BF16),
            pltpu.VMEM((chips, 2, rows, group_cols), BF16),
            dma((11,)),
            dma((2,)), dma((2,)), dma((2,)), dma((2,)),
            dma((4 * chips,)), dma((4 * chips,)), dma((4 * chips,)),
        ]
        + [dma((2 * chips * wide,))] * 4
        + [dma((2 * chips * narrow,))] * 4
        + [dma((2 * chips * fine,))] * 4
        + [dma((4 * chips,))] * 4,
        compiler_params=pltpu.CompilerParams(
            collective_id=0, has_side_effects=True, vmem_limit_bytes=VMEM_LIMIT
        ),
    )(hidden, w_query, w_key, w_value, w_out, *vectors, *tables_of(n, rows))


def fits_pair(n, groups, rows, w_query, w_out):
    chips = n // 2
    return (
        groups == 2
        and chips % 4 == 0
        and rows % 32 == 0
        and w_query.shape[1] % (2 * HEAD_DIM) == 0
        and w_query.shape[0] % 128 == 0
        and w_out.shape[1] % 512 == 0
    )


def local(n, groups, hidden, norm_gain, w_query, w_key, w_value, bias_query, bias_key, bias_value, w_out):
    rows, width = hidden.shape
    if fits_pair(n, groups, rows, w_query, w_out):
        return pair_local(n, hidden, norm_gain, w_query, w_key, w_value, bias_query, bias_key, bias_value, w_out)
    cols = w_query.shape[1]
    heads = cols // HEAD_DIM
    wide = cols + 2 * HEAD_DIM
    chips = n // 2
    exchange = groups > 1 and (rows // groups) % 16 == 0
    rh = rows // groups
    slices = 2 * n
    half_depth = w_query.shape[0] // 2
    half_cols = w_out.shape[1] // 2

    tables = tables_of(n, rows)
    vectors = [v.reshape(1, -1) for v in (norm_gain, bias_query, bias_key, bias_value)]

    any_spec = pl.BlockSpec(memory_space=pl.ANY)
    vmem = pl.BlockSpec(memory_space=pltpu.VMEM)
    links = max(groups - 1, 1) if exchange else 1
    pieces = slices if exchange else 1
    rpart = rh if exchange else 16
    dma = pltpu.SemaphoreType.DMA
    result = pl.pallas_call(
        functools.partial(kernel, n, groups, exchange),
        out_shape=jax.ShapeDtypeStruct((rh if exchange else rows, w_out.shape[1] * n), BF16),
        in_specs=[any_spec] * 5 + [vmem] * 8,
        out_specs=vmem,
        scratch_shapes=[
            pltpu.VMEM((rows, width), BF16),
            pltpu.VMEM((slices, half_depth, wide), BF16),
            pltpu.VMEM((slices, w_out.shape[0], half_cols), BF16),
            pltpu.VMEM((rows, wide), F32),
            pltpu.VMEM((chips, 2 * rows, 2 * HEAD_DIM), BF16),
            pltpu.VMEM((heads, rows, HEAD_DIM), BF16),
            pltpu.VMEM((heads, rows, 1), F32),
            pltpu.VMEM((heads, rows, 1), F32),
            pltpu.VMEM((heads, rows, HEAD_DIM), F32),
            pltpu.VMEM((rows, cols), BF16),
            pltpu.VMEM((links, pieces, rpart, half_cols), BF16),
            pltpu.VMEM((links, pieces, rpart, half_cols), BF16),
            pltpu.VMEM((pieces, rpart, half_cols), BF16),
            dma((9,)),
        ]
        + [dma((4 * chips,))] * 12
        + [dma((links * pieces,))] * 2,
        compiler_params=pltpu.CompilerParams(
            collective_id=0, has_side_effects=True, vmem_limit_bytes=64 * 1024 * 1024 - 128 * 1024
        ),
    )(hidden, w_query, w_key, w_value, w_out, *vectors, *tables)
    if exchange:
        return result
    return lax.psum_scatter(result, "head", scatter_dimension=0, tiled=True)


def solution(mesh):
    in_specs = (
        P("seq", None),
        P(),
        P("seq", "head"),
        P("seq", "head"),
        P("seq", "head"),
        P("head"),
        P("head"),
        P("head"),
        P("head", "seq"),
    )
    out_specs = P(("seq", "head"), None)
    body = functools.partial(local, mesh.shape["seq"], mesh.shape["head"])
    return jax.shard_map(body, mesh=mesh, in_specs=in_specs, out_specs=out_specs, check_vma=False)
```

```python
import functools

import jax
import jax.numpy as jnp
import numpy as np
from jax import lax
from jax.experimental import pallas as pl
from jax.experimental.pallas import tpu as pltpu
from jax.sharding import PartitionSpec as P

HEAD_DIM = 128
ROPE_BASE = 1000000.0
EPSILON = 1e-06
MESH = pl.DeviceIdType.MESH
F32 = jnp.float32
BF16 = jnp.bfloat16
OPS = (1, 0, 0, 1, 1, 8)
PIECES = (4, 2, 4, 2)
VMEM_LIMIT = 64 * 1024 * 1024 - 4096 * 1024


def kernel(
    n, groups, exchange,
    hidden, w_query, w_key, w_value, w_out, gain, bias_query, bias_key, bias_value,
    near_cos, near_sin, far_cos, far_sin,
    out,
    hid, w_all, wo_all, acc, kv_all, q_ref, high, total, mixed, att, ts, tr, tm,
    load_sem, ws, wr, wps, wpr, os_, or_, ops, opr, ks, kr, kps, kpr, ys, yr,
):
    chips = n // 2
    depth = chips // 2
    me = lax.axis_index("seq")
    group = lax.axis_index("head")
    core = me % 2
    chip = me // 2
    ring = chip // 2 + (chip % 2) * (2 * depth - 1 - 2 * (chip // 2))

    def device_at(position, which):
        position = (position + 2 * chips) % chips
        side = position // depth
        row = position + side * (2 * depth - 1 - 2 * position)
        return 2 * (2 * row + side) + which

    right = device_at(ring + 1, core)
    left = device_at(ring - 1, core)
    partner = 2 * chip + (1 - core)
    neighbours = (right, left)

    def source_at(direction, offset, which):
        return device_at(ring - offset if direction == 0 else ring + offset, which)

    rows, width = hidden.shape
    half_depth = w_query.shape[0] // 2
    q_cols = w_query.shape[1]
    heads = q_cols // HEAD_DIM
    half_cols = w_out.shape[1] // 2
    rh = rows // groups

    loads = []
    late = [pltpu.make_async_copy(hidden, hid, load_sem.at[0])]
    for h in range(2):
        span = pl.ds(h * half_depth, half_depth)
        slot = w_all.at[2 * me + h]
        loads.append(pltpu.make_async_copy(w_query.at[span], slot.at[:, pl.ds(0, q_cols)], load_sem.at[1 + 4 * h]))
        loads.append(pltpu.make_async_copy(w_key.at[span], slot.at[:, pl.ds(q_cols, HEAD_DIM)], load_sem.at[2 + 4 * h]))
        loads.append(pltpu.make_async_copy(w_value.at[span], slot.at[:, pl.ds(q_cols + HEAD_DIM, HEAD_DIM)], load_sem.at[3 + 4 * h]))
        late.append(pltpu.make_async_copy(w_out.at[:, pl.ds(h * half_cols, half_cols)], wo_all.at[2 * me + h], load_sem.at[4 + 4 * h]))
    for copy in loads + late:
        copy.start()

    barrier = pltpu.get_barrier_semaphore()
    for device in (right, left, partner):
        pl.semaphore_signal(barrier, inc=1, device_id={"seq": device}, device_id_type=MESH)
    peers = range(1, groups) if exchange else ()
    for p in peers:
        pl.semaphore_signal(barrier, inc=1, device_id={"head": (group + p) % groups}, device_id_type=MESH)
    pl.semaphore_wait(barrier, 3 + len(peers))

    def remote(ref, send, recv, key, device):
        return pltpu.make_async_remote_copy(
            src_ref=ref, dst_ref=ref, send_sem=send.at[key], recv_sem=recv.at[key],
            device_id={"seq": device}, device_id_type=MESH,
        )

    def piece(buffer, index, j):
        size = buffer.shape[1] // 2
        return buffer.at[index, pl.ds(j * size, size)]

    def key_of(direction, step, j):
        return (direction * chips + step) * 2 + j

    def ring_begin(buffer, sems):
        ss, rs, pss, prs = sems
        for j in range(2):
            for d in range(2):
                own = piece(buffer, 2 * me + d, j)
                remote(own, ss, rs, key_of(d, 0, j), neighbours[d]).start()
        for j in range(2):
            for d in range(2):
                own = piece(buffer, 2 * me + d, j)
                remote(own, pss, prs, key_of(d, chips - 1, j), partner).start()

    def ring_advance(buffer, sems, t):
        ss, rs, pss, prs = sems

        @pl.when(t < chips - 1)
        def _():
            for j in range(2):
                for d in range(2):
                    block = piece(buffer, 2 * source_at(d, t + 1, core) + d, j)
                    remote(block, ss, rs, key_of(d, t, j), neighbours[d]).wait_recv()

                    @pl.when(t < chips - 2)
                    def _():
                        remote(block, ss, rs, key_of(d, t + 1, j), neighbours[d]).start()

                    remote(block, pss, prs, key_of(d, t, j), partner).start()

    def partner_wait(buffer, sems, t):
        ss, rs, pss, prs = sems
        for j in range(2):
            for d in range(2):
                block = piece(buffer, 2 * source_at(d, t, 1 - core) + d, j)
                remote(block, pss, prs, key_of(d, (t + chips - 1) % chips, j), partner).wait_recv()

    def ring_drain(buffer, sems):
        ss, rs, pss, prs = sems

        def body(t, carry):
            for j in range(2):
                for d in range(2):
                    block = piece(buffer, 2 * me + d, j)

                    @pl.when(t < chips - 1)
                    def _():
                        remote(block, ss, rs, key_of(d, t, j), neighbours[d]).wait_send()

                    remote(block, pss, prs, key_of(d, t, j), partner).wait_send()
            return carry

        lax.fori_loop(0, chips, body, 0)

    w_sems = (ws, wr, wps, wpr)
    o_sems = (os_, or_, ops, opr)

    for copy in loads:
        copy.wait()
    ring_begin(w_all, w_sems)
    for copy in late:
        copy.wait()
    slices = 2 * n
    step_cols = width // slices

    def columns(i):
        return pl.ds(pl.multiple_of(i * step_cols, step_cols), step_cols)

    def square(i, carry):
        x = hid[:, columns(i)].astype(F32)
        return carry + x * x

    squares = lax.fori_loop(0, slices, square, jnp.zeros((rows, step_cols), F32))
    inverse = lax.rsqrt(jnp.sum(squares, axis=-1, keepdims=True) * (1.0 / width) + EPSILON)

    def normed(i):
        scaled = hid[:, columns(i)].astype(F32) * inverse * gain[:, columns(i)].astype(F32)
        return scaled.astype(BF16)

    bias = (bias_query, bias_key, bias_value)
    starts = (0, q_cols, q_cols + HEAD_DIM)
    for start, part in zip(starts, bias):
        span = pl.ds(start, part.shape[1])
        acc[:, span] = jnp.broadcast_to(part[...].astype(F32), (rows, part.shape[1]))

    def project(t, carry):
        ring_advance(w_all, w_sems, t)
        partner_wait(w_all, w_sems, t)
        for d in range(2):
            i = 2 * source_at(d, t, core) + d
            k = 2 * source_at(d, t, 1 - core) + d
            acc[...] += jnp.dot(normed(i), w_all[i], preferred_element_type=F32) + jnp.dot(
                normed(k), w_all[k], preferred_element_type=F32
            )
        return carry

    lax.fori_loop(0, chips, project, 0)

    block_cos, block_sin = far_cos[me], far_sin[me]
    cosine = near_cos[...] * block_cos - near_sin[...] * block_sin
    lane = lax.broadcasted_iota(jnp.int32, cosine.shape, 1)
    sine = near_sin[...] * block_cos + near_cos[...] * block_sin
    sine = jnp.where(lane < HEAD_DIM // 2, -sine, sine)

    def rotary(x):
        return x * cosine + pltpu.roll(x, HEAD_DIM // 2, 1) * sine

    def kv_rows(which):
        return pl.ds(pl.multiple_of(which * rows, rows), rows)

    kv_all[chip, kv_rows(core), pl.ds(0, HEAD_DIM)] = rotary(acc[:, pl.ds(q_cols, HEAD_DIM)]).astype(BF16)
    kv_all[chip, kv_rows(core), pl.ds(HEAD_DIM, HEAD_DIM)] = acc[:, pl.ds(q_cols + HEAD_DIM, HEAD_DIM)].astype(BF16)
    for h in range(heads):
        q_ref[h] = rotary(acc[:, pl.ds(h * HEAD_DIM, HEAD_DIM)]).astype(BF16)

    reach = (chips // 2, chips - 1 - chips // 2)

    parts = 2 if rows % 32 == 0 else 1
    piece_rows = rows // parts

    def kv_copy(owner, ss, rs, direction, step, j, device):
        start = pl.multiple_of((owner % 2) * rows + j * piece_rows, piece_rows)
        block = kv_all.at[owner // 2, pl.ds(start, piece_rows)]
        return remote(block, ss, rs, key_of(direction, step, j), device)

    for j in range(parts):
        for d in range(2):
            kv_copy(me, ks, kr, d, 0, j, neighbours[d]).start()
        kv_copy(me, kps, kpr, 0, chips - 1, j, partner).start()

    factor = HEAD_DIM ** (-0.5) * 1.4426950408889634

    def attend(c, own):
        for h in range(heads):
            scores = lax.dot_general(
                q_ref[h], kv_all[c, :, pl.ds(0, HEAD_DIM)], (((1,), (1,)), ((), ())),
                preferred_element_type=F32,
            )
            if own:
                row = lax.broadcasted_iota(jnp.int32, scores.shape, 0) + core * rows
                col = lax.broadcasted_iota(jnp.int32, scores.shape, 1)
                scores = jnp.where(row >= col, scores, -jnp.inf)
            top = jnp.max(scores, axis=-1, keepdims=True)
            if not own:
                old = high[h]
                top = jnp.maximum(old, top)
            probs = jnp.exp2((scores - top) * factor)
            part = jnp.sum(probs, axis=-1, keepdims=True)
            product = jnp.dot(
                probs.astype(BF16), kv_all[c, :, pl.ds(HEAD_DIM, HEAD_DIM)], preferred_element_type=F32
            )
            if not own:
                shrink = jnp.exp2((old - top) * factor)
                part = part + total[h] * shrink
                product = product + mixed[h] * shrink
            high[h] = top
            total[h] = part
            mixed[h] = product

    for j in range(parts):
        kv_copy(partner, kps, kpr, 0, chips - 1, j, partner).wait_recv()
    attend(chip, True)

    def attention(t, carry):
        for j in range(parts):
            for d in range(2):
                @pl.when(t < reach[d])
                def _():
                    owner = source_at(d, t + 1, core)
                    kv_copy(owner, ks, kr, d, t, j, neighbours[d]).wait_recv()

                    @pl.when(t + 1 < reach[d])
                    def _():
                        kv_copy(owner, ks, kr, d, t + 1, j, neighbours[d]).start()

                    kv_copy(owner, kps, kpr, d, t, j, partner).start()

        @pl.when(t == reach[0] - 1)
        def _():
            ring_begin(wo_all, o_sems)

        for d in range(2):
            @pl.when((t > 0) & (t <= reach[d]))
            def _():
                owner = source_at(d, t, 1 - core)
                for j in range(parts):
                    kv_copy(owner, kps, kpr, d, t - 1, j, partner).wait_recv()

                @pl.when(owner // 2 < chip)
                def _():
                    attend(owner // 2, False)
        return carry

    lax.fori_loop(0, reach[0] + 1, attention, 0)
    for h in range(heads):
        att[:, pl.ds(h * HEAD_DIM, HEAD_DIM)] = (mixed[h] / total[h]).astype(BF16)

    def term_copy(p, i):
        return pltpu.make_async_remote_copy(
            src_ref=ts.at[p - 1, i], dst_ref=tr.at[p - 1, i],
            send_sem=ys.at[(p - 1) * slices + i], recv_sem=yr.at[(p - 1) * slices + i],
            device_id={"head": (group + p) % groups}, device_id_type=MESH,
        )

    def out_columns(i):
        return pl.ds(pl.multiple_of(i * half_cols, half_cols), half_cols)

    def make_term(i):
        if not exchange:
            out[:, out_columns(i)] = jnp.dot(att[...], wo_all[i], preferred_element_type=F32).astype(BF16)
            return
        for p in peers:
            span = pl.ds(pl.multiple_of(((group + p) % groups) * rh, rh), rh)
            ts[p - 1, i] = jnp.dot(att[span, :], wo_all[i], preferred_element_type=F32).astype(BF16)
            term_copy(p, i).start()
        span = pl.ds(pl.multiple_of(group * rh, rh), rh)
        tm[i] = jnp.dot(att[span, :], wo_all[i], preferred_element_type=F32).astype(BF16)

    def blocks_of(t):
        return [2 * source_at(d, t, which) + d for d in range(2) for which in (core, 1 - core)]

    def finish(t, carry):
        for i in blocks_of(t):
            value = tm[i].astype(F32)
            for p in peers:
                term_copy(p, i).wait_recv()
                value = value + tr[p - 1, i].astype(F32)
            out[:, out_columns(i)] = value.astype(BF16)
        return carry

    lag = 3

    def partner_terms(t):
        partner_wait(wo_all, o_sems, t)
        for d in range(2):
            make_term(2 * source_at(d, t, 1 - core) + d)

    for d in range(2):
        make_term(2 * me + d)
    partner_terms(0)

    def project_out(t, carry):
        ring_advance(wo_all, o_sems, t)

        @pl.when(t < chips - 1)
        def _():
            for d in range(2):
                make_term(2 * source_at(d, t + 1, core) + d)

        @pl.when(t > 0)
        def _():
            partner_terms(t)

        if exchange:
            @pl.when(t >= lag)
            def _():
                finish(t - lag, 0)
        return carry

    lax.fori_loop(0, chips, project_out, 0)

    if exchange:
        lax.fori_loop(chips - lag, chips, finish, 0)

        def sent(i, carry):
            for p in peers:
                term_copy(p, i).wait_send()
            return carry

        lax.fori_loop(0, slices, sent, 0)

    ring_drain(w_all, w_sems)
    ring_drain(wo_all, o_sems)
    for j in range(parts):
        for d in range(2):
            for t in range(reach[d]):
                kv_copy(me, ks, kr, d, t, j, neighbours[d]).wait_send()
                kv_copy(me, kps, kpr, d, t, j, partner).wait_send()
        kv_copy(me, kps, kpr, 0, chips - 1, j, partner).wait_send()


def pair_kernel(
    n, chunks_wide, chunks_narrow, chunks_out,
    hidden, w_query, w_key, w_value, w_out, *rest_refs,
):
    small = rest_refs[:8]
    out = rest_refs[8]
    held = rest_refs[9:17]
    gain, bias_query, bias_key, bias_value, near_cos, near_sin, far_cos, far_sin = held
    (
    gains, small_sem, hid, w_first, w_second, wo, acc_first, acc_second, kv_all, q_ref, high, total, mixed, att, terms,
    load_sem, swap_s, swap_r, att_s, att_r, own_s, ys, yr,
    fs, fr, fps, fpr, ss, sr, sps, spr, os_, or_, ops, opr, ks, kr, kps, kpr,
    ) = rest_refs[17:]
    chips = n // 2
    depth = chips // 2
    ops_from, ops_first, ops_busy, ops_calm, ops_gap, ops_rest = OPS
    me = lax.axis_index("seq")
    group = lax.axis_index("head")
    peer = 1 - group
    core = me % 2
    chip = me // 2
    ring = chip // 2 + (chip % 2) * (2 * depth - 1 - 2 * (chip // 2))

    def device_at(position, which):
        position = (position + 2 * chips) % chips
        side = position // depth
        row = position + side * (2 * depth - 1 - 2 * position)
        return 2 * (2 * row + side) + which

    right = device_at(ring + 1, core)
    left = device_at(ring - 1, core)
    partner = 2 * chip + (1 - core)
    neighbours = (right, left)

    def source_at(direction, offset, which):
        return device_at(ring - offset if direction == 0 else ring + offset, which)

    rows, width = hidden.shape
    half_depth = w_query.shape[0] // 2
    q_cols = w_query.shape[1]
    heads = q_cols // HEAD_DIM
    early = heads // 2
    q_early = early * HEAD_DIM
    q_late = q_cols - q_early
    out_depth = w_out.shape[0]
    group_cols = w_out.shape[1] // 2
    lane_cols = group_cols // 2
    rh = rows // 2

    def remote(ref, send, recv, key, device):
        return pltpu.make_async_remote_copy(
            src_ref=ref, dst_ref=ref, send_sem=send.at[key], recv_sem=recv.at[key],
            device_id={"seq": device}, device_id_type=MESH,
        )

    def lanes(which):
        return pl.ds(pl.multiple_of(which * lane_cols, lane_cols), lane_cols)

    def wo_lanes(which, d):
        start = which * group_cols + d * lane_cols
        return pl.ds(pl.multiple_of(start, lane_cols), lane_cols)

    def group_rows(which):
        return pl.ds(pl.multiple_of(which * out_depth, out_depth), out_depth)

    loads, later, last = [], [], []
    for h in range(2):
        span = pl.ds(h * half_depth, half_depth)
        slot = w_first.at[2 * me + h]
        loads.append((w_key.at[span], slot.at[:, pl.ds(0, HEAD_DIM)]))
        loads.append((w_value.at[span], slot.at[:, pl.ds(HEAD_DIM, HEAD_DIM)]))
        loads.append((w_query.at[span, pl.ds(0, q_early)], slot.at[:, pl.ds(2 * HEAD_DIM, q_early)]))
        later.append((w_query.at[span, pl.ds(q_early, q_late)], w_second.at[2 * me + h]))
        last.append((w_out.at[:, wo_lanes(group, h)], wo.at[chip, h, group_rows(group), lanes(core)]))
    later.append((hidden, hid))
    copies = [pltpu.make_async_copy(a, b, load_sem.at[i]) for i, (a, b) in enumerate(loads + later + last)]
    small_copies = [pltpu.make_async_copy(a, b, small_sem.at[i]) for i, (a, b) in enumerate(zip(small, held))]
    for copy in copies[: len(loads)]:
        copy.start()

    barrier = pltpu.get_barrier_semaphore()
    for device in (right, left, partner):
        pl.semaphore_signal(barrier, inc=1, device_id={"seq": device}, device_id_type=MESH)
    pl.semaphore_signal(barrier, inc=1, device_id={"head": peer}, device_id_type=MESH)
    pl.semaphore_wait(barrier, 4)

    def across(src, dst, send, recv, key):
        return pltpu.make_async_remote_copy(
            src_ref=src, dst_ref=dst, send_sem=send.at[key], recv_sem=recv.at[key],
            device_id={"head": peer}, device_id_type=MESH,
        )

    def swap(d):
        return across(
            w_out.at[:, wo_lanes(peer, d)], wo.at[chip, d, group_rows(group), lanes(core)], swap_s, swap_r, d
        )

    class Ring:
        def __init__(self, view, sems, pieces):
            self.view, self.sems, self.pieces = view, sems, pieces

        def key(self, d, step, j):
            return (d * chips + step) * self.pieces + j

        def begin(self, j):
            send, recv, psend, precv = self.sems
            for d in range(2):
                own = self.view(me, d, j)
                remote(own, send, recv, self.key(d, 0, j), neighbours[d]).start()
            for d in range(2):
                own = self.view(me, d, j)
                remote(own, psend, precv, self.key(d, chips - 1, j), partner).start()

        def advance(self, t, j):
            send, recv, psend, precv = self.sems
            for d in range(2):
                block = self.view(source_at(d, t + 1, core), d, j)
                remote(block, send, recv, self.key(d, t, j), neighbours[d]).wait_recv()

                @pl.when(t < chips - 2)
                def _():
                    remote(block, send, recv, self.key(d, t + 1, j), neighbours[d]).start()

                remote(block, psend, precv, self.key(d, t, j), partner).start()

        def op(self, index):
            @pl.when(index < self.pieces)
            def _():
                self.begin(index)

            @pl.when((index >= self.pieces) & (index < self.pieces * chips))
            def _():
                done = index - self.pieces
                self.advance(done // self.pieces, done % self.pieces)

        def partner_wait(self, t):
            send, recv, psend, precv = self.sems
            for j in range(self.pieces):
                for d in range(2):
                    block = self.view(source_at(d, t, 1 - core), d, j)
                    remote(block, psend, precv, self.key(d, (t + chips - 1) % chips, j), partner).wait_recv()

        def drain(self):
            send, recv, psend, precv = self.sems

            def body(t, carry):
                for j in range(self.pieces):
                    for d in range(2):
                        block = self.view(me, d, j)

                        @pl.when(t < chips - 1)
                        def _():
                            remote(block, send, recv, self.key(d, t, j), neighbours[d]).wait_send()

                        remote(block, psend, precv, self.key(d, t, j), partner).wait_send()
                return carry

            lax.fori_loop(0, chips, body, 0)

    def rows_view(buffer, pieces):
        size = buffer.shape[1] // pieces
        return lambda owner, d, j: buffer.at[2 * owner + d, pl.ds(pl.multiple_of(j * size, size), size)]

    def wo_view(owner, d, j):
        size = wo.shape[2] // chunks_out
        return wo.at[owner // 2, d, pl.ds(pl.multiple_of(j * size, size), size), lanes(owner % 2)]

    first = Ring(rows_view(w_first, chunks_wide), (fs, fr, fps, fpr), chunks_wide)
    second = Ring(rows_view(w_second, chunks_narrow), (ss, sr, sps, spr), chunks_narrow)
    third = Ring(wo_view, (os_, or_, ops, opr), chunks_out)

    for copy in copies[: len(loads)]:
        copy.wait()
    for j in range(chunks_wide):
        first.begin(j)
    for d in range(2):
        swap(d).start()
    for copy in copies[len(loads):] + small_copies:
        copy.start()
    for copy in copies[len(loads):]:
        copy.wait()

    for copy in small_copies:
        copy.wait()
    gains[...] = gain[...].astype(F32)

    slices = 2 * n
    step_cols = width // slices
    gain_rows = step_cols // HEAD_DIM

    def columns(i):
        return pl.ds(pl.multiple_of(i * step_cols, step_cols), step_cols)

    def square(i, carry):
        x = hid[:, columns(i)].astype(F32)
        return carry + x * x

    squares = lax.fori_loop(0, slices, square, jnp.zeros((rows, step_cols), F32))
    inverse = lax.rsqrt(jnp.sum(squares, axis=-1, keepdims=True) * (1.0 / width) + EPSILON)

    def normed(i):
        line = jnp.concatenate([gains[pl.ds(i * gain_rows + r, 1), :] for r in range(gain_rows)], axis=1)
        scaled = hid[:, columns(i)].astype(F32) * inverse * line
        value = scaled.astype(BF16)
        hid[:, columns(i)] = value
        return value

    def widen(line):
        return jnp.broadcast_to(line.astype(F32), (rows, HEAD_DIM))

    acc_first[:, pl.ds(0, HEAD_DIM)] = widen(bias_key[...])
    acc_first[:, pl.ds(HEAD_DIM, HEAD_DIM)] = widen(bias_value[...])
    lines = bias_query[...].astype(F32)
    for h in range(early):
        acc_first[:, pl.ds((2 + h) * HEAD_DIM, HEAD_DIM)] = widen(lines[h : h + 1])
    for h in range(early, heads):
        acc_second[:, pl.ds((h - early) * HEAD_DIM, HEAD_DIM)] = widen(lines[h : h + 1])

    def project_first(t, carry):
        @pl.when(t < chips - 1)
        def _():
            for j in range(chunks_wide):
                first.advance(t, j)

        @pl.when(t == chips - 3)
        def _():
            for j in range(chunks_narrow):
                second.begin(j)

        @pl.when(t == ops_from)
        def _():
            for d in range(2):
                swap(d).wait_recv()

        @pl.when((t >= ops_from) & (t < ops_from + ops_first))
        def _():
            third.op(t - ops_from)

        @pl.when(t == chips - 1)
        def _():
            for j in range(chunks_narrow):
                second.advance(0, j)

        first.partner_wait(t)
        for d in range(2):
            i = 2 * source_at(d, t, core) + d
            k = 2 * source_at(d, t, 1 - core) + d
            acc_first[...] += jnp.dot(normed(i), w_first[i], preferred_element_type=F32) + jnp.dot(
                normed(k), w_first[k], preferred_element_type=F32
            )
        return carry

    lax.fori_loop(0, chips, project_first, 0)

    block_cos, block_sin = far_cos[me], far_sin[me]
    cosine = near_cos[...] * block_cos - near_sin[...] * block_sin
    lane = lax.broadcasted_iota(jnp.int32, cosine.shape, 1)
    sine = near_sin[...] * block_cos + near_cos[...] * block_sin
    sine = jnp.where(lane < HEAD_DIM // 2, -sine, sine)

    def rotary(x):
        return x * cosine + pltpu.roll(x, HEAD_DIM // 2, 1) * sine

    def kv_rows(which):
        return pl.ds(pl.multiple_of(which * rows, rows), rows)

    kv_all[chip, kv_rows(core), pl.ds(0, HEAD_DIM)] = rotary(acc_first[:, pl.ds(0, HEAD_DIM)]).astype(BF16)
    kv_all[chip, kv_rows(core), pl.ds(HEAD_DIM, HEAD_DIM)] = acc_first[:, pl.ds(HEAD_DIM, HEAD_DIM)].astype(BF16)
    for h in range(early):
        q_ref[h] = rotary(acc_first[:, pl.ds((2 + h) * HEAD_DIM, HEAD_DIM)]).astype(BF16)

    reach = (chips // 2, chips - 1 - chips // 2)
    parts = PIECES[3]
    piece_rows = rows // parts

    def kv_copy(owner, send, recv, direction, step, j, device):
        start = pl.multiple_of((owner % 2) * rows + j * piece_rows, piece_rows)
        block = kv_all.at[owner // 2, pl.ds(start, piece_rows)]
        return remote(block, send, recv, (direction * chips + step) * parts + j, device)

    for j in range(parts):
        for d in range(2):
            kv_copy(me, ks, kr, d, 0, j, neighbours[d]).start()
        kv_copy(me, kps, kpr, 0, chips - 1, j, partner).start()

    factor = HEAD_DIM ** (-0.5) * 1.4426950408889634

    def attend(c, own, which):
        for h in which:
            scores = lax.dot_general(
                q_ref[h], kv_all[c, :, pl.ds(0, HEAD_DIM)], (((1,), (1,)), ((), ())),
                preferred_element_type=F32,
            )
            if own:
                row = lax.broadcasted_iota(jnp.int32, scores.shape, 0) + core * rows
                col = lax.broadcasted_iota(jnp.int32, scores.shape, 1)
                scores = jnp.where(row >= col, scores, -jnp.inf)
            top = jnp.max(scores, axis=-1, keepdims=True)
            if not own:
                old = high[h]
                top = jnp.maximum(old, top)
            probs = jnp.exp2((scores - top) * factor)
            part = jnp.sum(probs, axis=-1, keepdims=True)
            product = jnp.dot(
                probs.astype(BF16), kv_all[c, :, pl.ds(HEAD_DIM, HEAD_DIM)], preferred_element_type=F32
            )
            if not own:
                shrink = jnp.exp2((old - top) * factor)
                part = part + total[h] * shrink
                product = product + mixed[h] * shrink
            high[h] = top
            total[h] = part
            mixed[h] = product

    sooner, rest = range(early), range(early, heads)
    for j in range(parts):
        kv_copy(partner, kps, kpr, 0, chips - 1, j, partner).wait_recv()
    attend(chip, True, sooner)

    def attention(t, carry):
        for j in range(parts):
            for d in range(2):
                @pl.when(t < reach[d])
                def _():
                    owner = source_at(d, t + 1, core)
                    kv_copy(owner, ks, kr, d, t, j, neighbours[d]).wait_recv()

                    @pl.when(t + 1 < reach[d])
                    def _():
                        kv_copy(owner, ks, kr, d, t + 1, j, neighbours[d]).start()

                    kv_copy(owner, kps, kpr, d, t, j, partner).start()

        @pl.when(t + 1 < chips - 1)
        def _():
            for j in range(chunks_narrow):
                second.advance(t + 1, j)

        busy = reach[0] - 1
        for k in range(max(ops_busy, ops_calm)):
            index = ops_first + ops_busy * jnp.minimum(t, busy) + ops_calm * jnp.maximum(t - busy, 0) + k

            @pl.when(((t < busy) & (k < ops_busy)) | ((t >= busy) & (k < ops_calm)))
            def _():
                third.op(index)

        for d in range(2):
            @pl.when((t > 0) & (t <= reach[d]))
            def _():
                owner = source_at(d, t, 1 - core)
                for j in range(parts):
                    kv_copy(owner, kps, kpr, d, t - 1, j, partner).wait_recv()

                @pl.when(owner // 2 < chip)
                def _():
                    attend(owner // 2, False, sooner)

        second.partner_wait(t)
        for d in range(2):
            i = 2 * source_at(d, t, core) + d
            k = 2 * source_at(d, t, 1 - core) + d
            acc_second[...] += jnp.dot(hid[:, columns(i)], w_second[i], preferred_element_type=F32) + jnp.dot(
                hid[:, columns(k)], w_second[k], preferred_element_type=F32
            )
        return carry

    lax.fori_loop(0, chips, attention, 0)

    def head_span(which):
        return pl.ds(which[0] * HEAD_DIM, len(which) * HEAD_DIM)

    def att_copy(key, which):
        ref = att.at[group, :, head_span(which)]
        return across(ref, ref, att_s, att_r, key)

    def settle(which):
        for h in which:
            att[group, :, pl.ds(h * HEAD_DIM, HEAD_DIM)] = (mixed[h] / total[h]).astype(BF16)

    settle(sooner)
    for h in rest:
        q_ref[h] = rotary(acc_second[:, pl.ds((h - early) * HEAD_DIM, HEAD_DIM)]).astype(BF16)
    att_copy(0, sooner).start()
    attend(chip, True, rest)

    ops_middle = ops_first + ops_busy * (reach[0] - 1) + ops_calm * (chips + 1 - reach[0])
    ops_done = ops_middle + ops_rest

    def attention_rest(c, carry):
        @pl.when((c % ops_gap == 0) & (c // ops_gap < ops_rest))
        def _():
            third.op(ops_middle + c // ops_gap)

        @pl.when(c < chip)
        def _():
            attend(c, False, rest)
        return carry

    lax.fori_loop(0, chips, attention_rest, 0)
    settle(rest)
    att_copy(1, rest).start()

    def out_copy(c, d, which, key):
        start = (2 * c + which) * 2 * group_cols + group * group_cols + d * lane_cols
        span = pl.ds(pl.multiple_of(start, lane_cols), lane_cols)
        src = terms.at[c, d, pl.ds(pl.multiple_of(group * rh, rh), rh), lanes(which)]
        return pltpu.make_async_copy(src, out.at[:, span], own_s.at[key])

    def peer_copy(c, d, which, key):
        start = (2 * c + which) * 2 * group_cols + group * group_cols + d * lane_cols
        span = pl.ds(pl.multiple_of(start, lane_cols), lane_cols)
        src = terms.at[c, d, pl.ds(pl.multiple_of(peer * rh, rh), rh), lanes(which)]
        return across(src, out.at[:, span], ys, yr, key)

    def chip_keys(c, d):
        return [(which, (2 * c + d) * 2 + which) for which in range(2)]

    def make_term(t, d):
        c = source_at(d, t, core) // 2
        value = None
        for g in range(2):
            depth_rows = pl.ds(g * out_depth, out_depth)
            term = jnp.dot(att[g], wo[c, d, depth_rows, :], preferred_element_type=F32).astype(BF16).astype(F32)
            value = term if value is None else value + term
        terms[c, d] = value.astype(BF16)
        for which, key in chip_keys(c, d):
            peer_copy(c, d, which, key).start()
            out_copy(c, d, which, key).start()

    att_copy(0, sooner).wait_recv()
    att_copy(1, rest).wait_recv()

    def project_out(t, carry):
        third.partner_wait(t)
        for j in range(chunks_out):
            @pl.when(((t + 1) * chunks_out + j >= ops_done) & (t < chips - 1))
            def _():
                third.advance(t, j)

            if j < 2:
                make_term(t, j)
        return carry

    lax.fori_loop(0, chips, project_out, 0)

    first.drain()
    second.drain()
    third.drain()
    for j in range(parts):
        for d in range(2):
            for t in range(reach[d]):
                kv_copy(me, ks, kr, d, t, j, neighbours[d]).wait_send()
                kv_copy(me, kps, kpr, d, t, j, partner).wait_send()
        kv_copy(me, kps, kpr, 0, chips - 1, j, partner).wait_send()
    for d in range(2):
        swap(d).wait_send()
    att_copy(0, sooner).wait_send()
    att_copy(1, rest).wait_send()

    def finish(c, carry):
        for d in range(2):
            for which, key in chip_keys(c, d):
                peer_copy(c, d, which, key).wait_send()
                out_copy(c, d, which, key).wait()
                peer_copy(c, d, which, key).wait_recv()
        return carry

    lax.fori_loop(0, chips, finish, 0)


def tables_of(n, rows):
    freq = ROPE_BASE ** (-2.0 * np.arange(HEAD_DIM // 2, dtype=np.float64) / HEAD_DIM)
    freq = np.concatenate([freq, freq])
    near = np.arange(rows, dtype=np.float64)[:, None] * freq
    far = (np.arange(n, dtype=np.float64) * rows)[:, None, None] * freq
    return [f(a).astype(np.float32) for a in (near, far) for f in (np.cos, np.sin)]


def pair_local(n, hidden, norm_gain, w_query, w_key, w_value, bias_query, bias_key, bias_value, w_out):
    rows, width = hidden.shape
    cols = w_query.shape[1]
    heads = cols // HEAD_DIM
    early = heads // 2 * HEAD_DIM
    chips = n // 2
    slices = 2 * n
    half_depth = w_query.shape[0] // 2
    group_cols = w_out.shape[1] // 2
    wide, narrow, fine, parts = PIECES
    vectors = [v.reshape(-1, HEAD_DIM) for v in (norm_gain, bias_query, bias_key, bias_value)]
    small = vectors + tables_of(n, rows)
    result = jax.ShapeDtypeStruct((rows // 2, w_out.shape[1] * n), BF16)
    any_spec = pl.BlockSpec(memory_space=pl.ANY)
    dma = pltpu.SemaphoreType.DMA
    return pl.pallas_call(
        functools.partial(pair_kernel, n, wide, narrow, fine),
        out_shape=pltpu.VMEM(result.shape, result.dtype),
        in_specs=[any_spec] * 13,
        out_specs=pl.BlockSpec(memory_space=pltpu.VMEM),
        scratch_shapes=[pltpu.VMEM(a.shape, a.dtype) for a in small]
        + [
            pltpu.VMEM((width // HEAD_DIM, HEAD_DIM), F32),
            dma((8,)),
            pltpu.VMEM((rows, width), BF16),
            pltpu.VMEM((slices, half_depth, 2 * HEAD_DIM + early), BF16),
            pltpu.VMEM((slices, half_depth, cols - early), BF16),
            pltpu.VMEM((chips, 2, 2 * w_out.shape[0], group_cols), BF16),
            pltpu.VMEM((rows, 2 * HEAD_DIM + early), F32),
            pltpu.VMEM((rows, cols - early), F32),
            pltpu.VMEM((chips, 2 * rows, 2 * HEAD_DIM), BF16),
            pltpu.VMEM((heads, rows, HEAD_DIM), BF16),
            pltpu.VMEM((heads, rows, 1), F32),
            pltpu.VMEM((heads, rows, 1), F32),
            pltpu.VMEM((heads, rows, HEAD_DIM), F32),
            pltpu.VMEM((2, rows, cols), BF16),
            pltpu.VMEM((chips, 2, rows, group_cols), BF16),
            dma((11,)),
            dma((2,)), dma((2,)), dma((2,)), dma((2,)),
            dma((4 * chips,)), dma((4 * chips,)), dma((4 * chips,)),
        ]
        + [dma((2 * chips * wide,))] * 4
        + [dma((2 * chips * narrow,))] * 4
        + [dma((2 * chips * fine,))] * 4
        + [dma((4 * chips,))] * 4,
        compiler_params=pltpu.CompilerParams(
            collective_id=0, has_side_effects=True, vmem_limit_bytes=VMEM_LIMIT - 2 * result.size
        ),
    )(hidden, w_query, w_key, w_value, w_out, *small)


def fits_pair(n, groups, rows, w_query, w_out):
    chips = n // 2
    return (
        groups == 2
        and chips % 4 == 0
        and rows % 32 == 0
        and w_query.shape[1] % (2 * HEAD_DIM) == 0
        and w_query.shape[0] % 128 == 0
        and w_out.shape[1] % 512 == 0
    )


def local(n, groups, hidden, norm_gain, w_query, w_key, w_value, bias_query, bias_key, bias_value, w_out):
    rows, width = hidden.shape
    if fits_pair(n, groups, rows, w_query, w_out):
        return pair_local(n, hidden, norm_gain, w_query, w_key, w_value, bias_query, bias_key, bias_value, w_out)
    cols = w_query.shape[1]
    heads = cols // HEAD_DIM
    wide = cols + 2 * HEAD_DIM
    chips = n // 2
    exchange = groups > 1 and (rows // groups) % 16 == 0
    rh = rows // groups
    slices = 2 * n
    half_depth = w_query.shape[0] // 2
    half_cols = w_out.shape[1] // 2

    tables = tables_of(n, rows)
    vectors = [v.reshape(1, -1) for v in (norm_gain, bias_query, bias_key, bias_value)]

    any_spec = pl.BlockSpec(memory_space=pl.ANY)
    vmem = pl.BlockSpec(memory_space=pltpu.VMEM)
    links = max(groups - 1, 1) if exchange else 1
    pieces = slices if exchange else 1
    rpart = rh if exchange else 16
    dma = pltpu.SemaphoreType.DMA
    result = pl.pallas_call(
        functools.partial(kernel, n, groups, exchange),
        out_shape=jax.ShapeDtypeStruct((rh if exchange else rows, w_out.shape[1] * n), BF16),
        in_specs=[any_spec] * 5 + [vmem] * 8,
        out_specs=vmem,
        scratch_shapes=[
            pltpu.VMEM((rows, width), BF16),
            pltpu.VMEM((slices, half_depth, wide), BF16),
            pltpu.VMEM((slices, w_out.shape[0], half_cols), BF16),
            pltpu.VMEM((rows, wide), F32),
            pltpu.VMEM((chips, 2 * rows, 2 * HEAD_DIM), BF16),
            pltpu.VMEM((heads, rows, HEAD_DIM), BF16),
            pltpu.VMEM((heads, rows, 1), F32),
            pltpu.VMEM((heads, rows, 1), F32),
            pltpu.VMEM((heads, rows, HEAD_DIM), F32),
            pltpu.VMEM((rows, cols), BF16),
            pltpu.VMEM((links, pieces, rpart, half_cols), BF16),
            pltpu.VMEM((links, pieces, rpart, half_cols), BF16),
            pltpu.VMEM((pieces, rpart, half_cols), BF16),
            dma((9,)),
        ]
        + [dma((4 * chips,))] * 12
        + [dma((links * pieces,))] * 2,
        compiler_params=pltpu.CompilerParams(
            collective_id=0, has_side_effects=True, vmem_limit_bytes=64 * 1024 * 1024 - 128 * 1024
        ),
    )(hidden, w_query, w_key, w_value, w_out, *vectors, *tables)
    if exchange:
        return result
    return lax.psum_scatter(result, "head", scatter_dimension=0, tiled=True)


def solution(mesh):
    in_specs = (
        P("seq", None),
        P(),
        P("seq", "head"),
        P("seq", "head"),
        P("seq", "head"),
        P("head"),
        P("head"),
        P("head"),
        P("head", "seq"),
    )
    out_specs = P(("seq", "head"), None)
    body = functools.partial(local, mesh.shape["seq"], mesh.shape["head"])
    return jax.shard_map(body, mesh=mesh, in_specs=in_specs, out_specs=out_specs, check_vma=False)
```

```python
import functools

import jax
import jax.numpy as jnp
import numpy as np
from jax import lax
from jax.experimental import pallas as pl
from jax.experimental.pallas import tpu as pltpu
from jax.sharding import PartitionSpec as P

HEAD_DIM = 128
ROPE_BASE = 1000000.0
EPSILON = 1e-06
MESH = pl.DeviceIdType.MESH
F32 = jnp.float32
BF16 = jnp.bfloat16
OPS = (6, 1, 0, 1)
PIECES = (2, 2, 2)
STACK = 2
VMEM_LIMIT = 64 * 1024 * 1024 - 4096 * 1024


def kernel(
    n, groups, exchange,
    hidden, w_query, w_key, w_value, w_out, gain, bias_query, bias_key, bias_value,
    near_cos, near_sin, far_cos, far_sin,
    out,
    hid, w_all, wo_all, acc, kv_all, q_ref, high, total, mixed, att, ts, tr, tm,
    load_sem, ws, wr, wps, wpr, os_, or_, ops, opr, ks, kr, kps, kpr, ys, yr,
):
    chips = n // 2
    depth = chips // 2
    me = lax.axis_index("seq")
    group = lax.axis_index("head")
    core = me % 2
    chip = me // 2
    ring = chip // 2 + (chip % 2) * (2 * depth - 1 - 2 * (chip // 2))

    def device_at(position, which):
        position = (position + 2 * chips) % chips
        side = position // depth
        row = position + side * (2 * depth - 1 - 2 * position)
        return 2 * (2 * row + side) + which

    right = device_at(ring + 1, core)
    left = device_at(ring - 1, core)
    partner = 2 * chip + (1 - core)
    neighbours = (right, left)

    def source_at(direction, offset, which):
        return device_at(ring - offset if direction == 0 else ring + offset, which)

    rows, width = hidden.shape
    half_depth = w_query.shape[0] // 2
    q_cols = w_query.shape[1]
    heads = q_cols // HEAD_DIM
    half_cols = w_out.shape[1] // 2
    rh = rows // groups

    loads = []
    late = [pltpu.make_async_copy(hidden, hid, load_sem.at[0])]
    for h in range(2):
        span = pl.ds(h * half_depth, half_depth)
        slot = w_all.at[2 * me + h]
        loads.append(pltpu.make_async_copy(w_query.at[span], slot.at[:, pl.ds(0, q_cols)], load_sem.at[1 + 4 * h]))
        loads.append(pltpu.make_async_copy(w_key.at[span], slot.at[:, pl.ds(q_cols, HEAD_DIM)], load_sem.at[2 + 4 * h]))
        loads.append(pltpu.make_async_copy(w_value.at[span], slot.at[:, pl.ds(q_cols + HEAD_DIM, HEAD_DIM)], load_sem.at[3 + 4 * h]))
        late.append(pltpu.make_async_copy(w_out.at[:, pl.ds(h * half_cols, half_cols)], wo_all.at[2 * me + h], load_sem.at[4 + 4 * h]))
    for copy in loads + late:
        copy.start()

    barrier = pltpu.get_barrier_semaphore()
    for device in (right, left, partner):
        pl.semaphore_signal(barrier, inc=1, device_id={"seq": device}, device_id_type=MESH)
    peers = range(1, groups) if exchange else ()
    for p in peers:
        pl.semaphore_signal(barrier, inc=1, device_id={"head": (group + p) % groups}, device_id_type=MESH)
    pl.semaphore_wait(barrier, 3 + len(peers))

    def remote(ref, send, recv, key, device):
        return pltpu.make_async_remote_copy(
            src_ref=ref, dst_ref=ref, send_sem=send.at[key], recv_sem=recv.at[key],
            device_id={"seq": device}, device_id_type=MESH,
        )

    def piece(buffer, index, j):
        size = buffer.shape[1] // 2
        return buffer.at[index, pl.ds(j * size, size)]

    def key_of(direction, step, j):
        return (direction * chips + step) * 2 + j

    def ring_begin(buffer, sems):
        ss, rs, pss, prs = sems
        for j in range(2):
            for d in range(2):
                own = piece(buffer, 2 * me + d, j)
                remote(own, ss, rs, key_of(d, 0, j), neighbours[d]).start()
        for j in range(2):
            for d in range(2):
                own = piece(buffer, 2 * me + d, j)
                remote(own, pss, prs, key_of(d, chips - 1, j), partner).start()

    def ring_advance(buffer, sems, t):
        ss, rs, pss, prs = sems

        @pl.when(t < chips - 1)
        def _():
            for j in range(2):
                for d in range(2):
                    block = piece(buffer, 2 * source_at(d, t + 1, core) + d, j)
                    remote(block, ss, rs, key_of(d, t, j), neighbours[d]).wait_recv()

                    @pl.when(t < chips - 2)
                    def _():
                        remote(block, ss, rs, key_of(d, t + 1, j), neighbours[d]).start()

                    remote(block, pss, prs, key_of(d, t, j), partner).start()

    def partner_wait(buffer, sems, t):
        ss, rs, pss, prs = sems
        for j in range(2):
            for d in range(2):
                block = piece(buffer, 2 * source_at(d, t, 1 - core) + d, j)
                remote(block, pss, prs, key_of(d, (t + chips - 1) % chips, j), partner).wait_recv()

    def ring_drain(buffer, sems):
        ss, rs, pss, prs = sems

        def body(t, carry):
            for j in range(2):
                for d in range(2):
                    block = piece(buffer, 2 * me + d, j)

                    @pl.when(t < chips - 1)
                    def _():
                        remote(block, ss, rs, key_of(d, t, j), neighbours[d]).wait_send()

                    remote(block, pss, prs, key_of(d, t, j), partner).wait_send()
            return carry

        lax.fori_loop(0, chips, body, 0)

    w_sems = (ws, wr, wps, wpr)
    o_sems = (os_, or_, ops, opr)

    for copy in loads:
        copy.wait()
    ring_begin(w_all, w_sems)
    for copy in late:
        copy.wait()
    slices = 2 * n
    step_cols = width // slices

    def columns(i):
        return pl.ds(pl.multiple_of(i * step_cols, step_cols), step_cols)

    def square(i, carry):
        x = hid[:, columns(i)].astype(F32)
        return carry + x * x

    squares = lax.fori_loop(0, slices, square, jnp.zeros((rows, step_cols), F32))
    inverse = lax.rsqrt(jnp.sum(squares, axis=-1, keepdims=True) * (1.0 / width) + EPSILON)

    def normed(i):
        scaled = hid[:, columns(i)].astype(F32) * inverse * gain[:, columns(i)].astype(F32)
        return scaled.astype(BF16)

    bias = (bias_query, bias_key, bias_value)
    starts = (0, q_cols, q_cols + HEAD_DIM)
    for start, part in zip(starts, bias):
        span = pl.ds(start, part.shape[1])
        acc[:, span] = jnp.broadcast_to(part[...].astype(F32), (rows, part.shape[1]))

    def project(t, carry):
        ring_advance(w_all, w_sems, t)
        partner_wait(w_all, w_sems, t)
        for d in range(2):
            i = 2 * source_at(d, t, core) + d
            k = 2 * source_at(d, t, 1 - core) + d
            acc[...] += jnp.dot(normed(i), w_all[i], preferred_element_type=F32) + jnp.dot(
                normed(k), w_all[k], preferred_element_type=F32
            )
        return carry

    lax.fori_loop(0, chips, project, 0)

    block_cos, block_sin = far_cos[me], far_sin[me]
    cosine = near_cos[...] * block_cos - near_sin[...] * block_sin
    lane = lax.broadcasted_iota(jnp.int32, cosine.shape, 1)
    sine = near_sin[...] * block_cos + near_cos[...] * block_sin
    sine = jnp.where(lane < HEAD_DIM // 2, -sine, sine)

    def rotary(x):
        return x * cosine + pltpu.roll(x, HEAD_DIM // 2, 1) * sine

    def kv_rows(which):
        return pl.ds(pl.multiple_of(which * rows, rows), rows)

    kv_all[chip, kv_rows(core), pl.ds(0, HEAD_DIM)] = rotary(acc[:, pl.ds(q_cols, HEAD_DIM)]).astype(BF16)
    kv_all[chip, kv_rows(core), pl.ds(HEAD_DIM, HEAD_DIM)] = acc[:, pl.ds(q_cols + HEAD_DIM, HEAD_DIM)].astype(BF16)
    for h in range(heads):
        q_ref[h] = rotary(acc[:, pl.ds(h * HEAD_DIM, HEAD_DIM)]).astype(BF16)

    reach = (chips // 2, chips - 1 - chips // 2)

    parts = 2 if rows % 32 == 0 else 1
    piece_rows = rows // parts

    def kv_copy(owner, ss, rs, direction, step, j, device):
        start = pl.multiple_of((owner % 2) * rows + j * piece_rows, piece_rows)
        block = kv_all.at[owner // 2, pl.ds(start, piece_rows)]
        return remote(block, ss, rs, key_of(direction, step, j), device)

    for j in range(parts):
        for d in range(2):
            kv_copy(me, ks, kr, d, 0, j, neighbours[d]).start()
        kv_copy(me, kps, kpr, 0, chips - 1, j, partner).start()

    factor = HEAD_DIM ** (-0.5) * 1.4426950408889634

    def attend(c, own):
        for h in range(heads):
            scores = lax.dot_general(
                q_ref[h], kv_all[c, :, pl.ds(0, HEAD_DIM)], (((1,), (1,)), ((), ())),
                preferred_element_type=F32,
            )
            if own:
                row = lax.broadcasted_iota(jnp.int32, scores.shape, 0) + core * rows
                col = lax.broadcasted_iota(jnp.int32, scores.shape, 1)
                scores = jnp.where(row >= col, scores, -jnp.inf)
            top = jnp.max(scores, axis=-1, keepdims=True)
            if not own:
                old = high[h]
                top = jnp.maximum(old, top)
            probs = jnp.exp2((scores - top) * factor)
            part = jnp.sum(probs, axis=-1, keepdims=True)
            product = jnp.dot(
                probs.astype(BF16), kv_all[c, :, pl.ds(HEAD_DIM, HEAD_DIM)], preferred_element_type=F32
            )
            if not own:
                shrink = jnp.exp2((old - top) * factor)
                part = part + total[h] * shrink
                product = product + mixed[h] * shrink
            high[h] = top
            total[h] = part
            mixed[h] = product

    for j in range(parts):
        kv_copy(partner, kps, kpr, 0, chips - 1, j, partner).wait_recv()
    attend(chip, True)

    def attention(t, carry):
        for j in range(parts):
            for d in range(2):
                @pl.when(t < reach[d])
                def _():
                    owner = source_at(d, t + 1, core)
                    kv_copy(owner, ks, kr, d, t, j, neighbours[d]).wait_recv()

                    @pl.when(t + 1 < reach[d])
                    def _():
                        kv_copy(owner, ks, kr, d, t + 1, j, neighbours[d]).start()

                    kv_copy(owner, kps, kpr, d, t, j, partner).start()

        @pl.when(t == reach[0] - 1)
        def _():
            ring_begin(wo_all, o_sems)

        for d in range(2):
            @pl.when((t > 0) & (t <= reach[d]))
            def _():
                owner = source_at(d, t, 1 - core)
                for j in range(parts):
                    kv_copy(owner, kps, kpr, d, t - 1, j, partner).wait_recv()

                @pl.when(owner // 2 < chip)
                def _():
                    attend(owner // 2, False)
        return carry

    lax.fori_loop(0, reach[0] + 1, attention, 0)
    for h in range(heads):
        att[:, pl.ds(h * HEAD_DIM, HEAD_DIM)] = (mixed[h] / total[h]).astype(BF16)

    def term_copy(p, i):
        return pltpu.make_async_remote_copy(
            src_ref=ts.at[p - 1, i], dst_ref=tr.at[p - 1, i],
            send_sem=ys.at[(p - 1) * slices + i], recv_sem=yr.at[(p - 1) * slices + i],
            device_id={"head": (group + p) % groups}, device_id_type=MESH,
        )

    def out_columns(i):
        return pl.ds(pl.multiple_of(i * half_cols, half_cols), half_cols)

    def make_term(i):
        if not exchange:
            out[:, out_columns(i)] = jnp.dot(att[...], wo_all[i], preferred_element_type=F32).astype(BF16)
            return
        for p in peers:
            span = pl.ds(pl.multiple_of(((group + p) % groups) * rh, rh), rh)
            ts[p - 1, i] = jnp.dot(att[span, :], wo_all[i], preferred_element_type=F32).astype(BF16)
            term_copy(p, i).start()
        span = pl.ds(pl.multiple_of(group * rh, rh), rh)
        tm[i] = jnp.dot(att[span, :], wo_all[i], preferred_element_type=F32).astype(BF16)

    def blocks_of(t):
        return [2 * source_at(d, t, which) + d for d in range(2) for which in (core, 1 - core)]

    def finish(t, carry):
        for i in blocks_of(t):
            value = tm[i].astype(F32)
            for p in peers:
                term_copy(p, i).wait_recv()
                value = value + tr[p - 1, i].astype(F32)
            out[:, out_columns(i)] = value.astype(BF16)
        return carry

    lag = 3

    def partner_terms(t):
        partner_wait(wo_all, o_sems, t)
        for d in range(2):
            make_term(2 * source_at(d, t, 1 - core) + d)

    for d in range(2):
        make_term(2 * me + d)
    partner_terms(0)

    def project_out(t, carry):
        ring_advance(wo_all, o_sems, t)

        @pl.when(t < chips - 1)
        def _():
            for d in range(2):
                make_term(2 * source_at(d, t + 1, core) + d)

        @pl.when(t > 0)
        def _():
            partner_terms(t)

        if exchange:
            @pl.when(t >= lag)
            def _():
                finish(t - lag, 0)
        return carry

    lax.fori_loop(0, chips, project_out, 0)

    if exchange:
        lax.fori_loop(chips - lag, chips, finish, 0)

        def sent(i, carry):
            for p in peers:
                term_copy(p, i).wait_send()
            return carry

        lax.fori_loop(0, slices, sent, 0)

    ring_drain(w_all, w_sems)
    ring_drain(wo_all, o_sems)
    for j in range(parts):
        for d in range(2):
            for t in range(reach[d]):
                kv_copy(me, ks, kr, d, t, j, neighbours[d]).wait_send()
                kv_copy(me, kps, kpr, d, t, j, partner).wait_send()
        kv_copy(me, kps, kpr, 0, chips - 1, j, partner).wait_send()


def pair_kernel(
    n, chunks_in, chunks_out, parts,
    hidden, w_query, w_key, w_value, w_out, *rest_refs,
):
    small = rest_refs[:8]
    out = rest_refs[8]
    held = rest_refs[9:17]
    gain, bias_query, bias_key, bias_value, near_cos, near_sin, far_cos, far_sin = held
    (
    gains, small_sem, hid, w_all, wo, acc, kv_all, q_ref, high, total, mixed, att, terms, wo_own,
    own_s, own_r, load_sem, swap_s, swap_r, att_s, att_r, ys, yr,
    ws, wr, wps, wpr, os_, or_, ops, opr, ks, kr, kps, kpr,
    ) = rest_refs[17:]
    chips = n // 2
    depth = chips // 2
    ops_from, ops_first, ops_busy, ops_calm = OPS
    stack = STACK
    me = lax.axis_index("seq")
    group = lax.axis_index("head")
    peer = 1 - group
    core = me % 2
    chip = me // 2
    ring = chip // 2 + (chip % 2) * (2 * depth - 1 - 2 * (chip // 2))

    def device_at(position, which):
        position = (position + 2 * chips) % chips
        side = position // depth
        row = position + side * (2 * depth - 1 - 2 * position)
        return 2 * (2 * row + side) + which

    right = device_at(ring + 1, core)
    left = device_at(ring - 1, core)
    partner = 2 * chip + (1 - core)
    neighbours = (right, left)

    def source_at(direction, offset, which):
        return device_at(ring - offset if direction == 0 else ring + offset, which)

    rows, width = hidden.shape
    half_depth = w_query.shape[0] // 2
    q_cols = w_query.shape[1]
    heads = q_cols // HEAD_DIM
    out_depth = w_out.shape[0]
    group_cols = w_out.shape[1] // 2
    lane_cols = group_cols // 2
    rh = rows // 2

    def remote(ref, send, recv, key, device):
        return pltpu.make_async_remote_copy(
            src_ref=ref, dst_ref=ref, send_sem=send.at[key], recv_sem=recv.at[key],
            device_id={"seq": device}, device_id_type=MESH,
        )

    def lanes(which):
        return pl.ds(pl.multiple_of(which * lane_cols, lane_cols), lane_cols)

    def wo_lanes(which, d):
        start = which * group_cols + d * lane_cols
        return pl.ds(pl.multiple_of(start, lane_cols), lane_cols)

    def group_rows(which):
        return pl.ds(pl.multiple_of(which * out_depth, out_depth), out_depth)

    loads, last = [], []
    for h in range(2):
        span = pl.ds(h * half_depth, half_depth)
        slot = w_all.at[2 * me + h]
        loads.append((w_key.at[span], slot.at[:, pl.ds(0, HEAD_DIM)]))
        loads.append((w_value.at[span], slot.at[:, pl.ds(HEAD_DIM, HEAD_DIM)]))
        loads.append((w_query.at[span], slot.at[:, pl.ds(2 * HEAD_DIM, q_cols)]))
        last.append((w_out.at[:, wo_lanes(group, h)], wo.at[chip, h, group_rows(group), lanes(core)]))
        last.append((w_out.at[:, wo_lanes(peer, h)], wo_own.at[h, group_rows(group), lanes(core)]))
    copies = [pltpu.make_async_copy(a, b, load_sem.at[i]) for i, (a, b) in enumerate(loads + [(hidden, hid)] + last)]
    small_copies = [pltpu.make_async_copy(a, b, small_sem.at[i]) for i, (a, b) in enumerate(zip(small, held))]
    for copy in copies[: len(loads)]:
        copy.start()

    barrier = pltpu.get_barrier_semaphore()
    for device in (right, left, partner):
        pl.semaphore_signal(barrier, inc=1, device_id={"seq": device}, device_id_type=MESH)
    pl.semaphore_signal(barrier, inc=1, device_id={"head": peer}, device_id_type=MESH)
    pl.semaphore_wait(barrier, 4)

    def across(src, dst, send, recv, key):
        return pltpu.make_async_remote_copy(
            src_ref=src, dst_ref=dst, send_sem=send.at[key], recv_sem=recv.at[key],
            device_id={"head": peer}, device_id_type=MESH,
        )

    def swap(d):
        return across(
            w_out.at[:, wo_lanes(peer, d)], wo.at[chip, d, group_rows(group), lanes(core)], swap_s, swap_r, d
        )

    def swap_own(d):
        return across(
            w_out.at[:, wo_lanes(group, d)], wo_own.at[d, group_rows(group), lanes(core)], swap_s, swap_r, 2 + d
        )

    def own_copy(d, which):
        return remote(wo_own.at[d, :, lanes(which)], own_s, own_r, d, partner)

    class Ring:
        def __init__(self, view, sems, pieces):
            self.view, self.sems, self.pieces = view, sems, pieces

        def key(self, d, step, j):
            return (d * chips + step) * self.pieces + j

        def begin(self, j):
            send, recv, psend, precv = self.sems
            for d in range(2):
                own = self.view(me, d, j)
                remote(own, send, recv, self.key(d, 0, j), neighbours[d]).start()
            for d in range(2):
                own = self.view(me, d, j)
                remote(own, psend, precv, self.key(d, chips - 1, j), partner).start()

        def advance(self, t, j):
            send, recv, psend, precv = self.sems
            for d in range(2):
                block = self.view(source_at(d, t + 1, core), d, j)
                remote(block, send, recv, self.key(d, t, j), neighbours[d]).wait_recv()

                @pl.when(t < chips - 2)
                def _():
                    remote(block, send, recv, self.key(d, t + 1, j), neighbours[d]).start()

                remote(block, psend, precv, self.key(d, t, j), partner).start()

        def op(self, index):
            @pl.when(index < self.pieces)
            def _():
                self.begin(index)

            @pl.when((index >= self.pieces) & (index < self.pieces * chips))
            def _():
                done = index - self.pieces
                self.advance(done // self.pieces, done % self.pieces)

        def partner_wait(self, t, some=None):
            send, recv, psend, precv = self.sems
            for j in range(self.pieces) if some is None else some:
                for d in range(2):
                    block = self.view(source_at(d, t, 1 - core), d, j)
                    remote(block, psend, precv, self.key(d, (t + chips - 1) % chips, j), partner).wait_recv()

        def drain(self):
            send, recv, psend, precv = self.sems

            def body(t, carry):
                for j in range(self.pieces):
                    for d in range(2):
                        block = self.view(me, d, j)

                        @pl.when(t < chips - 1)
                        def _():
                            remote(block, send, recv, self.key(d, t, j), neighbours[d]).wait_send()

                        remote(block, psend, precv, self.key(d, t, j), partner).wait_send()
                return carry

            lax.fori_loop(0, chips, body, 0)

    def rows_view(buffer, pieces):
        size = buffer.shape[1] // pieces
        return lambda owner, d, j: buffer.at[2 * owner + d, pl.ds(pl.multiple_of(j * size, size), size)]

    def wo_view(owner, d, j):
        size = wo.shape[2] // chunks_out
        return wo.at[owner // 2, d, pl.ds(pl.multiple_of(j * size, size), size), lanes(owner % 2)]

    first = Ring(rows_view(w_all, chunks_in), (ws, wr, wps, wpr), chunks_in)
    third = Ring(wo_view, (os_, or_, ops, opr), chunks_out)

    for copy in copies[: len(loads)]:
        copy.wait()
    for j in range(chunks_in):
        first.begin(j)
    for d in range(2):
        swap(d).start()
    for d in range(2):
        swap_own(d).start()
    for copy in copies[len(loads):] + small_copies:
        copy.start()
    for copy in copies[len(loads):]:
        copy.wait()

    for copy in small_copies:
        copy.wait()
    gains[...] = gain[...].astype(F32)

    slices = 2 * n
    step_cols = width // slices
    gain_rows = step_cols // HEAD_DIM

    def columns(i):
        return pl.ds(pl.multiple_of(i * step_cols, step_cols), step_cols)

    def square(i, carry):
        x = hid[:, columns(i)].astype(F32)
        return carry + x * x

    squares = lax.fori_loop(0, slices, square, jnp.zeros((rows, step_cols), F32))
    inverse = lax.rsqrt(jnp.sum(squares, axis=-1, keepdims=True) * (1.0 / width) + EPSILON)

    def normed(i):
        line = jnp.concatenate([gains[pl.ds(i * gain_rows + r, 1), :] for r in range(gain_rows)], axis=1)
        scaled = hid[:, columns(i)].astype(F32) * inverse * line
        return scaled.astype(BF16)

    def widen(line):
        return jnp.broadcast_to(line.astype(F32), (rows, HEAD_DIM))

    acc[:, pl.ds(0, HEAD_DIM)] = widen(bias_key[...])
    acc[:, pl.ds(HEAD_DIM, HEAD_DIM)] = widen(bias_value[...])
    lines = bias_query[...].astype(F32)
    for h in range(heads):
        acc[:, pl.ds((2 + h) * HEAD_DIM, HEAD_DIM)] = widen(lines[h : h + 1])

    def project(t, carry):
        @pl.when(t < chips - 1)
        def _():
            for j in range(chunks_in):
                first.advance(t, j)

        @pl.when(t == ops_from)
        def _():
            for d in range(2):
                swap(d).wait_recv()

        @pl.when(t == chips // 2)
        def _():
            for d in range(2):
                swap_own(d).wait_recv()
                own_copy(d, core).start()

        @pl.when((t >= ops_from) & (t < ops_from + ops_first))
        def _():
            third.op(t - ops_from)

        first.partner_wait(t)
        for d in range(2):
            i = 2 * source_at(d, t, core) + d
            k = 2 * source_at(d, t, 1 - core) + d
            acc[...] += jnp.dot(normed(i), w_all[i], preferred_element_type=F32) + jnp.dot(
                normed(k), w_all[k], preferred_element_type=F32
            )
        return carry

    lax.fori_loop(0, chips, project, 0)

    block_cos, block_sin = far_cos[me], far_sin[me]
    cosine = near_cos[...] * block_cos - near_sin[...] * block_sin
    lane = lax.broadcasted_iota(jnp.int32, cosine.shape, 1)
    sine = near_sin[...] * block_cos + near_cos[...] * block_sin
    sine = jnp.where(lane < HEAD_DIM // 2, -sine, sine)

    def rotary(x):
        return x * cosine + pltpu.roll(x, HEAD_DIM // 2, 1) * sine

    def kv_rows(which):
        return pl.ds(pl.multiple_of(which * rows, rows), rows)

    kv_all[chip, kv_rows(core), pl.ds(0, HEAD_DIM)] = rotary(acc[:, pl.ds(0, HEAD_DIM)]).astype(BF16)
    kv_all[chip, kv_rows(core), pl.ds(HEAD_DIM, HEAD_DIM)] = acc[:, pl.ds(HEAD_DIM, HEAD_DIM)].astype(BF16)
    q_ref[pl.ds(0, rows), :] = rotary(acc[:, pl.ds(2 * HEAD_DIM, HEAD_DIM)]).astype(BF16)

    far_steps = chips // 2
    reach = [[far_steps - (j * 2 // parts != d) for j in range(parts)] for d in range(2)]
    piece_rows = rows // parts

    def kv_copy(owner, send, recv, direction, step, j, device):
        start = pl.multiple_of((owner % 2) * rows + j * piece_rows, piece_rows)
        block = kv_all.at[owner // 2, pl.ds(start, piece_rows)]
        return remote(block, send, recv, (direction * chips + step) * parts + j, device)

    for j in range(parts):
        for d in range(2):
            kv_copy(me, ks, kr, d, 0, j, neighbours[d]).start()
        kv_copy(me, kps, kpr, 0, chips - 1, j, partner).start()
    for h in range(1, heads):
        q_ref[pl.ds(h * rows, rows), :] = rotary(acc[:, pl.ds((2 + h) * HEAD_DIM, HEAD_DIM)]).astype(BF16)

    factor = HEAD_DIM ** (-0.5) * 1.4426950408889634

    def attend(c, own):
        for h in range(0, heads, stack):
            some = pl.ds(h * rows, stack * rows)
            scores = lax.dot_general(
                q_ref[some, :], kv_all[c, :, pl.ds(0, HEAD_DIM)], (((1,), (1,)), ((), ())),
                preferred_element_type=F32,
            )
            if own:
                row = lax.broadcasted_iota(jnp.int32, scores.shape, 0) % rows + core * rows
                col = lax.broadcasted_iota(jnp.int32, scores.shape, 1)
                scores = jnp.where(row >= col, scores, -jnp.inf)
            top = jnp.max(scores, axis=-1, keepdims=True)
            if not own:
                old = high[some, :]
                top = jnp.maximum(old, top)
            probs = jnp.exp2((scores - top) * factor)
            part = jnp.sum(probs, axis=-1, keepdims=True)
            product = jnp.dot(
                probs.astype(BF16), kv_all[c, :, pl.ds(HEAD_DIM, HEAD_DIM)], preferred_element_type=F32
            )
            if not own:
                shrink = jnp.exp2((old - top) * factor)
                part = part + total[some, :] * shrink
                product = product + mixed[some, :] * shrink
            high[some, :] = top
            total[some, :] = part
            mixed[some, :] = product

    for j in range(parts):
        kv_copy(partner, kps, kpr, 0, chips - 1, j, partner).wait_recv()
    attend(chip, True)

    busy_steps = far_steps - 1

    def attention(t, carry):
        for j in range(parts):
            for d in range(2):
                @pl.when(t < reach[d][j])
                def _():
                    owner = source_at(d, t + 1, core)
                    kv_copy(owner, ks, kr, d, t, j, neighbours[d]).wait_recv()

                    @pl.when(t + 1 < reach[d][j])
                    def _():
                        kv_copy(owner, ks, kr, d, t + 1, j, neighbours[d]).start()

                    kv_copy(owner, kps, kpr, d, t, j, partner).start()

        for k in range(max(ops_busy, ops_calm)):
            index = ops_first + ops_busy * jnp.minimum(t, busy_steps) + ops_calm * jnp.maximum(t - busy_steps, 0) + k

            @pl.when(((t < busy_steps) & (k < ops_busy)) | ((t >= busy_steps) & (k < ops_calm)))
            def _():
                third.op(index)

        for j in range(parts):
            for d in range(2):
                @pl.when((t > 0) & (t <= reach[d][j]))
                def _():
                    owner = source_at(d, t, 1 - core)
                    kv_copy(owner, kps, kpr, d, t - 1, j, partner).wait_recv()

        for d in range(2):
            other = source_at(d, t, core) // 2

            @pl.when((t > 0) & (t <= far_steps - d) & (other < chip))
            def _():
                attend(other, False)
        return carry

    lax.fori_loop(0, far_steps + 1, attention, 0)
    ops_done = ops_first + ops_busy * busy_steps + ops_calm * (far_steps + 1 - busy_steps)

    def row_span(which):
        return pl.ds(pl.multiple_of(which * rh, rh), rh)

    def att_copy(key):
        ref = att.at[group, row_span((group + key) % 2), :]
        return across(ref, ref, att_s, att_r, key)

    for h in range(heads):
        att[group, :, pl.ds(h * HEAD_DIM, HEAD_DIM)] = (
            mixed[pl.ds(h * rows, rows), :] / total[pl.ds(h * rows, rows), :]
        ).astype(BF16)
    for key in range(2):
        att_copy(key).start()

    def out_span(c, d, which):
        start = (2 * c + which) * 2 * group_cols + group * group_cols + d * lane_cols
        return pl.ds(pl.multiple_of(start, lane_cols), lane_cols)

    def term_copy(c, d, which):
        src = terms.at[c, d, :, pl.ds(which * lane_cols, lane_cols)]
        return across(src, out.at[:, out_span(c, d, which)], ys, yr, (2 * c + d) * 2 + which)

    def part(weights, which, g):
        return jnp.dot(
            att[g, row_span(which), :], weights[pl.ds(g * out_depth, out_depth), :], preferred_element_type=F32
        ).astype(BF16).astype(F32)

    def product(weights, which):
        return (part(weights, which, 0) + part(weights, which, 1)).astype(BF16)

    def send_terms(c, d, value):
        terms[c, d] = value
        for which in range(2):
            term_copy(c, d, which).start()

    def give(t, d):
        c = source_at(d, t, core) // 2
        send_terms(c, d, product(wo.at[c, d], peer))

    def put(c, d, owner, value):
        for which in range(2):
            start = (2 * c + which) * 2 * group_cols + owner * group_cols + d * lane_cols
            span = pl.ds(pl.multiple_of(start, lane_cols), lane_cols)
            out[:, span] = value[:, which * lane_cols : (which + 1) * lane_cols]

    def keep(t, d):
        c = source_at(d, t, core) // 2
        put(c, d, group, product(wo.at[c, d], group))

    def keep_own(d):
        put(chip, d, group, product(wo.at[chip, d], group))
        put(chip, d, peer, product(wo_own.at[d], group))

    third.partner_wait(0)

    def project_out(t, carry):
        third.partner_wait(t)

        @pl.when(t == 1)
        def _():
            att_copy(0).wait_recv()

        def move(j):
            @pl.when((t + 1) * chunks_out + j >= ops_done)
            def _():
                third.advance(t, j)

        for j in range(chunks_out - 1):
            move(j)
        for d in range(2):
            give(t, d)

        @pl.when(t == 1)
        def _():
            att_copy(1).wait_recv()

        for d in range(2):
            keep(t, d)
        move(chunks_out - 1)

        @pl.when(t == chips // 2)
        def _():
            for d in range(2):
                own_copy(d, 1 - core).wait_recv()
                keep_own(d)
        return carry

    for j in range(chunks_out):
        if chunks_out + j >= ops_done:
            third.advance(0, j)
    lax.fori_loop(1, chips - 1, project_out, 0)
    final = chips - 1
    held_parts = []
    for j in range(chunks_out):
        third.partner_wait(final, (j,))
        for d in range(2):
            held_parts.append(part(wo.at[source_at(d, final, core) // 2, d], peer, j))
    for d in range(2):
        send_terms(source_at(d, final, core) // 2, d, (held_parts[d] + held_parts[2 + d]).astype(BF16))
    for d in range(2):
        keep(final, d)


    first.drain()
    third.drain()
    for j in range(parts):
        for d in range(2):
            for t in range(reach[d][j]):
                kv_copy(me, ks, kr, d, t, j, neighbours[d]).wait_send()
                kv_copy(me, kps, kpr, d, t, j, partner).wait_send()
        kv_copy(me, kps, kpr, 0, chips - 1, j, partner).wait_send()
    for d in range(2):
        swap(d).wait_send()
        swap_own(d).wait_send()
        own_copy(d, core).wait_send()
    for key in range(2):
        att_copy(key).wait_send()

    def finish(c, carry):
        @pl.when(c != chip)
        def _():
            for d in range(2):
                for which in range(2):
                    term_copy(c, d, which).wait_send()
                    term_copy(c, d, which).wait_recv()
        return carry

    lax.fori_loop(0, chips, finish, 0)


def tables_of(n, rows):
    freq = ROPE_BASE ** (-2.0 * np.arange(HEAD_DIM // 2, dtype=np.float64) / HEAD_DIM)
    freq = np.concatenate([freq, freq])
    near = np.arange(rows, dtype=np.float64)[:, None] * freq
    far = (np.arange(n, dtype=np.float64) * rows)[:, None, None] * freq
    return [f(a).astype(np.float32) for a in (near, far) for f in (np.cos, np.sin)]


def pair_local(n, hidden, norm_gain, w_query, w_key, w_value, bias_query, bias_key, bias_value, w_out):
    rows, width = hidden.shape
    cols = w_query.shape[1]
    heads = cols // HEAD_DIM
    chips = n // 2
    slices = 2 * n
    half_depth = w_query.shape[0] // 2
    group_cols = w_out.shape[1] // 2
    chunks_in, chunks_out, parts = PIECES
    vectors = [v.reshape(-1, HEAD_DIM) for v in (norm_gain, bias_query, bias_key, bias_value)]
    small = vectors + tables_of(n, rows)
    result = jax.ShapeDtypeStruct((rows // 2, w_out.shape[1] * n), BF16)
    any_spec = pl.BlockSpec(memory_space=pl.ANY)
    dma = pltpu.SemaphoreType.DMA
    return pl.pallas_call(
        functools.partial(pair_kernel, n, chunks_in, chunks_out, parts),
        out_shape=pltpu.VMEM(result.shape, result.dtype),
        in_specs=[any_spec] * 13,
        out_specs=pl.BlockSpec(memory_space=pltpu.VMEM),
        scratch_shapes=[pltpu.VMEM(a.shape, a.dtype) for a in small]
        + [
            pltpu.VMEM((width // HEAD_DIM, HEAD_DIM), F32),
            dma((8,)),
            pltpu.VMEM((rows, width), BF16),
            pltpu.VMEM((slices, half_depth, 2 * HEAD_DIM + cols), BF16),
            pltpu.VMEM((chips, 2, 2 * w_out.shape[0], group_cols), BF16),
            pltpu.VMEM((rows, 2 * HEAD_DIM + cols), F32),
            pltpu.VMEM((chips, 2 * rows, 2 * HEAD_DIM), BF16),
            pltpu.VMEM((heads * rows, HEAD_DIM), BF16),
            pltpu.VMEM((heads * rows, 1), F32),
            pltpu.VMEM((heads * rows, 1), F32),
            pltpu.VMEM((heads * rows, HEAD_DIM), F32),
            pltpu.VMEM((2, rows, cols), BF16),
            pltpu.VMEM((chips, 2, rows // 2, group_cols), BF16),
            pltpu.VMEM((2, 2 * w_out.shape[0], group_cols), BF16),
            dma((2,)), dma((2,)),
            dma((11,)),
            dma((4,)), dma((4,)), dma((2,)), dma((2,)),
            dma((4 * chips,)), dma((4 * chips,)),
        ]
        + [dma((2 * chips * chunks_in,))] * 4
        + [dma((2 * chips * chunks_out,))] * 4
        + [dma((2 * chips * parts,))] * 4,
        compiler_params=pltpu.CompilerParams(
            collective_id=0, has_side_effects=True, vmem_limit_bytes=VMEM_LIMIT - 2 * result.size
        ),
    )(hidden, w_query, w_key, w_value, w_out, *small)


def fits_pair(n, groups, rows, w_query, w_out):
    chips = n // 2
    return (
        groups == 2
        and chips % 4 == 0
        and rows % 32 == 0
        and w_query.shape[1] % HEAD_DIM == 0
        and w_query.shape[0] % 128 == 0
        and w_out.shape[1] % 512 == 0
    )


def local(n, groups, hidden, norm_gain, w_query, w_key, w_value, bias_query, bias_key, bias_value, w_out):
    rows, width = hidden.shape
    if fits_pair(n, groups, rows, w_query, w_out):
        return pair_local(n, hidden, norm_gain, w_query, w_key, w_value, bias_query, bias_key, bias_value, w_out)
    cols = w_query.shape[1]
    heads = cols // HEAD_DIM
    wide = cols + 2 * HEAD_DIM
    chips = n // 2
    exchange = groups > 1 and (rows // groups) % 16 == 0
    rh = rows // groups
    slices = 2 * n
    half_depth = w_query.shape[0] // 2
    half_cols = w_out.shape[1] // 2

    tables = tables_of(n, rows)
    vectors = [v.reshape(1, -1) for v in (norm_gain, bias_query, bias_key, bias_value)]

    any_spec = pl.BlockSpec(memory_space=pl.ANY)
    vmem = pl.BlockSpec(memory_space=pltpu.VMEM)
    links = max(groups - 1, 1) if exchange else 1
    pieces = slices if exchange else 1
    rpart = rh if exchange else 16
    dma = pltpu.SemaphoreType.DMA
    result = pl.pallas_call(
        functools.partial(kernel, n, groups, exchange),
        out_shape=jax.ShapeDtypeStruct((rh if exchange else rows, w_out.shape[1] * n), BF16),
        in_specs=[any_spec] * 5 + [vmem] * 8,
        out_specs=vmem,
        scratch_shapes=[
            pltpu.VMEM((rows, width), BF16),
            pltpu.VMEM((slices, half_depth, wide), BF16),
            pltpu.VMEM((slices, w_out.shape[0], half_cols), BF16),
            pltpu.VMEM((rows, wide), F32),
            pltpu.VMEM((chips, 2 * rows, 2 * HEAD_DIM), BF16),
            pltpu.VMEM((heads, rows, HEAD_DIM), BF16),
            pltpu.VMEM((heads, rows, 1), F32),
            pltpu.VMEM((heads, rows, 1), F32),
            pltpu.VMEM((heads, rows, HEAD_DIM), F32),
            pltpu.VMEM((rows, cols), BF16),
            pltpu.VMEM((links, pieces, rpart, half_cols), BF16),
            pltpu.VMEM((links, pieces, rpart, half_cols), BF16),
            pltpu.VMEM((pieces, rpart, half_cols), BF16),
            dma((9,)),
        ]
        + [dma((4 * chips,))] * 12
        + [dma((links * pieces,))] * 2,
        compiler_params=pltpu.CompilerParams(
            collective_id=0, has_side_effects=True, vmem_limit_bytes=64 * 1024 * 1024 - 128 * 1024
        ),
    )(hidden, w_query, w_key, w_value, w_out, *vectors, *tables)
    if exchange:
        return result
    return lax.psum_scatter(result, "head", scatter_dimension=0, tiled=True)


def solution(mesh):
    in_specs = (
        P("seq", None),
        P(),
        P("seq", "head"),
        P("seq", "head"),
        P("seq", "head"),
        P("head"),
        P("head"),
        P("head"),
        P("head", "seq"),
    )
    out_specs = P(("seq", "head"), None)
    body = functools.partial(local, mesh.shape["seq"], mesh.shape["head"])
    return jax.shard_map(body, mesh=mesh, in_specs=in_specs, out_specs=out_specs, check_vma=False)
```

```python
import functools

import jax
import jax.numpy as jnp
import numpy as np
from jax import lax
from jax.experimental import pallas as pl
from jax.experimental.pallas import tpu as pltpu
from jax.sharding import PartitionSpec as P

HEAD_DIM = 128
ROPE_BASE = 1000000.0
EPSILON = 1e-06
MESH = pl.DeviceIdType.MESH
F32 = jnp.float32
BF16 = jnp.bfloat16
OPS = (5, 0, 1, 1, 3)
PIECES = (2, 2, 2)
STACK = 2
VMEM_LIMIT = 64 * 1024 * 1024 - 4096 * 1024


def kernel(
    n, groups, exchange,
    hidden, w_query, w_key, w_value, w_out, gain, bias_query, bias_key, bias_value,
    near_cos, near_sin, far_cos, far_sin,
    out,
    hid, w_all, wo_all, acc, kv_all, q_ref, high, total, mixed, att, ts, tr, tm,
    load_sem, ws, wr, wps, wpr, os_, or_, ops, opr, ks, kr, kps, kpr, ys, yr,
):
    chips = n // 2
    depth = chips // 2
    me = lax.axis_index("seq")
    group = lax.axis_index("head")
    core = me % 2
    chip = me // 2
    ring = chip // 2 + (chip % 2) * (2 * depth - 1 - 2 * (chip // 2))

    def device_at(position, which):
        position = (position + 2 * chips) % chips
        side = position // depth
        row = position + side * (2 * depth - 1 - 2 * position)
        return 2 * (2 * row + side) + which

    right = device_at(ring + 1, core)
    left = device_at(ring - 1, core)
    partner = 2 * chip + (1 - core)
    neighbours = (right, left)

    def source_at(direction, offset, which):
        return device_at(ring - offset if direction == 0 else ring + offset, which)

    rows, width = hidden.shape
    half_depth = w_query.shape[0] // 2
    q_cols = w_query.shape[1]
    heads = q_cols // HEAD_DIM
    half_cols = w_out.shape[1] // 2
    rh = rows // groups

    loads = []
    late = [pltpu.make_async_copy(hidden, hid, load_sem.at[0])]
    for h in range(2):
        span = pl.ds(h * half_depth, half_depth)
        slot = w_all.at[2 * me + h]
        loads.append(pltpu.make_async_copy(w_query.at[span], slot.at[:, pl.ds(0, q_cols)], load_sem.at[1 + 4 * h]))
        loads.append(pltpu.make_async_copy(w_key.at[span], slot.at[:, pl.ds(q_cols, HEAD_DIM)], load_sem.at[2 + 4 * h]))
        loads.append(pltpu.make_async_copy(w_value.at[span], slot.at[:, pl.ds(q_cols + HEAD_DIM, HEAD_DIM)], load_sem.at[3 + 4 * h]))
        late.append(pltpu.make_async_copy(w_out.at[:, pl.ds(h * half_cols, half_cols)], wo_all.at[2 * me + h], load_sem.at[4 + 4 * h]))
    for copy in loads + late:
        copy.start()

    barrier = pltpu.get_barrier_semaphore()
    for device in (right, left, partner):
        pl.semaphore_signal(barrier, inc=1, device_id={"seq": device}, device_id_type=MESH)
    peers = range(1, groups) if exchange else ()
    for p in peers:
        pl.semaphore_signal(barrier, inc=1, device_id={"head": (group + p) % groups}, device_id_type=MESH)
    pl.semaphore_wait(barrier, 3 + len(peers))

    def remote(ref, send, recv, key, device):
        return pltpu.make_async_remote_copy(
            src_ref=ref, dst_ref=ref, send_sem=send.at[key], recv_sem=recv.at[key],
            device_id={"seq": device}, device_id_type=MESH,
        )

    def piece(buffer, index, j):
        size = buffer.shape[1] // 2
        return buffer.at[index, pl.ds(j * size, size)]

    def key_of(direction, step, j):
        return (direction * chips + step) * 2 + j

    def ring_begin(buffer, sems):
        ss, rs, pss, prs = sems
        for j in range(2):
            for d in range(2):
                own = piece(buffer, 2 * me + d, j)
                remote(own, ss, rs, key_of(d, 0, j), neighbours[d]).start()
        for j in range(2):
            for d in range(2):
                own = piece(buffer, 2 * me + d, j)
                remote(own, pss, prs, key_of(d, chips - 1, j), partner).start()

    def ring_advance(buffer, sems, t):
        ss, rs, pss, prs = sems

        @pl.when(t < chips - 1)
        def _():
            for j in range(2):
                for d in range(2):
                    block = piece(buffer, 2 * source_at(d, t + 1, core) + d, j)
                    remote(block, ss, rs, key_of(d, t, j), neighbours[d]).wait_recv()

                    @pl.when(t < chips - 2)
                    def _():
                        remote(block, ss, rs, key_of(d, t + 1, j), neighbours[d]).start()

                    remote(block, pss, prs, key_of(d, t, j), partner).start()

    def partner_wait(buffer, sems, t):
        ss, rs, pss, prs = sems
        for j in range(2):
            for d in range(2):
                block = piece(buffer, 2 * source_at(d, t, 1 - core) + d, j)
                remote(block, pss, prs, key_of(d, (t + chips - 1) % chips, j), partner).wait_recv()

    def ring_drain(buffer, sems):
        ss, rs, pss, prs = sems

        def body(t, carry):
            for j in range(2):
                for d in range(2):
                    block = piece(buffer, 2 * me + d, j)

                    @pl.when(t < chips - 1)
                    def _():
                        remote(block, ss, rs, key_of(d, t, j), neighbours[d]).wait_send()

                    remote(block, pss, prs, key_of(d, t, j), partner).wait_send()
            return carry

        lax.fori_loop(0, chips, body, 0)

    w_sems = (ws, wr, wps, wpr)
    o_sems = (os_, or_, ops, opr)

    for copy in loads:
        copy.wait()
    ring_begin(w_all, w_sems)
    for copy in late:
        copy.wait()
    slices = 2 * n
    step_cols = width // slices

    def columns(i):
        return pl.ds(pl.multiple_of(i * step_cols, step_cols), step_cols)

    def square(i, carry):
        x = hid[:, columns(i)].astype(F32)
        return carry + x * x

    squares = lax.fori_loop(0, slices, square, jnp.zeros((rows, step_cols), F32))
    inverse = lax.rsqrt(jnp.sum(squares, axis=-1, keepdims=True) * (1.0 / width) + EPSILON)

    def normed(i):
        scaled = hid[:, columns(i)].astype(F32) * inverse * gain[:, columns(i)].astype(F32)
        return scaled.astype(BF16)

    bias = (bias_query, bias_key, bias_value)
    starts = (0, q_cols, q_cols + HEAD_DIM)
    for start, part in zip(starts, bias):
        span = pl.ds(start, part.shape[1])
        acc[:, span] = jnp.broadcast_to(part[...].astype(F32), (rows, part.shape[1]))

    def project(t, carry):
        ring_advance(w_all, w_sems, t)
        partner_wait(w_all, w_sems, t)
        for d in range(2):
            i = 2 * source_at(d, t, core) + d
            k = 2 * source_at(d, t, 1 - core) + d
            acc[...] += jnp.dot(normed(i), w_all[i], preferred_element_type=F32) + jnp.dot(
                normed(k), w_all[k], preferred_element_type=F32
            )
        return carry

    lax.fori_loop(0, chips, project, 0)

    block_cos, block_sin = far_cos[me], far_sin[me]
    cosine = near_cos[...] * block_cos - near_sin[...] * block_sin
    lane = lax.broadcasted_iota(jnp.int32, cosine.shape, 1)
    sine = near_sin[...] * block_cos + near_cos[...] * block_sin
    sine = jnp.where(lane < HEAD_DIM // 2, -sine, sine)

    def rotary(x):
        return x * cosine + pltpu.roll(x, HEAD_DIM // 2, 1) * sine

    def kv_rows(which):
        return pl.ds(pl.multiple_of(which * rows, rows), rows)

    kv_all[chip, kv_rows(core), pl.ds(0, HEAD_DIM)] = rotary(acc[:, pl.ds(q_cols, HEAD_DIM)]).astype(BF16)
    kv_all[chip, kv_rows(core), pl.ds(HEAD_DIM, HEAD_DIM)] = acc[:, pl.ds(q_cols + HEAD_DIM, HEAD_DIM)].astype(BF16)
    for h in range(heads):
        q_ref[h] = rotary(acc[:, pl.ds(h * HEAD_DIM, HEAD_DIM)]).astype(BF16)

    reach = (chips // 2, chips - 1 - chips // 2)

    parts = 2 if rows % 32 == 0 else 1
    piece_rows = rows // parts

    def kv_copy(owner, ss, rs, direction, step, j, device):
        start = pl.multiple_of((owner % 2) * rows + j * piece_rows, piece_rows)
        block = kv_all.at[owner // 2, pl.ds(start, piece_rows)]
        return remote(block, ss, rs, key_of(direction, step, j), device)

    for j in range(parts):
        for d in range(2):
            kv_copy(me, ks, kr, d, 0, j, neighbours[d]).start()
        kv_copy(me, kps, kpr, 0, chips - 1, j, partner).start()

    factor = HEAD_DIM ** (-0.5) * 1.4426950408889634

    def attend(c, own):
        for h in range(heads):
            scores = lax.dot_general(
                q_ref[h], kv_all[c, :, pl.ds(0, HEAD_DIM)], (((1,), (1,)), ((), ())),
                preferred_element_type=F32,
            )
            if own:
                row = lax.broadcasted_iota(jnp.int32, scores.shape, 0) + core * rows
                col = lax.broadcasted_iota(jnp.int32, scores.shape, 1)
                scores = jnp.where(row >= col, scores, -jnp.inf)
            top = jnp.max(scores, axis=-1, keepdims=True)
            if not own:
                old = high[h]
                top = jnp.maximum(old, top)
            probs = jnp.exp2((scores - top) * factor)
            part = jnp.sum(probs, axis=-1, keepdims=True)
            product = jnp.dot(
                probs.astype(BF16), kv_all[c, :, pl.ds(HEAD_DIM, HEAD_DIM)], preferred_element_type=F32
            )
            if not own:
                shrink = jnp.exp2((old - top) * factor)
                part = part + total[h] * shrink
                product = product + mixed[h] * shrink
            high[h] = top
            total[h] = part
            mixed[h] = product

    for j in range(parts):
        kv_copy(partner, kps, kpr, 0, chips - 1, j, partner).wait_recv()
    attend(chip, True)

    def attention(t, carry):
        for j in range(parts):
            for d in range(2):
                @pl.when(t < reach[d])
                def _():
                    owner = source_at(d, t + 1, core)
                    kv_copy(owner, ks, kr, d, t, j, neighbours[d]).wait_recv()

                    @pl.when(t + 1 < reach[d])
                    def _():
                        kv_copy(owner, ks, kr, d, t + 1, j, neighbours[d]).start()

                    kv_copy(owner, kps, kpr, d, t, j, partner).start()

        @pl.when(t == reach[0] - 1)
        def _():
            ring_begin(wo_all, o_sems)

        for d in range(2):
            @pl.when((t > 0) & (t <= reach[d]))
            def _():
                owner = source_at(d, t, 1 - core)
                for j in range(parts):
                    kv_copy(owner, kps, kpr, d, t - 1, j, partner).wait_recv()

                @pl.when(owner // 2 < chip)
                def _():
                    attend(owner // 2, False)
        return carry

    lax.fori_loop(0, reach[0] + 1, attention, 0)
    for h in range(heads):
        att[:, pl.ds(h * HEAD_DIM, HEAD_DIM)] = (mixed[h] / total[h]).astype(BF16)

    def term_copy(p, i):
        return pltpu.make_async_remote_copy(
            src_ref=ts.at[p - 1, i], dst_ref=tr.at[p - 1, i],
            send_sem=ys.at[(p - 1) * slices + i], recv_sem=yr.at[(p - 1) * slices + i],
            device_id={"head": (group + p) % groups}, device_id_type=MESH,
        )

    def out_columns(i):
        return pl.ds(pl.multiple_of(i * half_cols, half_cols), half_cols)

    def make_term(i):
        if not exchange:
            out[:, out_columns(i)] = jnp.dot(att[...], wo_all[i], preferred_element_type=F32).astype(BF16)
            return
        for p in peers:
            span = pl.ds(pl.multiple_of(((group + p) % groups) * rh, rh), rh)
            ts[p - 1, i] = jnp.dot(att[span, :], wo_all[i], preferred_element_type=F32).astype(BF16)
            term_copy(p, i).start()
        span = pl.ds(pl.multiple_of(group * rh, rh), rh)
        tm[i] = jnp.dot(att[span, :], wo_all[i], preferred_element_type=F32).astype(BF16)

    def blocks_of(t):
        return [2 * source_at(d, t, which) + d for d in range(2) for which in (core, 1 - core)]

    def finish(t, carry):
        for i in blocks_of(t):
            value = tm[i].astype(F32)
            for p in peers:
                term_copy(p, i).wait_recv()
                value = value + tr[p - 1, i].astype(F32)
            out[:, out_columns(i)] = value.astype(BF16)
        return carry

    lag = 3

    def partner_terms(t):
        partner_wait(wo_all, o_sems, t)
        for d in range(2):
            make_term(2 * source_at(d, t, 1 - core) + d)

    for d in range(2):
        make_term(2 * me + d)
    partner_terms(0)

    def project_out(t, carry):
        ring_advance(wo_all, o_sems, t)

        @pl.when(t < chips - 1)
        def _():
            for d in range(2):
                make_term(2 * source_at(d, t + 1, core) + d)

        @pl.when(t > 0)
        def _():
            partner_terms(t)

        if exchange:
            @pl.when(t >= lag)
            def _():
                finish(t - lag, 0)
        return carry

    lax.fori_loop(0, chips, project_out, 0)

    if exchange:
        lax.fori_loop(chips - lag, chips, finish, 0)

        def sent(i, carry):
            for p in peers:
                term_copy(p, i).wait_send()
            return carry

        lax.fori_loop(0, slices, sent, 0)

    ring_drain(w_all, w_sems)
    ring_drain(wo_all, o_sems)
    for j in range(parts):
        for d in range(2):
            for t in range(reach[d]):
                kv_copy(me, ks, kr, d, t, j, neighbours[d]).wait_send()
                kv_copy(me, kps, kpr, d, t, j, partner).wait_send()
        kv_copy(me, kps, kpr, 0, chips - 1, j, partner).wait_send()


def pair_kernel(
    n, chunks_in, chunks_out, parts,
    hidden, w_query, w_key, w_value, w_out, *rest_refs,
):
    small = rest_refs[:8]
    out = rest_refs[8]
    held = rest_refs[9:17]
    gain, bias_query, bias_key, bias_value, near_cos, near_sin, far_cos, far_sin = held
    (
    gains, small_sem, hid, w_all, w_second, wo, acc, kv_all, q_ref, high, total, mixed, att, terms, wo_own,
    own_s, own_r, load_sem, swap_s, swap_r, att_s, att_r, ys, yr,
    ws, wr, wps, wpr, os_, or_, ops, opr, ks, kr, kps, kpr, ss, sr, sps, spr,
    ) = rest_refs[17:]
    chips = n // 2
    depth = chips // 2
    ops_from, ops_first, ops_busy, ops_calm, ops_gap = OPS
    stack = STACK
    me = lax.axis_index("seq")
    group = lax.axis_index("head")
    peer = 1 - group
    core = me % 2
    chip = me // 2
    ring = chip // 2 + (chip % 2) * (2 * depth - 1 - 2 * (chip // 2))

    def device_at(position, which):
        position = (position + 2 * chips) % chips
        side = position // depth
        row = position + side * (2 * depth - 1 - 2 * position)
        return 2 * (2 * row + side) + which

    right = device_at(ring + 1, core)
    left = device_at(ring - 1, core)
    partner = 2 * chip + (1 - core)
    neighbours = (right, left)

    def source_at(direction, offset, which):
        return device_at(ring - offset if direction == 0 else ring + offset, which)

    rows, width = hidden.shape
    half_depth = w_query.shape[0] // 2
    q_cols = w_query.shape[1]
    heads = q_cols // HEAD_DIM
    early = heads // 2
    q_early = early * HEAD_DIM
    first_cols = 2 * HEAD_DIM + q_early
    out_depth = w_out.shape[0]
    group_cols = w_out.shape[1] // 2
    lane_cols = group_cols // 2
    rh = rows // 2

    def remote(ref, send, recv, key, device):
        return pltpu.make_async_remote_copy(
            src_ref=ref, dst_ref=ref, send_sem=send.at[key], recv_sem=recv.at[key],
            device_id={"seq": device}, device_id_type=MESH,
        )

    def lanes(which):
        return pl.ds(pl.multiple_of(which * lane_cols, lane_cols), lane_cols)

    def wo_lanes(which, d):
        start = which * group_cols + d * lane_cols
        return pl.ds(pl.multiple_of(start, lane_cols), lane_cols)

    def group_rows(which):
        return pl.ds(pl.multiple_of(which * out_depth, out_depth), out_depth)

    loads, last = [], []
    for h in range(2):
        span = pl.ds(h * half_depth, half_depth)
        slot = w_all.at[2 * me + h]
        loads.append((w_key.at[span], slot.at[:, pl.ds(0, HEAD_DIM)]))
        loads.append((w_value.at[span], slot.at[:, pl.ds(HEAD_DIM, HEAD_DIM)]))
        loads.append((w_query.at[span, pl.ds(0, q_early)], slot.at[:, pl.ds(2 * HEAD_DIM, q_early)]))
        last.append((w_query.at[span, pl.ds(q_early, q_cols - q_early)], w_second.at[2 * me + h]))
        last.append((w_out.at[:, wo_lanes(group, h)], wo.at[chip, h, group_rows(group), lanes(core)]))
        last.append((w_out.at[:, wo_lanes(peer, h)], wo_own.at[h, group_rows(group), lanes(core)]))
    copies = [pltpu.make_async_copy(a, b, load_sem.at[i]) for i, (a, b) in enumerate(loads + [(hidden, hid)] + last)]
    small_copies = [pltpu.make_async_copy(a, b, small_sem.at[i]) for i, (a, b) in enumerate(zip(small, held))]
    for copy in copies[: len(loads)]:
        copy.start()

    barrier = pltpu.get_barrier_semaphore()
    for device in (right, left, partner):
        pl.semaphore_signal(barrier, inc=1, device_id={"seq": device}, device_id_type=MESH)
    pl.semaphore_signal(barrier, inc=1, device_id={"head": peer}, device_id_type=MESH)
    pl.semaphore_wait(barrier, 4)

    def across(src, dst, send, recv, key):
        return pltpu.make_async_remote_copy(
            src_ref=src, dst_ref=dst, send_sem=send.at[key], recv_sem=recv.at[key],
            device_id={"head": peer}, device_id_type=MESH,
        )

    def swap(d):
        return across(
            w_out.at[:, wo_lanes(peer, d)], wo.at[chip, d, group_rows(group), lanes(core)], swap_s, swap_r, d
        )

    def swap_own(d):
        return across(
            w_out.at[:, wo_lanes(group, d)], wo_own.at[d, group_rows(group), lanes(core)], swap_s, swap_r, 2 + d
        )

    def own_copy(d, which):
        return remote(wo_own.at[d, :, lanes(which)], own_s, own_r, d, partner)

    class Ring:
        def __init__(self, view, sems, pieces):
            self.view, self.sems, self.pieces = view, sems, pieces

        def key(self, d, step, j):
            return (d * chips + step) * self.pieces + j

        def begin(self, j):
            send, recv, psend, precv = self.sems
            for d in range(2):
                own = self.view(me, d, j)
                remote(own, send, recv, self.key(d, 0, j), neighbours[d]).start()
            for d in range(2):
                own = self.view(me, d, j)
                remote(own, psend, precv, self.key(d, chips - 1, j), partner).start()

        def advance(self, t, j):
            send, recv, psend, precv = self.sems
            for d in range(2):
                block = self.view(source_at(d, t + 1, core), d, j)
                remote(block, send, recv, self.key(d, t, j), neighbours[d]).wait_recv()

                @pl.when(t < chips - 2)
                def _():
                    remote(block, send, recv, self.key(d, t + 1, j), neighbours[d]).start()

                remote(block, psend, precv, self.key(d, t, j), partner).start()

        def op(self, index):
            @pl.when(index < self.pieces)
            def _():
                self.begin(index)

            @pl.when((index >= self.pieces) & (index < self.pieces * chips))
            def _():
                done = index - self.pieces
                self.advance(done // self.pieces, done % self.pieces)

        def partner_wait(self, t, some=None):
            send, recv, psend, precv = self.sems
            for j in range(self.pieces) if some is None else some:
                for d in range(2):
                    block = self.view(source_at(d, t, 1 - core), d, j)
                    remote(block, psend, precv, self.key(d, (t + chips - 1) % chips, j), partner).wait_recv()

        def drain(self):
            send, recv, psend, precv = self.sems

            def body(t, carry):
                for j in range(self.pieces):
                    for d in range(2):
                        block = self.view(me, d, j)

                        @pl.when(t < chips - 1)
                        def _():
                            remote(block, send, recv, self.key(d, t, j), neighbours[d]).wait_send()

                        remote(block, psend, precv, self.key(d, t, j), partner).wait_send()
                return carry

            lax.fori_loop(0, chips, body, 0)

    def rows_view(buffer, pieces):
        size = buffer.shape[1] // pieces
        return lambda owner, d, j: buffer.at[2 * owner + d, pl.ds(pl.multiple_of(j * size, size), size)]

    def wo_view(owner, d, j):
        size = wo.shape[2] // chunks_out
        return wo.at[owner // 2, d, pl.ds(pl.multiple_of(j * size, size), size), lanes(owner % 2)]

    first = Ring(rows_view(w_all, chunks_in), (ws, wr, wps, wpr), chunks_in)
    third = Ring(wo_view, (os_, or_, ops, opr), chunks_out)

    for copy in copies[: len(loads)]:
        copy.wait()
    for j in range(chunks_in):
        first.begin(j)
    for d in range(2):
        swap(d).start()
    for d in range(2):
        swap_own(d).start()
    for copy in copies[len(loads):] + small_copies:
        copy.start()
    for copy in copies[len(loads):]:
        copy.wait()

    for copy in small_copies:
        copy.wait()
    gains[...] = gain[...].astype(F32)

    slices = 2 * n
    step_cols = width // slices
    gain_rows = step_cols // HEAD_DIM

    def columns(i):
        return pl.ds(pl.multiple_of(i * step_cols, step_cols), step_cols)

    def square(i, carry):
        x = hid[:, columns(i)].astype(F32)
        return carry + x * x

    squares = lax.fori_loop(0, slices, square, jnp.zeros((rows, step_cols), F32))
    inverse = lax.rsqrt(jnp.sum(squares, axis=-1, keepdims=True) * (1.0 / width) + EPSILON)

    def normed(i):
        line = jnp.concatenate([gains[pl.ds(i * gain_rows + r, 1), :] for r in range(gain_rows)], axis=1)
        scaled = hid[:, columns(i)].astype(F32) * inverse * line
        value = scaled.astype(BF16)
        hid[:, columns(i)] = value
        return value

    def widen(line):
        return jnp.broadcast_to(line.astype(F32), (rows, HEAD_DIM))

    acc[:, pl.ds(0, HEAD_DIM)] = widen(bias_key[...])
    acc[:, pl.ds(HEAD_DIM, HEAD_DIM)] = widen(bias_value[...])
    lines = bias_query[...].astype(F32)
    for h in range(heads):
        acc[:, pl.ds((2 + h) * HEAD_DIM, HEAD_DIM)] = widen(lines[h : h + 1])

    far_steps = chips // 2
    reach = [[far_steps - (j * 2 // parts != d) for j in range(parts)] for d in range(2)]

    def second_copy(owner, send, recv, direction, step, j, device):
        return remote(w_second.at[2 * owner + j], send, recv, (direction * chips + step) * 2 + j, device)

    def second_begin():
        for j in range(2):
            for d in range(2):
                second_copy(me, ss, sr, d, 0, j, neighbours[d]).start()
        for j in range(2):
            second_copy(me, sps, spr, 0, chips - 1, j, partner).start()

    def second_advance(t):
        for j in range(2):
            for d in range(2):
                @pl.when(t < reach[d][j])
                def _():
                    owner = source_at(d, t + 1, core)
                    second_copy(owner, ss, sr, d, t, j, neighbours[d]).wait_recv()

                    @pl.when(t + 1 < reach[d][j])
                    def _():
                        second_copy(owner, ss, sr, d, t + 1, j, neighbours[d]).start()

                    second_copy(owner, sps, spr, d, t, j, partner).start()

    def project(t, carry):
        @pl.when(t < chips - 1)
        def _():
            for j in range(chunks_in):
                first.advance(t, j)

        @pl.when(t == chips - 3)
        def _():
            second_begin()

        @pl.when(t == ops_from)
        def _():
            for d in range(2):
                swap(d).wait_recv()

        @pl.when(t == chips // 2)
        def _():
            for d in range(2):
                swap_own(d).wait_recv()
                own_copy(d, core).start()

        @pl.when((t >= ops_from) & (t < ops_from + ops_first))
        def _():
            third.op(t - ops_from)

        first.partner_wait(t)
        for d in range(2):
            i = 2 * source_at(d, t, core) + d
            k = 2 * source_at(d, t, 1 - core) + d
            acc[:, pl.ds(0, first_cols)] += jnp.dot(normed(i), w_all[i], preferred_element_type=F32) + jnp.dot(
                normed(k), w_all[k], preferred_element_type=F32
            )
        return carry

    lax.fori_loop(0, chips, project, 0)

    block_cos, block_sin = far_cos[me], far_sin[me]
    cosine = near_cos[...] * block_cos - near_sin[...] * block_sin
    lane = lax.broadcasted_iota(jnp.int32, cosine.shape, 1)
    sine = near_sin[...] * block_cos + near_cos[...] * block_sin
    sine = jnp.where(lane < HEAD_DIM // 2, -sine, sine)

    def rotary(x):
        return x * cosine + pltpu.roll(x, HEAD_DIM // 2, 1) * sine

    def kv_rows(which):
        return pl.ds(pl.multiple_of(which * rows, rows), rows)

    kv_all[chip, kv_rows(core), pl.ds(0, HEAD_DIM)] = rotary(acc[:, pl.ds(0, HEAD_DIM)]).astype(BF16)
    kv_all[chip, kv_rows(core), pl.ds(HEAD_DIM, HEAD_DIM)] = acc[:, pl.ds(HEAD_DIM, HEAD_DIM)].astype(BF16)
    def turn(h):
        q_ref[pl.ds(h * rows, rows), :] = rotary(acc[:, pl.ds((2 + h) * HEAD_DIM, HEAD_DIM)]).astype(BF16)

    turn(0)
    piece_rows = rows // parts

    def kv_copy(owner, send, recv, direction, step, j, device):
        start = pl.multiple_of((owner % 2) * rows + j * piece_rows, piece_rows)
        block = kv_all.at[owner // 2, pl.ds(start, piece_rows)]
        return remote(block, send, recv, (direction * chips + step) * parts + j, device)

    for j in range(parts):
        for d in range(2):
            kv_copy(me, ks, kr, d, 0, j, neighbours[d]).start()
        kv_copy(me, kps, kpr, 0, chips - 1, j, partner).start()
    second_advance(0)
    for h in range(1, early):
        turn(h)

    factor = HEAD_DIM ** (-0.5) * 1.4426950408889634

    def attend(c, own, which):
        for h in range(which[0], which[1], stack):
            some = pl.ds(h * rows, stack * rows)
            scores = lax.dot_general(
                q_ref[some, :], kv_all[c, :, pl.ds(0, HEAD_DIM)], (((1,), (1,)), ((), ())),
                preferred_element_type=F32,
            )
            if own:
                row = lax.broadcasted_iota(jnp.int32, scores.shape, 0) % rows + core * rows
                col = lax.broadcasted_iota(jnp.int32, scores.shape, 1)
                scores = jnp.where(row >= col, scores, -jnp.inf)
            top = jnp.max(scores, axis=-1, keepdims=True)
            if not own:
                old = high[some, :]
                top = jnp.maximum(old, top)
            probs = jnp.exp2((scores - top) * factor)
            part = jnp.sum(probs, axis=-1, keepdims=True)
            product = jnp.dot(
                probs.astype(BF16), kv_all[c, :, pl.ds(HEAD_DIM, HEAD_DIM)], preferred_element_type=F32
            )
            if not own:
                shrink = jnp.exp2((old - top) * factor)
                part = part + total[some, :] * shrink
                product = product + mixed[some, :] * shrink
            high[some, :] = top
            total[some, :] = part
            mixed[some, :] = product

    for j in range(parts):
        kv_copy(partner, kps, kpr, 0, chips - 1, j, partner).wait_recv()
    attend(chip, True, (0, early))

    busy_steps = far_steps - 1

    def project_second(c):
        total_part = None
        for which in range(2):
            for j in range(2):
                k = 2 * (2 * c + which) + j
                value = jnp.dot(hid[:, columns(k)], w_second[k], preferred_element_type=F32)
                total_part = value if total_part is None else total_part + value
        acc[:, pl.ds(first_cols, q_cols - q_early)] += total_part

    def attention(t, carry):
        second_advance(t + 1)
        for j in range(parts):
            for d in range(2):
                @pl.when(t < reach[d][j])
                def _():
                    owner = source_at(d, t + 1, core)
                    kv_copy(owner, ks, kr, d, t, j, neighbours[d]).wait_recv()

                    @pl.when(t + 1 < reach[d][j])
                    def _():
                        kv_copy(owner, ks, kr, d, t + 1, j, neighbours[d]).start()

                    kv_copy(owner, kps, kpr, d, t, j, partner).start()

        for k in range(max(ops_busy, ops_calm)):
            index = ops_first + ops_busy * jnp.minimum(t, busy_steps) + ops_calm * jnp.maximum(t - busy_steps, 0) + k

            @pl.when(((t < busy_steps) & (k < ops_busy)) | ((t >= busy_steps) & (k < ops_calm)))
            def _():
                third.op(index)

        for j in range(parts):
            for d in range(2):
                @pl.when((t > 0) & (t <= reach[d][j]))
                def _():
                    owner = source_at(d, t, 1 - core)
                    kv_copy(owner, kps, kpr, d, t - 1, j, partner).wait_recv()
                    second_copy(owner, sps, spr, d, t - 1, j, partner).wait_recv()

        @pl.when(t == 0)
        def _():
            for j in range(2):
                second_copy(partner, sps, spr, 0, chips - 1, j, partner).wait_recv()

        for d in range(2):
            other = source_at(d, t, core) // 2

            @pl.when((t > 0) & (t <= far_steps - d) & (other < chip))
            def _():
                attend(other, False, (0, early))

            @pl.when(((t > 0) | (d == 0)) & (t <= far_steps - d))
            def _():
                project_second(other)
        return carry

    lax.fori_loop(0, far_steps + 1, attention, 0)
    ops_middle = ops_first + ops_busy * busy_steps + ops_calm * (far_steps + 1 - busy_steps)
    ops_done = ops_middle + (chips + ops_gap - 1) // ops_gap
    for h in range(early, heads):
        turn(h)
    attend(chip, True, (early, heads))

    def attention_rest(c, carry):
        @pl.when(c % ops_gap == 0)
        def _():
            third.op(ops_middle + c // ops_gap)

        @pl.when(c < chip)
        def _():
            attend(c, False, (early, heads))
        return carry

    lax.fori_loop(0, chips, attention_rest, 0)

    def row_span(which):
        return pl.ds(pl.multiple_of(which * rh, rh), rh)

    def att_copy(key):
        ref = att.at[group, row_span((group + key) % 2), :]
        return across(ref, ref, att_s, att_r, key)

    for h in range(heads):
        att[group, :, pl.ds(h * HEAD_DIM, HEAD_DIM)] = (
            mixed[pl.ds(h * rows, rows), :] / total[pl.ds(h * rows, rows), :]
        ).astype(BF16)
    for key in range(2):
        att_copy(key).start()

    def out_span(c, d, which):
        start = (2 * c + which) * 2 * group_cols + group * group_cols + d * lane_cols
        return pl.ds(pl.multiple_of(start, lane_cols), lane_cols)

    def term_copy(c, d, which):
        src = terms.at[c, d, :, pl.ds(which * lane_cols, lane_cols)]
        return across(src, out.at[:, out_span(c, d, which)], ys, yr, (2 * c + d) * 2 + which)

    def part(weights, which, g):
        return jnp.dot(
            att[g, row_span(which), :], weights[pl.ds(g * out_depth, out_depth), :], preferred_element_type=F32
        ).astype(BF16).astype(F32)

    def product(weights, which):
        return (part(weights, which, 0) + part(weights, which, 1)).astype(BF16)

    def send_terms(c, d, value):
        terms[c, d] = value
        for which in range(2):
            term_copy(c, d, which).start()

    def give(t, d):
        c = source_at(d, t, core) // 2
        send_terms(c, d, product(wo.at[c, d], peer))

    def put(c, d, owner, value):
        for which in range(2):
            start = (2 * c + which) * 2 * group_cols + owner * group_cols + d * lane_cols
            span = pl.ds(pl.multiple_of(start, lane_cols), lane_cols)
            out[:, span] = value[:, which * lane_cols : (which + 1) * lane_cols]

    def keep(t, d):
        c = source_at(d, t, core) // 2
        put(c, d, group, product(wo.at[c, d], group))

    def keep_own(d):
        put(chip, d, group, product(wo.at[chip, d], group))
        put(chip, d, peer, product(wo_own.at[d], group))

    third.partner_wait(0)

    def project_out(t, carry):
        third.partner_wait(t)

        @pl.when(t == 1)
        def _():
            att_copy(0).wait_recv()

        def move(j):
            @pl.when((t + 1) * chunks_out + j >= ops_done)
            def _():
                third.advance(t, j)

        for j in range(chunks_out - 1):
            move(j)
        for d in range(2):
            give(t, d)

        @pl.when(t == 1)
        def _():
            att_copy(1).wait_recv()

        for d in range(2):
            keep(t, d)
        move(chunks_out - 1)

        @pl.when(t == chips // 2)
        def _():
            for d in range(2):
                own_copy(d, 1 - core).wait_recv()
                keep_own(d)
        return carry

    for j in range(chunks_out):
        if chunks_out + j >= ops_done:
            third.advance(0, j)
    lax.fori_loop(1, chips - 1, project_out, 0)
    final = chips - 1
    held_parts = []
    for j in range(chunks_out):
        third.partner_wait(final, (j,))
        for d in range(2):
            held_parts.append(part(wo.at[source_at(d, final, core) // 2, d], peer, j))
    for d in range(2):
        send_terms(source_at(d, final, core) // 2, d, (held_parts[d] + held_parts[2 + d]).astype(BF16))
    for d in range(2):
        keep(final, d)


    first.drain()
    third.drain()
    for j in range(parts):
        for d in range(2):
            for t in range(reach[d][j]):
                kv_copy(me, ks, kr, d, t, j, neighbours[d]).wait_send()
                kv_copy(me, kps, kpr, d, t, j, partner).wait_send()
                second_copy(me, ss, sr, d, t, j, neighbours[d]).wait_send()
                second_copy(me, sps, spr, d, t, j, partner).wait_send()
        kv_copy(me, kps, kpr, 0, chips - 1, j, partner).wait_send()
        second_copy(me, sps, spr, 0, chips - 1, j, partner).wait_send()
    for d in range(2):
        swap(d).wait_send()
        swap_own(d).wait_send()
        own_copy(d, core).wait_send()
    for key in range(2):
        att_copy(key).wait_send()

    def finish(c, carry):
        @pl.when(c != chip)
        def _():
            for d in range(2):
                for which in range(2):
                    term_copy(c, d, which).wait_send()
                    term_copy(c, d, which).wait_recv()
        return carry

    lax.fori_loop(0, chips, finish, 0)


def tables_of(n, rows):
    freq = ROPE_BASE ** (-2.0 * np.arange(HEAD_DIM // 2, dtype=np.float64) / HEAD_DIM)
    freq = np.concatenate([freq, freq])
    near = np.arange(rows, dtype=np.float64)[:, None] * freq
    far = (np.arange(n, dtype=np.float64) * rows)[:, None, None] * freq
    return [f(a).astype(np.float32) for a in (near, far) for f in (np.cos, np.sin)]


def pair_local(n, hidden, norm_gain, w_query, w_key, w_value, bias_query, bias_key, bias_value, w_out):
    rows, width = hidden.shape
    cols = w_query.shape[1]
    heads = cols // HEAD_DIM
    early = heads // 2 * HEAD_DIM
    chips = n // 2
    slices = 2 * n
    half_depth = w_query.shape[0] // 2
    group_cols = w_out.shape[1] // 2
    chunks_in, chunks_out, parts = PIECES
    vectors = [v.reshape(-1, HEAD_DIM) for v in (norm_gain, bias_query, bias_key, bias_value)]
    small = vectors + tables_of(n, rows)
    result = jax.ShapeDtypeStruct((rows // 2, w_out.shape[1] * n), BF16)
    any_spec = pl.BlockSpec(memory_space=pl.ANY)
    dma = pltpu.SemaphoreType.DMA
    return pl.pallas_call(
        functools.partial(pair_kernel, n, chunks_in, chunks_out, parts),
        out_shape=pltpu.VMEM(result.shape, result.dtype),
        in_specs=[any_spec] * 13,
        out_specs=pl.BlockSpec(memory_space=pltpu.VMEM),
        scratch_shapes=[pltpu.VMEM(a.shape, a.dtype) for a in small]
        + [
            pltpu.VMEM((width // HEAD_DIM, HEAD_DIM), F32),
            dma((8,)),
            pltpu.VMEM((rows, width), BF16),
            pltpu.VMEM((slices, half_depth, 2 * HEAD_DIM + early), BF16),
            pltpu.VMEM((slices, half_depth, cols - early), BF16),
            pltpu.VMEM((chips, 2, 2 * w_out.shape[0], group_cols), BF16),
            pltpu.VMEM((rows, 2 * HEAD_DIM + cols), F32),
            pltpu.VMEM((chips, 2 * rows, 2 * HEAD_DIM), BF16),
            pltpu.VMEM((heads * rows, HEAD_DIM), BF16),
            pltpu.VMEM((heads * rows, 1), F32),
            pltpu.VMEM((heads * rows, 1), F32),
            pltpu.VMEM((heads * rows, HEAD_DIM), F32),
            pltpu.VMEM((2, rows, cols), BF16),
            pltpu.VMEM((chips, 2, rows // 2, group_cols), BF16),
            pltpu.VMEM((2, 2 * w_out.shape[0], group_cols), BF16),
            dma((2,)), dma((2,)),
            dma((13,)),
            dma((4,)), dma((4,)), dma((2,)), dma((2,)),
            dma((4 * chips,)), dma((4 * chips,)),
        ]
        + [dma((2 * chips * chunks_in,))] * 4
        + [dma((2 * chips * chunks_out,))] * 4
        + [dma((2 * chips * parts,))] * 4
        + [dma((4 * chips,))] * 4,
        compiler_params=pltpu.CompilerParams(
            collective_id=0, has_side_effects=True, vmem_limit_bytes=VMEM_LIMIT - 2 * result.size
        ),
    )(hidden, w_query, w_key, w_value, w_out, *small)


def fits_pair(n, groups, rows, w_query, w_out):
    chips = n // 2
    return (
        groups == 2
        and chips % 4 == 0
        and rows % 32 == 0
        and w_query.shape[1] % (4 * HEAD_DIM) == 0
        and w_query.shape[0] % 128 == 0
        and w_out.shape[1] % 512 == 0
    )


def local(n, groups, hidden, norm_gain, w_query, w_key, w_value, bias_query, bias_key, bias_value, w_out):
    rows, width = hidden.shape
    if fits_pair(n, groups, rows, w_query, w_out):
        return pair_local(n, hidden, norm_gain, w_query, w_key, w_value, bias_query, bias_key, bias_value, w_out)
    cols = w_query.shape[1]
    heads = cols // HEAD_DIM
    wide = cols + 2 * HEAD_DIM
    chips = n // 2
    exchange = groups > 1 and (rows // groups) % 16 == 0
    rh = rows // groups
    slices = 2 * n
    half_depth = w_query.shape[0] // 2
    half_cols = w_out.shape[1] // 2

    tables = tables_of(n, rows)
    vectors = [v.reshape(1, -1) for v in (norm_gain, bias_query, bias_key, bias_value)]

    any_spec = pl.BlockSpec(memory_space=pl.ANY)
    vmem = pl.BlockSpec(memory_space=pltpu.VMEM)
    links = max(groups - 1, 1) if exchange else 1
    pieces = slices if exchange else 1
    rpart = rh if exchange else 16
    dma = pltpu.SemaphoreType.DMA
    result = pl.pallas_call(
        functools.partial(kernel, n, groups, exchange),
        out_shape=jax.ShapeDtypeStruct((rh if exchange else rows, w_out.shape[1] * n), BF16),
        in_specs=[any_spec] * 5 + [vmem] * 8,
        out_specs=vmem,
        scratch_shapes=[
            pltpu.VMEM((rows, width), BF16),
            pltpu.VMEM((slices, half_depth, wide), BF16),
            pltpu.VMEM((slices, w_out.shape[0], half_cols), BF16),
            pltpu.VMEM((rows, wide), F32),
            pltpu.VMEM((chips, 2 * rows, 2 * HEAD_DIM), BF16),
            pltpu.VMEM((heads, rows, HEAD_DIM), BF16),
            pltpu.VMEM((heads, rows, 1), F32),
            pltpu.VMEM((heads, rows, 1), F32),
            pltpu.VMEM((heads, rows, HEAD_DIM), F32),
            pltpu.VMEM((rows, cols), BF16),
            pltpu.VMEM((links, pieces, rpart, half_cols), BF16),
            pltpu.VMEM((links, pieces, rpart, half_cols), BF16),
            pltpu.VMEM((pieces, rpart, half_cols), BF16),
            dma((9,)),
        ]
        + [dma((4 * chips,))] * 12
        + [dma((links * pieces,))] * 2,
        compiler_params=pltpu.CompilerParams(
            collective_id=0, has_side_effects=True, vmem_limit_bytes=64 * 1024 * 1024 - 128 * 1024
        ),
    )(hidden, w_query, w_key, w_value, w_out, *vectors, *tables)
    if exchange:
        return result
    return lax.psum_scatter(result, "head", scatter_dimension=0, tiled=True)


def solution(mesh):
    in_specs = (
        P("seq", None),
        P(),
        P("seq", "head"),
        P("seq", "head"),
        P("seq", "head"),
        P("head"),
        P("head"),
        P("head"),
        P("head", "seq"),
    )
    out_specs = P(("seq", "head"), None)
    body = functools.partial(local, mesh.shape["seq"], mesh.shape["head"])
    return jax.shard_map(body, mesh=mesh, in_specs=in_specs, out_specs=out_specs, check_vma=False)
```

```python
import functools

import jax
import jax.numpy as jnp
import numpy as np
from jax import lax
from jax.experimental import pallas as pl
from jax.experimental.pallas import tpu as pltpu
from jax.sharding import PartitionSpec as P

HEAD_DIM = 128
ROPE_BASE = 1000000.0
EPSILON = 1e-06
MESH = pl.DeviceIdType.MESH
F32 = jnp.float32
BF16 = jnp.bfloat16
OPS = (5, 0, 1, 1, 3)
PIECES = (2, 2, 2)
STACK = 2
VMEM_LIMIT = 64 * 1024 * 1024 - 4096 * 1024


def kernel(
    n, groups, exchange,
    hidden, w_query, w_key, w_value, w_out, gain, bias_query, bias_key, bias_value,
    near_cos, near_sin, far_cos, far_sin,
    out,
    hid, w_all, wo_all, acc, kv_all, q_ref, high, total, mixed, att, ts, tr, tm,
    load_sem, ws, wr, wps, wpr, os_, or_, ops, opr, ks, kr, kps, kpr, ys, yr,
):
    chips = n // 2
    depth = chips // 2
    me = lax.axis_index("seq")
    group = lax.axis_index("head")
    core = me % 2
    chip = me // 2
    ring = chip // 2 + (chip % 2) * (2 * depth - 1 - 2 * (chip // 2))

    def device_at(position, which):
        position = (position + 2 * chips) % chips
        side = position // depth
        row = position + side * (2 * depth - 1 - 2 * position)
        return 2 * (2 * row + side) + which

    right = device_at(ring + 1, core)
    left = device_at(ring - 1, core)
    partner = 2 * chip + (1 - core)
    neighbours = (right, left)

    def source_at(direction, offset, which):
        return device_at(ring - offset if direction == 0 else ring + offset, which)

    rows, width = hidden.shape
    half_depth = w_query.shape[0] // 2
    q_cols = w_query.shape[1]
    heads = q_cols // HEAD_DIM
    half_cols = w_out.shape[1] // 2
    rh = rows // groups

    loads = []
    late = [pltpu.make_async_copy(hidden, hid, load_sem.at[0])]
    for h in range(2):
        span = pl.ds(h * half_depth, half_depth)
        slot = w_all.at[2 * me + h]
        loads.append(pltpu.make_async_copy(w_query.at[span], slot.at[:, pl.ds(0, q_cols)], load_sem.at[1 + 4 * h]))
        loads.append(pltpu.make_async_copy(w_key.at[span], slot.at[:, pl.ds(q_cols, HEAD_DIM)], load_sem.at[2 + 4 * h]))
        loads.append(pltpu.make_async_copy(w_value.at[span], slot.at[:, pl.ds(q_cols + HEAD_DIM, HEAD_DIM)], load_sem.at[3 + 4 * h]))
        late.append(pltpu.make_async_copy(w_out.at[:, pl.ds(h * half_cols, half_cols)], wo_all.at[2 * me + h], load_sem.at[4 + 4 * h]))
    for copy in loads + late:
        copy.start()

    barrier = pltpu.get_barrier_semaphore()
    for device in (right, left, partner):
        pl.semaphore_signal(barrier, inc=1, device_id={"seq": device}, device_id_type=MESH)
    peers = range(1, groups) if exchange else ()
    for p in peers:
        pl.semaphore_signal(barrier, inc=1, device_id={"head": (group + p) % groups}, device_id_type=MESH)
    pl.semaphore_wait(barrier, 3 + len(peers))

    def remote(ref, send, recv, key, device):
        return pltpu.make_async_remote_copy(
            src_ref=ref, dst_ref=ref, send_sem=send.at[key], recv_sem=recv.at[key],
            device_id={"seq": device}, device_id_type=MESH,
        )

    def piece(buffer, index, j):
        size = buffer.shape[1] // 2
        return buffer.at[index, pl.ds(j * size, size)]

    def key_of(direction, step, j):
        return (direction * chips + step) * 2 + j

    def ring_begin(buffer, sems):
        ss, rs, pss, prs = sems
        for j in range(2):
            for d in range(2):
                own = piece(buffer, 2 * me + d, j)
                remote(own, ss, rs, key_of(d, 0, j), neighbours[d]).start()
        for j in range(2):
            for d in range(2):
                own = piece(buffer, 2 * me + d, j)
                remote(own, pss, prs, key_of(d, chips - 1, j), partner).start()

    def ring_advance(buffer, sems, t):
        ss, rs, pss, prs = sems

        @pl.when(t < chips - 1)
        def _():
            for j in range(2):
                for d in range(2):
                    block = piece(buffer, 2 * source_at(d, t + 1, core) + d, j)
                    remote(block, ss, rs, key_of(d, t, j), neighbours[d]).wait_recv()

                    @pl.when(t < chips - 2)
                    def _():
                        remote(block, ss, rs, key_of(d, t + 1, j), neighbours[d]).start()

                    remote(block, pss, prs, key_of(d, t, j), partner).start()

    def partner_wait(buffer, sems, t):
        ss, rs, pss, prs = sems
        for j in range(2):
            for d in range(2):
                block = piece(buffer, 2 * source_at(d, t, 1 - core) + d, j)
                remote(block, pss, prs, key_of(d, (t + chips - 1) % chips, j), partner).wait_recv()

    def ring_drain(buffer, sems):
        ss, rs, pss, prs = sems

        def body(t, carry):
            for j in range(2):
                for d in range(2):
                    block = piece(buffer, 2 * me + d, j)

                    @pl.when(t < chips - 1)
                    def _():
                        remote(block, ss, rs, key_of(d, t, j), neighbours[d]).wait_send()

                    remote(block, pss, prs, key_of(d, t, j), partner).wait_send()
            return carry

        lax.fori_loop(0, chips, body, 0)

    w_sems = (ws, wr, wps, wpr)
    o_sems = (os_, or_, ops, opr)

    for copy in loads:
        copy.wait()
    ring_begin(w_all, w_sems)
    for copy in late:
        copy.wait()
    slices = 2 * n
    step_cols = width // slices

    def columns(i):
        return pl.ds(pl.multiple_of(i * step_cols, step_cols), step_cols)

    def square(i, carry):
        x = hid[:, columns(i)].astype(F32)
        return carry + x * x

    squares = lax.fori_loop(0, slices, square, jnp.zeros((rows, step_cols), F32))
    inverse = lax.rsqrt(jnp.sum(squares, axis=-1, keepdims=True) * (1.0 / width) + EPSILON)

    def normed(i):
        scaled = hid[:, columns(i)].astype(F32) * inverse * gain[:, columns(i)].astype(F32)
        return scaled.astype(BF16)

    bias = (bias_query, bias_key, bias_value)
    starts = (0, q_cols, q_cols + HEAD_DIM)
    for start, part in zip(starts, bias):
        span = pl.ds(start, part.shape[1])
        acc[:, span] = jnp.broadcast_to(part[...].astype(F32), (rows, part.shape[1]))

    def project(t, carry):
        ring_advance(w_all, w_sems, t)
        partner_wait(w_all, w_sems, t)
        for d in range(2):
            i = 2 * source_at(d, t, core) + d
            k = 2 * source_at(d, t, 1 - core) + d
            acc[...] += jnp.dot(normed(i), w_all[i], preferred_element_type=F32) + jnp.dot(
                normed(k), w_all[k], preferred_element_type=F32
            )
        return carry

    lax.fori_loop(0, chips, project, 0)

    block_cos, block_sin = far_cos[me], far_sin[me]
    cosine = near_cos[...] * block_cos - near_sin[...] * block_sin
    lane = lax.broadcasted_iota(jnp.int32, cosine.shape, 1)
    sine = near_sin[...] * block_cos + near_cos[...] * block_sin
    sine = jnp.where(lane < HEAD_DIM // 2, -sine, sine)

    def rotary(x):
        return x * cosine + pltpu.roll(x, HEAD_DIM // 2, 1) * sine

    def kv_rows(which):
        return pl.ds(pl.multiple_of(which * rows, rows), rows)

    kv_all[chip, kv_rows(core), pl.ds(0, HEAD_DIM)] = rotary(acc[:, pl.ds(q_cols, HEAD_DIM)]).astype(BF16)
    kv_all[chip, kv_rows(core), pl.ds(HEAD_DIM, HEAD_DIM)] = acc[:, pl.ds(q_cols + HEAD_DIM, HEAD_DIM)].astype(BF16)
    for h in range(heads):
        q_ref[h] = rotary(acc[:, pl.ds(h * HEAD_DIM, HEAD_DIM)]).astype(BF16)

    reach = (chips // 2, chips - 1 - chips // 2)

    parts = 2 if rows % 32 == 0 else 1
    piece_rows = rows // parts

    def kv_copy(owner, ss, rs, direction, step, j, device):
        start = pl.multiple_of((owner % 2) * rows + j * piece_rows, piece_rows)
        block = kv_all.at[owner // 2, pl.ds(start, piece_rows)]
        return remote(block, ss, rs, key_of(direction, step, j), device)

    for j in range(parts):
        for d in range(2):
            kv_copy(me, ks, kr, d, 0, j, neighbours[d]).start()
        kv_copy(me, kps, kpr, 0, chips - 1, j, partner).start()

    factor = HEAD_DIM ** (-0.5) * 1.4426950408889634

    def attend(c, own):
        for h in range(heads):
            scores = lax.dot_general(
                q_ref[h], kv_all[c, :, pl.ds(0, HEAD_DIM)], (((1,), (1,)), ((), ())),
                preferred_element_type=F32,
            )
            if own:
                row = lax.broadcasted_iota(jnp.int32, scores.shape, 0) + core * rows
                col = lax.broadcasted_iota(jnp.int32, scores.shape, 1)
                scores = jnp.where(row >= col, scores, -jnp.inf)
            top = jnp.max(scores, axis=-1, keepdims=True)
            if not own:
                old = high[h]
                top = jnp.maximum(old, top)
            probs = jnp.exp2((scores - top) * factor)
            part = jnp.sum(probs, axis=-1, keepdims=True)
            product = jnp.dot(
                probs.astype(BF16), kv_all[c, :, pl.ds(HEAD_DIM, HEAD_DIM)], preferred_element_type=F32
            )
            if not own:
                shrink = jnp.exp2((old - top) * factor)
                part = part + total[h] * shrink
                product = product + mixed[h] * shrink
            high[h] = top
            total[h] = part
            mixed[h] = product

    for j in range(parts):
        kv_copy(partner, kps, kpr, 0, chips - 1, j, partner).wait_recv()
    attend(chip, True)

    def attention(t, carry):
        for j in range(parts):
            for d in range(2):
                @pl.when(t < reach[d])
                def _():
                    owner = source_at(d, t + 1, core)
                    kv_copy(owner, ks, kr, d, t, j, neighbours[d]).wait_recv()

                    @pl.when(t + 1 < reach[d])
                    def _():
                        kv_copy(owner, ks, kr, d, t + 1, j, neighbours[d]).start()

                    kv_copy(owner, kps, kpr, d, t, j, partner).start()

        @pl.when(t == reach[0] - 1)
        def _():
            ring_begin(wo_all, o_sems)

        for d in range(2):
            @pl.when((t > 0) & (t <= reach[d]))
            def _():
                owner = source_at(d, t, 1 - core)
                for j in range(parts):
                    kv_copy(owner, kps, kpr, d, t - 1, j, partner).wait_recv()

                @pl.when(owner // 2 < chip)
                def _():
                    attend(owner // 2, False)
        return carry

    lax.fori_loop(0, reach[0] + 1, attention, 0)
    for h in range(heads):
        att[:, pl.ds(h * HEAD_DIM, HEAD_DIM)] = (mixed[h] / total[h]).astype(BF16)

    def term_copy(p, i):
        return pltpu.make_async_remote_copy(
            src_ref=ts.at[p - 1, i], dst_ref=tr.at[p - 1, i],
            send_sem=ys.at[(p - 1) * slices + i], recv_sem=yr.at[(p - 1) * slices + i],
            device_id={"head": (group + p) % groups}, device_id_type=MESH,
        )

    def out_columns(i):
        return pl.ds(pl.multiple_of(i * half_cols, half_cols), half_cols)

    def make_term(i):
        if not exchange:
            out[:, out_columns(i)] = jnp.dot(att[...], wo_all[i], preferred_element_type=F32).astype(BF16)
            return
        for p in peers:
            span = pl.ds(pl.multiple_of(((group + p) % groups) * rh, rh), rh)
            ts[p - 1, i] = jnp.dot(att[span, :], wo_all[i], preferred_element_type=F32).astype(BF16)
            term_copy(p, i).start()
        span = pl.ds(pl.multiple_of(group * rh, rh), rh)
        tm[i] = jnp.dot(att[span, :], wo_all[i], preferred_element_type=F32).astype(BF16)

    def blocks_of(t):
        return [2 * source_at(d, t, which) + d for d in range(2) for which in (core, 1 - core)]

    def finish(t, carry):
        for i in blocks_of(t):
            value = tm[i].astype(F32)
            for p in peers:
                term_copy(p, i).wait_recv()
                value = value + tr[p - 1, i].astype(F32)
            out[:, out_columns(i)] = value.astype(BF16)
        return carry

    lag = 3

    def partner_terms(t):
        partner_wait(wo_all, o_sems, t)
        for d in range(2):
            make_term(2 * source_at(d, t, 1 - core) + d)

    for d in range(2):
        make_term(2 * me + d)
    partner_terms(0)

    def project_out(t, carry):
        ring_advance(wo_all, o_sems, t)

        @pl.when(t < chips - 1)
        def _():
            for d in range(2):
                make_term(2 * source_at(d, t + 1, core) + d)

        @pl.when(t > 0)
        def _():
            partner_terms(t)

        if exchange:
            @pl.when(t >= lag)
            def _():
                finish(t - lag, 0)
        return carry

    lax.fori_loop(0, chips, project_out, 0)

    if exchange:
        lax.fori_loop(chips - lag, chips, finish, 0)

        def sent(i, carry):
            for p in peers:
                term_copy(p, i).wait_send()
            return carry

        lax.fori_loop(0, slices, sent, 0)

    ring_drain(w_all, w_sems)
    ring_drain(wo_all, o_sems)
    for j in range(parts):
        for d in range(2):
            for t in range(reach[d]):
                kv_copy(me, ks, kr, d, t, j, neighbours[d]).wait_send()
                kv_copy(me, kps, kpr, d, t, j, partner).wait_send()
        kv_copy(me, kps, kpr, 0, chips - 1, j, partner).wait_send()


def pair_kernel(
    n, chunks_in, chunks_out, parts,
    hidden, w_query, w_key, w_value, w_out, *rest_refs,
):
    small = rest_refs[:8]
    out = rest_refs[8]
    held = rest_refs[9:17]
    gain, bias_query, bias_key, bias_value, near_cos, near_sin, far_cos, far_sin = held
    (
    gains, small_sem, hid, w_all, w_second, wo, acc, kv_all, q_ref, high, total, mixed, att, terms, wo_own,
    own_s, own_r, load_sem, swap_s, swap_r, att_s, att_r, ys, yr,
    ws, wr, wps, wpr, os_, or_, ops, opr, ks, kr, kps, kpr, ss, sr, sps, spr,
    ) = rest_refs[17:]
    chips = n // 2
    depth = chips // 2
    ops_from, ops_first, ops_busy, ops_calm, ops_gap = OPS
    stack = STACK
    me = lax.axis_index("seq")
    group = lax.axis_index("head")
    peer = 1 - group
    core = me % 2
    chip = me // 2
    ring = chip // 2 + (chip % 2) * (2 * depth - 1 - 2 * (chip // 2))

    def device_at(position, which):
        position = (position + 2 * chips) % chips
        side = position // depth
        row = position + side * (2 * depth - 1 - 2 * position)
        return 2 * (2 * row + side) + which

    right = device_at(ring + 1, core)
    left = device_at(ring - 1, core)
    partner = 2 * chip + (1 - core)
    neighbours = (right, left)

    def source_at(direction, offset, which):
        return device_at(ring - offset if direction == 0 else ring + offset, which)

    rows, width = hidden.shape
    half_depth = w_query.shape[0] // 2
    q_cols = w_query.shape[1]
    heads = q_cols // HEAD_DIM
    early = heads // 2
    q_early = early * HEAD_DIM
    first_cols = 2 * HEAD_DIM + q_early
    out_depth = w_out.shape[0]
    group_cols = w_out.shape[1] // 2
    lane_cols = group_cols // 2
    rh = rows // 2

    def remote(ref, send, recv, key, device):
        return pltpu.make_async_remote_copy(
            src_ref=ref, dst_ref=ref, send_sem=send.at[key], recv_sem=recv.at[key],
            device_id={"seq": device}, device_id_type=MESH,
        )

    def lanes(which):
        return pl.ds(pl.multiple_of(which * lane_cols, lane_cols), lane_cols)

    def wo_lanes(which, d):
        start = which * group_cols + d * lane_cols
        return pl.ds(pl.multiple_of(start, lane_cols), lane_cols)

    def group_rows(which):
        return pl.ds(pl.multiple_of(which * out_depth, out_depth), out_depth)

    loads, last = [], []
    for h in range(2):
        span = pl.ds(h * half_depth, half_depth)
        slot = w_all.at[2 * me + h]
        loads.append((w_key.at[span], slot.at[:, pl.ds(0, HEAD_DIM)]))
        loads.append((w_value.at[span], slot.at[:, pl.ds(HEAD_DIM, HEAD_DIM)]))
        loads.append((w_query.at[span, pl.ds(0, q_early)], slot.at[:, pl.ds(2 * HEAD_DIM, q_early)]))
        last.append((w_query.at[span, pl.ds(q_early, q_cols - q_early)], w_second.at[2 * me + h]))
        last.append((w_out.at[:, wo_lanes(group, h)], wo.at[chip, h, group_rows(group), lanes(core)]))
        last.append((w_out.at[:, wo_lanes(peer, h)], wo_own.at[h, group_rows(group), lanes(core)]))
    copies = [pltpu.make_async_copy(a, b, load_sem.at[i]) for i, (a, b) in enumerate(loads + [(hidden, hid)] + last)]
    small_copies = [pltpu.make_async_copy(a, b, small_sem.at[i]) for i, (a, b) in enumerate(zip(small, held))]
    for copy in copies[: len(loads)]:
        copy.start()

    barrier = pltpu.get_barrier_semaphore()
    for device in (right, left, partner):
        pl.semaphore_signal(barrier, inc=1, device_id={"seq": device}, device_id_type=MESH)
    pl.semaphore_signal(barrier, inc=1, device_id={"head": peer}, device_id_type=MESH)
    pl.semaphore_wait(barrier, 4)

    def across(src, dst, send, recv, key):
        return pltpu.make_async_remote_copy(
            src_ref=src, dst_ref=dst, send_sem=send.at[key], recv_sem=recv.at[key],
            device_id={"head": peer}, device_id_type=MESH,
        )

    def swap(d):
        return across(
            w_out.at[:, wo_lanes(peer, d)], wo.at[chip, d, group_rows(group), lanes(core)], swap_s, swap_r, d
        )

    def swap_own(d):
        return across(
            w_out.at[:, wo_lanes(group, d)], wo_own.at[d, group_rows(group), lanes(core)], swap_s, swap_r, 2 + d
        )

    def own_copy(d, which):
        return remote(wo_own.at[d, :, lanes(which)], own_s, own_r, d, partner)

    class Ring:
        def __init__(self, view, sems, pieces):
            self.view, self.sems, self.pieces = view, sems, pieces

        def key(self, d, step, j):
            return (d * chips + step) * self.pieces + j

        def begin(self, j):
            send, recv, psend, precv = self.sems
            for d in range(2):
                own = self.view(me, d, j)
                remote(own, send, recv, self.key(d, 0, j), neighbours[d]).start()
            for d in range(2):
                own = self.view(me, d, j)
                remote(own, psend, precv, self.key(d, chips - 1, j), partner).start()

        def advance(self, t, j):
            send, recv, psend, precv = self.sems
            for d in range(2):
                block = self.view(source_at(d, t + 1, core), d, j)
                remote(block, send, recv, self.key(d, t, j), neighbours[d]).wait_recv()

                @pl.when(t < chips - 2)
                def _():
                    remote(block, send, recv, self.key(d, t + 1, j), neighbours[d]).start()

                remote(block, psend, precv, self.key(d, t, j), partner).start()

        def op(self, index):
            @pl.when(index < self.pieces)
            def _():
                self.begin(index)

            @pl.when((index >= self.pieces) & (index < self.pieces * chips))
            def _():
                done = index - self.pieces
                self.advance(done // self.pieces, done % self.pieces)

        def partner_wait(self, t, some=None):
            send, recv, psend, precv = self.sems
            for j in range(self.pieces) if some is None else some:
                for d in range(2):
                    block = self.view(source_at(d, t, 1 - core), d, j)
                    remote(block, psend, precv, self.key(d, (t + chips - 1) % chips, j), partner).wait_recv()

        def drain(self):
            send, recv, psend, precv = self.sems

            def body(t, carry):
                for j in range(self.pieces):
                    for d in range(2):
                        block = self.view(me, d, j)

                        @pl.when(t < chips - 1)
                        def _():
                            remote(block, send, recv, self.key(d, t, j), neighbours[d]).wait_send()

                        remote(block, psend, precv, self.key(d, t, j), partner).wait_send()
                return carry

            lax.fori_loop(0, chips, body, 0)

    def rows_view(buffer, pieces):
        size = buffer.shape[1] // pieces
        return lambda owner, d, j: buffer.at[2 * owner + d, pl.ds(pl.multiple_of(j * size, size), size)]

    def wo_view(owner, d, j):
        size = wo.shape[2] // chunks_out
        return wo.at[owner // 2, d, pl.ds(pl.multiple_of(j * size, size), size), lanes(owner % 2)]

    first = Ring(rows_view(w_all, chunks_in), (ws, wr, wps, wpr), chunks_in)
    third = Ring(wo_view, (os_, or_, ops, opr), chunks_out)

    for copy in copies[: len(loads)]:
        copy.wait()
    for j in range(chunks_in):
        first.begin(j)
    for d in range(2):
        swap(d).start()
    for d in range(2):
        swap_own(d).start()
    for copy in copies[len(loads):] + small_copies:
        copy.start()
    for copy in copies[len(loads):]:
        copy.wait()

    for copy in small_copies:
        copy.wait()
    gains[...] = gain[...].astype(F32)

    slices = 2 * n
    step_cols = width // slices
    gain_rows = step_cols // HEAD_DIM

    def columns(i):
        return pl.ds(pl.multiple_of(i * step_cols, step_cols), step_cols)

    def square(i, carry):
        x = hid[:, columns(i)].astype(F32)
        return carry + x * x

    squares = lax.fori_loop(0, slices, square, jnp.zeros((rows, step_cols), F32))
    inverse = lax.rsqrt(jnp.sum(squares, axis=-1, keepdims=True) * (1.0 / width) + EPSILON)

    def normed(i):
        line = jnp.concatenate([gains[pl.ds(i * gain_rows + r, 1), :] for r in range(gain_rows)], axis=1)
        scaled = hid[:, columns(i)].astype(F32) * inverse * line
        value = scaled.astype(BF16)
        hid[:, columns(i)] = value
        return value

    def widen(line):
        return jnp.broadcast_to(line.astype(F32), (rows, HEAD_DIM))

    acc[:, pl.ds(0, HEAD_DIM)] = widen(bias_key[...])
    acc[:, pl.ds(HEAD_DIM, HEAD_DIM)] = widen(bias_value[...])
    lines = bias_query[...].astype(F32)
    for h in range(heads):
        acc[:, pl.ds((2 + h) * HEAD_DIM, HEAD_DIM)] = widen(lines[h : h + 1])

    far_steps = chips // 2
    reach = [[far_steps - (j * 2 // parts != d) for j in range(parts)] for d in range(2)]

    def second_copy(owner, send, recv, direction, step, j, device):
        return remote(w_second.at[2 * owner + j], send, recv, (direction * chips + step) * 2 + j, device)

    def second_begin():
        for j in range(2):
            for d in range(2):
                second_copy(me, ss, sr, d, 0, j, neighbours[d]).start()
        for j in range(2):
            second_copy(me, sps, spr, 0, chips - 1, j, partner).start()

    def second_advance(t):
        for j in range(2):
            for d in range(2):
                @pl.when(t < reach[d][j])
                def _():
                    owner = source_at(d, t + 1, core)
                    second_copy(owner, ss, sr, d, t, j, neighbours[d]).wait_recv()

                    @pl.when(t + 1 < reach[d][j])
                    def _():
                        second_copy(owner, ss, sr, d, t + 1, j, neighbours[d]).start()

                    second_copy(owner, sps, spr, d, t, j, partner).start()

    def project(t, carry):
        @pl.when(t < chips - 1)
        def _():
            for j in range(chunks_in):
                first.advance(t, j)

        @pl.when(t == chips - 3)
        def _():
            second_begin()

        @pl.when(t == ops_from)
        def _():
            for d in range(2):
                swap(d).wait_recv()

        @pl.when(t == chips // 2)
        def _():
            for d in range(2):
                swap_own(d).wait_recv()
                own_copy(d, core).start()

        @pl.when((t >= ops_from) & (t < ops_from + ops_first))
        def _():
            third.op(t - ops_from)

        first.partner_wait(t)
        for d in range(2):
            i = 2 * source_at(d, t, core) + d
            k = 2 * source_at(d, t, 1 - core) + d
            acc[:, pl.ds(0, first_cols)] += jnp.dot(normed(i), w_all[i], preferred_element_type=F32) + jnp.dot(
                normed(k), w_all[k], preferred_element_type=F32
            )
        return carry

    lax.fori_loop(0, chips, project, 0)

    block_cos, block_sin = far_cos[me], far_sin[me]
    cosine = near_cos[...] * block_cos - near_sin[...] * block_sin
    lane = lax.broadcasted_iota(jnp.int32, cosine.shape, 1)
    sine = near_sin[...] * block_cos + near_cos[...] * block_sin
    sine = jnp.where(lane < HEAD_DIM // 2, -sine, sine)

    def rotary(x):
        return x * cosine + pltpu.roll(x, HEAD_DIM // 2, 1) * sine

    def kv_rows(which):
        return pl.ds(pl.multiple_of(which * rows, rows), rows)

    kv_all[chip, kv_rows(core), pl.ds(0, HEAD_DIM)] = rotary(acc[:, pl.ds(0, HEAD_DIM)]).astype(BF16)
    kv_all[chip, kv_rows(core), pl.ds(HEAD_DIM, HEAD_DIM)] = acc[:, pl.ds(HEAD_DIM, HEAD_DIM)].astype(BF16)
    def turn(h):
        q_ref[pl.ds(h * rows, rows), :] = rotary(acc[:, pl.ds((2 + h) * HEAD_DIM, HEAD_DIM)]).astype(BF16)

    turn(0)
    piece_rows = rows // parts

    def kv_copy(owner, send, recv, direction, step, j, device):
        start = pl.multiple_of((owner % 2) * rows + j * piece_rows, piece_rows)
        block = kv_all.at[owner // 2, pl.ds(start, piece_rows)]
        return remote(block, send, recv, (direction * chips + step) * parts + j, device)

    for j in range(parts):
        for d in range(2):
            kv_copy(me, ks, kr, d, 0, j, neighbours[d]).start()
        kv_copy(me, kps, kpr, 0, chips - 1, j, partner).start()
    second_advance(0)
    for h in range(1, early):
        turn(h)

    factor = HEAD_DIM ** (-0.5) * 1.4426950408889634

    def attend(c, own, which):
        for h in range(which[0], which[1], stack):
            some = pl.ds(h * rows, stack * rows)
            scores = lax.dot_general(
                q_ref[some, :], kv_all[c, :, pl.ds(0, HEAD_DIM)], (((1,), (1,)), ((), ())),
                preferred_element_type=F32,
            )
            if own:
                row = lax.broadcasted_iota(jnp.int32, scores.shape, 0) % rows + core * rows
                col = lax.broadcasted_iota(jnp.int32, scores.shape, 1)
                scores = jnp.where(row >= col, scores, -jnp.inf)
            top = jnp.max(scores, axis=-1, keepdims=True)
            if not own:
                old = high[some, :]
                top = jnp.maximum(old, top)
            probs = jnp.exp2((scores - top) * factor)
            part = jnp.sum(probs, axis=-1, keepdims=True)
            product = jnp.dot(
                probs.astype(BF16), kv_all[c, :, pl.ds(HEAD_DIM, HEAD_DIM)], preferred_element_type=F32
            )
            if not own:
                shrink = jnp.exp2((old - top) * factor)
                part = part + total[some, :] * shrink
                product = product + mixed[some, :] * shrink
            high[some, :] = top
            total[some, :] = part
            mixed[some, :] = product

    for j in range(parts):
        kv_copy(partner, kps, kpr, 0, chips - 1, j, partner).wait_recv()
    attend(chip, True, (0, early))

    busy_steps = far_steps - 1

    def project_second(c):
        total_part = None
        for which in range(2):
            for j in range(2):
                k = 2 * (2 * c + which) + j
                value = jnp.dot(hid[:, columns(k)], w_second[k], preferred_element_type=F32)
                total_part = value if total_part is None else total_part + value
        acc[:, pl.ds(first_cols, q_cols - q_early)] += total_part

    def attention(t, carry):
        second_advance(t + 1)
        for j in range(parts):
            for d in range(2):
                @pl.when(t < reach[d][j])
                def _():
                    owner = source_at(d, t + 1, core)
                    kv_copy(owner, ks, kr, d, t, j, neighbours[d]).wait_recv()

                    @pl.when(t + 1 < reach[d][j])
                    def _():
                        kv_copy(owner, ks, kr, d, t + 1, j, neighbours[d]).start()

                    kv_copy(owner, kps, kpr, d, t, j, partner).start()

        for k in range(max(ops_busy, ops_calm)):
            index = ops_first + ops_busy * jnp.minimum(t, busy_steps) + ops_calm * jnp.maximum(t - busy_steps, 0) + k

            @pl.when(((t < busy_steps) & (k < ops_busy)) | ((t >= busy_steps) & (k < ops_calm)))
            def _():
                third.op(index)

        for j in range(parts):
            for d in range(2):
                @pl.when((t > 0) & (t <= reach[d][j]))
                def _():
                    owner = source_at(d, t, 1 - core)
                    kv_copy(owner, kps, kpr, d, t - 1, j, partner).wait_recv()
                    second_copy(owner, sps, spr, d, t - 1, j, partner).wait_recv()

        @pl.when(t == 0)
        def _():
            for j in range(2):
                second_copy(partner, sps, spr, 0, chips - 1, j, partner).wait_recv()

        for d in range(2):
            other = source_at(d, t, core) // 2

            @pl.when((t > 0) & (t <= far_steps - d) & (other < chip))
            def _():
                attend(other, False, (0, early))

            @pl.when(((t > 0) | (d == 0)) & (t <= far_steps - d))
            def _():
                project_second(other)
        return carry

    lax.fori_loop(0, far_steps + 1, attention, 0)
    ops_middle = ops_first + ops_busy * busy_steps + ops_calm * (far_steps + 1 - busy_steps)
    ops_done = ops_middle + (chips + ops_gap - 1) // ops_gap
    for h in range(early, heads):
        turn(h)
    attend(chip, True, (early, heads))

    def attention_rest(c, carry):
        @pl.when(c % ops_gap == 0)
        def _():
            third.op(ops_middle + c // ops_gap)

        @pl.when(c < chip)
        def _():
            attend(c, False, (early, heads))
        return carry

    lax.fori_loop(0, chips, attention_rest, 0)

    def row_span(which):
        return pl.ds(pl.multiple_of(which * rh, rh), rh)

    def att_copy(key):
        ref = att.at[group, row_span((group + key) % 2), :]
        return across(ref, ref, att_s, att_r, key)

    for h in range(heads):
        att[group, :, pl.ds(h * HEAD_DIM, HEAD_DIM)] = (
            mixed[pl.ds(h * rows, rows), :] / total[pl.ds(h * rows, rows), :]
        ).astype(BF16)
    for key in range(2):
        att_copy(key).start()

    def out_span(c, d, which):
        start = (2 * c + which) * 2 * group_cols + group * group_cols + d * lane_cols
        return pl.ds(pl.multiple_of(start, lane_cols), lane_cols)

    def term_copy(c, d, which):
        src = terms.at[c, d, :, pl.ds(which * lane_cols, lane_cols)]
        return across(src, out.at[:, out_span(c, d, which)], ys, yr, (2 * c + d) * 2 + which)

    def part(weights, which, g):
        return jnp.dot(
            att[g, row_span(which), :], weights[pl.ds(g * out_depth, out_depth), :], preferred_element_type=F32
        ).astype(BF16).astype(F32)

    def product(weights, which):
        return (part(weights, which, 0) + part(weights, which, 1)).astype(BF16)

    def send_terms(c, d, value):
        terms[c, d] = value
        for which in range(2):
            term_copy(c, d, which).start()

    def give(t, d):
        c = source_at(d, t, core) // 2
        send_terms(c, d, product(wo.at[c, d], peer))

    def put(c, d, owner, value):
        for which in range(2):
            start = (2 * c + which) * 2 * group_cols + owner * group_cols + d * lane_cols
            span = pl.ds(pl.multiple_of(start, lane_cols), lane_cols)
            out[:, span] = value[:, which * lane_cols : (which + 1) * lane_cols]

    def keep(t, d):
        c = source_at(d, t, core) // 2
        put(c, d, group, product(wo.at[c, d], group))

    def keep_own(d):
        put(chip, d, group, product(wo.at[chip, d], group))
        put(chip, d, peer, product(wo_own.at[d], group))

    third.partner_wait(0)

    def project_out(t, carry):
        third.partner_wait(t)

        @pl.when(t == 1)
        def _():
            att_copy(0).wait_recv()

        def move(j):
            @pl.when((t + 1) * chunks_out + j >= ops_done)
            def _():
                third.advance(t, j)

        for j in range(chunks_out - 1):
            move(j)
        for d in range(2):
            give(t, d)

        move(chunks_out - 1)

        @pl.when(t == 1)
        def _():
            att_copy(1).wait_recv()

        for d in range(2):
            keep(t, d)

        @pl.when(t == chips // 2)
        def _():
            for d in range(2):
                own_copy(d, 1 - core).wait_recv()
                keep_own(d)
        return carry

    for j in range(chunks_out):
        if chunks_out + j >= ops_done:
            third.advance(0, j)
    lax.fori_loop(1, chips - 1, project_out, 0)
    final = chips - 1
    held_parts = []
    for j in range(chunks_out):
        third.partner_wait(final, (j,))
        for d in range(2):
            held_parts.append(part(wo.at[source_at(d, final, core) // 2, d], peer, j))
    for d in range(2):
        send_terms(source_at(d, final, core) // 2, d, (held_parts[d] + held_parts[2 + d]).astype(BF16))
    for d in range(2):
        keep(final, d)


    first.drain()
    third.drain()
    for j in range(parts):
        for d in range(2):
            for t in range(reach[d][j]):
                kv_copy(me, ks, kr, d, t, j, neighbours[d]).wait_send()
                kv_copy(me, kps, kpr, d, t, j, partner).wait_send()
                second_copy(me, ss, sr, d, t, j, neighbours[d]).wait_send()
                second_copy(me, sps, spr, d, t, j, partner).wait_send()
        kv_copy(me, kps, kpr, 0, chips - 1, j, partner).wait_send()
        second_copy(me, sps, spr, 0, chips - 1, j, partner).wait_send()
    for d in range(2):
        swap(d).wait_send()
        swap_own(d).wait_send()
        own_copy(d, core).wait_send()
    for key in range(2):
        att_copy(key).wait_send()

    def finish(c, carry):
        @pl.when(c != chip)
        def _():
            for d in range(2):
                for which in range(2):
                    term_copy(c, d, which).wait_send()
                    term_copy(c, d, which).wait_recv()
        return carry

    lax.fori_loop(0, chips, finish, 0)


def tables_of(n, rows):
    freq = ROPE_BASE ** (-2.0 * np.arange(HEAD_DIM // 2, dtype=np.float64) / HEAD_DIM)
    freq = np.concatenate([freq, freq])
    near = np.arange(rows, dtype=np.float64)[:, None] * freq
    far = (np.arange(n, dtype=np.float64) * rows)[:, None, None] * freq
    return [f(a).astype(np.float32) for a in (near, far) for f in (np.cos, np.sin)]


def pair_local(n, hidden, norm_gain, w_query, w_key, w_value, bias_query, bias_key, bias_value, w_out):
    rows, width = hidden.shape
    cols = w_query.shape[1]
    heads = cols // HEAD_DIM
    early = heads // 2 * HEAD_DIM
    chips = n // 2
    slices = 2 * n
    half_depth = w_query.shape[0] // 2
    group_cols = w_out.shape[1] // 2
    chunks_in, chunks_out, parts = PIECES
    vectors = [v.reshape(-1, HEAD_DIM) for v in (norm_gain, bias_query, bias_key, bias_value)]
    small = vectors + tables_of(n, rows)
    result = jax.ShapeDtypeStruct((rows // 2, w_out.shape[1] * n), BF16)
    any_spec = pl.BlockSpec(memory_space=pl.ANY)
    dma = pltpu.SemaphoreType.DMA
    return pl.pallas_call(
        functools.partial(pair_kernel, n, chunks_in, chunks_out, parts),
        out_shape=pltpu.VMEM(result.shape, result.dtype),
        in_specs=[any_spec] * 13,
        out_specs=pl.BlockSpec(memory_space=pltpu.VMEM),
        scratch_shapes=[pltpu.VMEM(a.shape, a.dtype) for a in small]
        + [
            pltpu.VMEM((width // HEAD_DIM, HEAD_DIM), F32),
            dma((8,)),
            pltpu.VMEM((rows, width), BF16),
            pltpu.VMEM((slices, half_depth, 2 * HEAD_DIM + early), BF16),
            pltpu.VMEM((slices, half_depth, cols - early), BF16),
            pltpu.VMEM((chips, 2, 2 * w_out.shape[0], group_cols), BF16),
            pltpu.VMEM((rows, 2 * HEAD_DIM + cols), F32),
            pltpu.VMEM((chips, 2 * rows, 2 * HEAD_DIM), BF16),
            pltpu.VMEM((heads * rows, HEAD_DIM), BF16),
            pltpu.VMEM((heads * rows, 1), F32),
            pltpu.VMEM((heads * rows, 1), F32),
            pltpu.VMEM((heads * rows, HEAD_DIM), F32),
            pltpu.VMEM((2, rows, cols), BF16),
            pltpu.VMEM((chips, 2, rows // 2, group_cols), BF16),
            pltpu.VMEM((2, 2 * w_out.shape[0], group_cols), BF16),
            dma((2,)), dma((2,)),
            dma((13,)),
            dma((4,)), dma((4,)), dma((2,)), dma((2,)),
            dma((4 * chips,)), dma((4 * chips,)),
        ]
        + [dma((2 * chips * chunks_in,))] * 4
        + [dma((2 * chips * chunks_out,))] * 4
        + [dma((2 * chips * parts,))] * 4
        + [dma((4 * chips,))] * 4,
        compiler_params=pltpu.CompilerParams(
            collective_id=0, has_side_effects=True, vmem_limit_bytes=VMEM_LIMIT - 2 * result.size
        ),
    )(hidden, w_query, w_key, w_value, w_out, *small)


def fits_pair(n, groups, rows, w_query, w_out):
    chips = n // 2
    return (
        groups == 2
        and chips % 4 == 0
        and rows % 32 == 0
        and w_query.shape[1] % (4 * HEAD_DIM) == 0
        and w_query.shape[0] % 128 == 0
        and w_out.shape[1] % 512 == 0
    )


def local(n, groups, hidden, norm_gain, w_query, w_key, w_value, bias_query, bias_key, bias_value, w_out):
    rows, width = hidden.shape
    if fits_pair(n, groups, rows, w_query, w_out):
        return pair_local(n, hidden, norm_gain, w_query, w_key, w_value, bias_query, bias_key, bias_value, w_out)
    cols = w_query.shape[1]
    heads = cols // HEAD_DIM
    wide = cols + 2 * HEAD_DIM
    chips = n // 2
    exchange = groups > 1 and (rows // groups) % 16 == 0
    rh = rows // groups
    slices = 2 * n
    half_depth = w_query.shape[0] // 2
    half_cols = w_out.shape[1] // 2

    tables = tables_of(n, rows)
    vectors = [v.reshape(1, -1) for v in (norm_gain, bias_query, bias_key, bias_value)]

    any_spec = pl.BlockSpec(memory_space=pl.ANY)
    vmem = pl.BlockSpec(memory_space=pltpu.VMEM)
    links = max(groups - 1, 1) if exchange else 1
    pieces = slices if exchange else 1
    rpart = rh if exchange else 16
    dma = pltpu.SemaphoreType.DMA
    result = pl.pallas_call(
        functools.partial(kernel, n, groups, exchange),
        out_shape=jax.ShapeDtypeStruct((rh if exchange else rows, w_out.shape[1] * n), BF16),
        in_specs=[any_spec] * 5 + [vmem] * 8,
        out_specs=vmem,
        scratch_shapes=[
            pltpu.VMEM((rows, width), BF16),
            pltpu.VMEM((slices, half_depth, wide), BF16),
            pltpu.VMEM((slices, w_out.shape[0], half_cols), BF16),
            pltpu.VMEM((rows, wide), F32),
            pltpu.VMEM((chips, 2 * rows, 2 * HEAD_DIM), BF16),
            pltpu.VMEM((heads, rows, HEAD_DIM), BF16),
            pltpu.VMEM((heads, rows, 1), F32),
            pltpu.VMEM((heads, rows, 1), F32),
            pltpu.VMEM((heads, rows, HEAD_DIM), F32),
            pltpu.VMEM((rows, cols), BF16),
            pltpu.VMEM((links, pieces, rpart, half_cols), BF16),
            pltpu.VMEM((links, pieces, rpart, half_cols), BF16),
            pltpu.VMEM((pieces, rpart, half_cols), BF16),
            dma((9,)),
        ]
        + [dma((4 * chips,))] * 12
        + [dma((links * pieces,))] * 2,
        compiler_params=pltpu.CompilerParams(
            collective_id=0, has_side_effects=True, vmem_limit_bytes=64 * 1024 * 1024 - 128 * 1024
        ),
    )(hidden, w_query, w_key, w_value, w_out, *vectors, *tables)
    if exchange:
        return result
    return lax.psum_scatter(result, "head", scatter_dimension=0, tiled=True)


def solution(mesh):
    in_specs = (
        P("seq", None),
        P(),
        P("seq", "head"),
        P("seq", "head"),
        P("seq", "head"),
        P("head"),
        P("head"),
        P("head"),
        P("head", "seq"),
    )
    out_specs = P(("seq", "head"), None)
    body = functools.partial(local, mesh.shape["seq"], mesh.shape["head"])
    return jax.shard_map(body, mesh=mesh, in_specs=in_specs, out_specs=out_specs, check_vma=False)
```
